32 devices in a mesh: dp: 4 (over z), row: 4 (over y, core), col: 2 (over x).
Axes of the slice: x: 2, y: 2, z: 4, core: 2. Of those that a mesh axis runs over, the one named last changes fastest.
Arguments:
- inputs: bfloat16 [16384, 1024], P(('dp', 'col'), 'row'), may hold values from -6 to 6
- gain_first: float32 [1024], P('row'), may hold values from 0.5 to 1.5
- shift_first: float32 [1024], P('row'), may hold values from -1 to 1
- w_query: bfloat16 [1024, 1024], P('row', 'col'), may hold values from -0.1875 to 0.1875
- w_key: bfloat16 [1024, 1024], P('row', 'col'), may hold values from -0.1875 to 0.1875
- w_value: bfloat16 [1024, 1024], P('row', 'col'), may hold values from -0.1875 to 0.1875
- w_output: bfloat16 [1024, 1024], P('col', 'row'), may hold values from -1.5 to 1.5
- gain_second: float32 [1024], P('row'), may hold values from 0.5 to 1.5
- shift_second: float32 [1024], P('row'), may hold values from -1 to 1
- w_up: bfloat16 [1024, 4096], P('row', 'col'), may hold values from -0.1875 to 0.1875
- bias_up: float32 [4096], P('col'), may hold values from -1.5 to 1.5
- w_down: bfloat16 [4096, 1024], P('col', 'row'), may hold values from -0.09375 to 0.09375
- bias_down: float32 [1024], P('row'), may hold values from -2.5 to 2.5
- segments: int32 [16, 1024], P(('dp', 'row')), may hold values from 0 to 4, as said below
- random_blocks: int32 [16, 16, 3], P('col'), may hold values from 0 to 15
- global_blocks: int32 [2], replicated, may hold values from 0 to 15, as said below
- cotangent: bfloat16 [16384, 1024], P(('dp', 'col'), 'row'), may hold values from -6 to 6
Outputs:
- layer_out: bfloat16 [16384, 1024], P(('dp', 'col'), 'row')
- grad_inputs: float32 [16384, 1024], P(('dp', 'col'), 'row')
- grad_gain_first: float32 [1024], P('row')
- grad_shift_first: float32 [1024], P('row')
- grad_w_query: float32 [1024, 1024], P('row', 'col')
- grad_w_key: float32 [1024, 1024], P('row', 'col')
- grad_w_value: float32 [1024, 1024], P('row', 'col')
- grad_w_output: float32 [1024, 1024], P('col', 'row')
- grad_gain_second: float32 [1024], P('row')
- grad_shift_second: float32 [1024], P('row')
- grad_w_up: float32 [1024, 4096], P('row', 'col')
- grad_bias_up: float32 [4096], P('col')
- grad_w_down: float32 [4096, 1024], P('col', 'row')
- grad_bias_down: float32 [1024], P('row')
The draws below stay inside these ranges and needn't reach their ends.
Inputs may be any that keep to these rules, and one draw needn't show every extreme that they name: `segments`: each sequence of 1024 tokens holds four documents labelled 1, 2, 3, 4 in order, then 1 to 64 padding tokens labelled 0; each of the first three documents has 100 to 300 tokens. `global_blocks`: distinct block positions; one of them is the last block, 15.
All inputs are finite; a program needn't handle non-finite values.
Results may differ from the reference program's by a relative error of at most 0.015.
Values may be sent and summed in bfloat16 or wider, within the bound.
No kernel may reach another device: no remote copies, remote signals or barrier semaphores. Data moves between devices by JAX's collectives and lax.ppermute only.
A program may use at most 256 MiB of HBM per device.

```python
import math
import jax
import jax.numpy as jnp
from jax import lax

D = 1024
H = 16
HD = 64
FF = 4096
BLK = 64
NRAND = 3
NGLOB = 2
L = 1024
NB = 16
SEQS = 16
TOKENS = 16384


def draw_segments(key, part):
    lowest = 100 * L // 1024
    highest = 300 * L // 1024
    key_docs = jax.random.fold_in(key, 11)
    key_pads = jax.random.fold_in(key, 23)
    doc_sizes = jax.random.randint(key_docs, (SEQS, 3), lowest, highest + 1)
    padding = jax.random.randint(key_pads, (SEQS, 1), 1, L // 16 + 1)
    doc_ends = jnp.cumsum(doc_sizes, axis=1)
    places = jnp.arange(L, dtype=jnp.int32)[None, :]
    labels = 1 + jnp.sum((places[:, :, None] >= doc_ends[:, None, :]).astype(jnp.int32), axis=2)
    labels = jnp.where(places >= L - padding, 0, labels)
    return labels.astype(jnp.int32)


def draw_global_blocks(key, part):
    others = jax.random.permutation(jax.random.fold_in(key, 5), NB - 1)[:NGLOB - 1].astype(jnp.int32)
    chosen = jnp.concatenate((others, jnp.full((1,), NB - 1, dtype=jnp.int32)))
    order = jax.random.permutation(jax.random.fold_in(key, 7), NGLOB)
    return chosen[order].astype(jnp.int32)


def touch_ends(drawn, own_key, smallest, top_value):
    place = [jax.random.randint(jax.random.fold_in(own_key, axis), (), 0, length) for axis, length in enumerate(drawn.shape)]
    widest = drawn.shape.index(max(drawn.shape))
    next_to = place[:widest] + [(place[widest] + 1) % drawn.shape[widest]] + place[widest + 1:]
    return drawn.at[tuple(place)].set(smallest).at[tuple(next_to)].set(top_value)


def shard_levels(own_key, dims, cuts, smallest, high):
    loudness, own = 1.0, jax.random.fold_in(own_key, 6)
    for axis_at, blocks in cuts:
        draws = jnp.exp(jax.random.uniform(jax.random.fold_in(own, axis_at), (blocks,), jnp.float32, smallest / len(cuts), high / len(cuts)))
        loudness = loudness * jnp.repeat(draws, dims[axis_at] // blocks).reshape([-1 if axis == axis_at else 1 for axis in range(len(dims))])
    return loudness


def centred(own_key, shape, scale, bound, shards=(), held_as=jnp.bfloat16):
    drawn = jax.random.normal(own_key, shape, jnp.float32) * scale
    if len(shards) > 0:
        drawn = shard_levels(own_key, shape, shards, -0.22, 0.18) * drawn
    return jnp.clip(drawn, min=-bound, max=bound).astype(held_as)


def setup_inputs(seed: int = 0) -> dict:
    key_of = jax.random.split(jax.random.key(seed), 18)
    return {
        "inputs": centred(key_of[0], (TOKENS, D), 1.0, 6.0, ((0, 8), (1, 4))),
        "gain_first": jnp.clip(1.0 + 0.1 * jax.random.normal(key_of[1], (D,), jnp.float32), 0.5, 1.5),
        "shift_first": centred(key_of[2], (D,), 0.2, 1.0, ((0, 4),), jnp.float32),
        "w_query": centred(key_of[3], (D, D), D ** -0.5, 0.1875, ((0, 4), (1, 2))),
        "w_key": centred(key_of[4], (D, D), D ** -0.5, 0.1875, ((0, 4), (1, 2))),
        "w_value": centred(key_of[5], (D, D), D ** -0.5, 0.1875, ((0, 4), (1, 2))),
        "w_output": centred(key_of[6], (D, D), 16 ** -0.5, 1.5, ((0, 2), (1, 4))),
        "gain_second": jnp.clip(1.0 + 0.1 * jax.random.normal(key_of[7], (D,), jnp.float32), 0.5, 1.5),
        "shift_second": centred(key_of[8], (D,), 0.2, 1.0, ((0, 4),), jnp.float32),
        "w_up": centred(key_of[9], (D, FF), D ** -0.5, 0.1875, ((0, 4), (1, 2))),
        "bias_up": centred(key_of[10], (FF,), 0.3, 1.5, ((0, 2),), jnp.float32),
        "w_down": centred(key_of[11], (FF, D), FF ** -0.5, 0.09375, ((0, 2), (1, 4))),
        "bias_down": centred(key_of[12], (D,), 0.5, 2.5, ((0, 4),), jnp.float32),
        "segments": draw_segments(jax.random.fold_in(key_of[17], 71), 0),
        "random_blocks": touch_ends(jax.random.randint(key_of[14], (H, NB, NRAND), 0, NB), jax.random.fold_in(key_of[14], 1), 0, NB - 1).astype(jnp.int32),
        "global_blocks": draw_global_blocks(jax.random.fold_in(key_of[17], 71), 0),
        "cotangent": centred(key_of[16], (TOKENS, D), 1.0, 6.0, ((0, 8), (1, 4))),
    }


EPS = 1e-05
HIGHEST = lax.Precision.HIGHEST

@jax.custom_vjp
def low(v):
    return lax.optimization_barrier(v.astype(jnp.bfloat16)).astype(jnp.float32)

@jax.custom_vjp
def low_back(v):
    return v

def low_keep(v):
    return (low(v), None)

def low_pass(kept, grad):
    return (grad,)

def back_keep(v):
    return (v, None)

def back_low(kept, grad):
    return (low(grad),)
low.defvjp(low_keep, low_pass)
low_back.defvjp(back_keep, back_low)

def matmul(left, right):
    return jnp.dot(left, right, precision=HIGHEST)

def layer_norm(moving, gain_row, shift_row):
    center = lax.optimization_barrier(jnp.mean(moving, axis=1, keepdims=True))
    spread = lax.optimization_barrier(jnp.mean(moving * moving, axis=1, keepdims=True)) - center * center
    return (moving - center) * lax.rsqrt(spread + EPS) * gain_row + shift_row

def expand_table(random_blocks, global_blocks):
    block_ids = jnp.arange(NB, dtype=jnp.int32)
    nearby = jnp.abs(block_ids[:, None] - block_ids[None, :]) <= 1
    chosen = jnp.any(random_blocks[:, :, :, None] == block_ids[None, None, None, :], axis=2)
    marked = jnp.any(global_blocks[:, None] == block_ids[None, :], axis=0)
    block_table = nearby[None] | chosen | marked[None, None, :] | marked[None, :, None]
    return jnp.repeat(jnp.repeat(block_table, BLK, axis=1), BLK, axis=2)

def attention(queries, key_block, value_block, segments, pattern):
    seq_shape = (SEQS, L, H, HD)
    score_scale = 1.0 / math.sqrt(HD)

    def one_seq(pieces):
        seq_queries, seq_keys, seq_values, labels = pieces
        same_doc = (labels[:, None] == labels[None, :]) & (labels[None, :] != 0)
        allowed = pattern & same_doc[None]
        raw_scores = low_back(jnp.einsum('qhd,khd->hqk', seq_queries, seq_keys, precision=HIGHEST))
        logits = jnp.where(allowed, raw_scores * score_scale, -1000000000.0)
        row_peak = lax.optimization_barrier(jnp.max(logits, axis=2, keepdims=True))
        exp_terms = jnp.exp(logits - row_peak)
        softmax = exp_terms / lax.optimization_barrier(jnp.sum(exp_terms, axis=2, keepdims=True))
        attended = jnp.einsum('hqk,khd->qhd', low(softmax), seq_values, precision=HIGHEST)
        return attended * (labels != 0).astype(jnp.float32)[:, None, None]
    outputs = lax.map(jax.checkpoint(one_seq), (queries.reshape(seq_shape), key_block.reshape(seq_shape), value_block.reshape(seq_shape), segments))
    return outputs.reshape(SEQS * L, H * HD)

def forward(params, segments, pattern):
    inputs, gain_first, shift_first, w_query, w_key, w_value, w_output, gain_second, shift_second, w_up, bias_up, w_down, bias_down = params
    first_low = low(layer_norm(inputs, gain_first, shift_first))
    queries = low(low_back(matmul(first_low, w_query)))
    key_block = low(low_back(matmul(first_low, w_key)))
    value_block = low(low_back(matmul(first_low, w_value)))
    heads = low(low_back(attention(queries, key_block, value_block, segments, pattern)))
    mixed = low_back(matmul(heads, w_output))
    residual = inputs + mixed
    second_low = low(layer_norm(residual, gain_second, shift_second))
    upward = low_back(matmul(second_low, w_up) + bias_up)
    hidden = low(jax.nn.gelu(upward, approximate=True))
    return residual + matmul(hidden, w_down) + bias_down

def reference(inputs, gain_first, shift_first, w_query, w_key, w_value, w_output, gain_second, shift_second, w_up, bias_up, w_down, bias_down, segments, random_blocks, global_blocks, cotangent):
    pattern = expand_table(random_blocks, global_blocks)
    floats = tuple((item.astype(jnp.float32) for item in (inputs, gain_first, shift_first, w_query, w_key, w_value, w_output, gain_second, shift_second, w_up, bias_up, w_down, bias_down)))

    def forward_only(*params):
        return forward(params, segments, pattern)
    result_out, pull_back = jax.vjp(forward_only, *floats)
    gradients = pull_back(cotangent.astype(jnp.float32))
    return (result_out.astype(jnp.bfloat16), gradients[0], gradients[1], gradients[2], gradients[3], gradients[4], gradients[5], gradients[6], gradients[7], gradients[8], gradients[9], gradients[10], gradients[11], gradients[12])
```

```python
import math

import jax
import jax.numpy as jnp
from jax import lax
from jax.experimental import pallas as pl
from jax.experimental.pallas import tpu as pltpu
from jax.sharding import PartitionSpec as P

D = 1024
HD = 64
BLK = 64
NB = 16


EPS = 1e-05


def product(picked, weight, flipped):
    if flipped:
        return lax.dot_general(
            picked, weight, (((1,), (1,)), ((), ())), preferred_element_type=jnp.float32
        )
    return jnp.dot(picked, weight, preferred_element_type=jnp.float32)


def to_columns(moving, weight, flipped):
    gathered = lax.all_gather(moving, "col", axis=0, tiled=True)
    row_count = gathered.shape[0] // lax.axis_size("row")

    def term_rows(first_row, how_many):
        return product(gathered, weight, flipped)

    result = lax.psum_scatter(
        term_rows(jnp.int32(0), lax.axis_size("row") * row_count),
        "row",
        scatter_dimension=0,
        tiled=True,
    )
    return (result, gathered)


def to_rows(moving, weight, flipped):
    gathered = lax.all_gather(moving, "row", axis=0, tiled=True)
    row_count = gathered.shape[0] // lax.axis_size("col")

    def term_rows(first_row, how_many):
        return product(gathered, weight, flipped)

    return (
        lax.psum_scatter(
            term_rows(jnp.int32(0), lax.axis_size("col") * row_count),
            "col",
            scatter_dimension=0,
            tiled=True,
        ),
        gathered,
    )


def norm_sums(first_sum, second_sum):
    return lax.psum((first_sum, second_sum), "row")


def norm_forward(moving, gain_row, shift_row):
    totals, squares = norm_sums(jnp.sum(moving, axis=1), jnp.sum(moving * moving, axis=1))
    center = totals / D
    spread = squares / D - center * center
    inverse = lax.rsqrt(spread + EPS)
    normed = (moving - center[:, None]) * inverse[:, None]
    return (normed * gain_row + shift_row, normed, inverse)


def norm_backward(upstream, normed, inverse, gain_row):
    scaled = upstream * gain_row
    first_sum, second_sum = norm_sums(jnp.sum(scaled, axis=1), jnp.sum(scaled * normed, axis=1))
    return inverse[:, None] * (scaled - first_sum[:, None] / D - normed * (second_sum[:, None] / D))


def head_masks(random_blocks, global_blocks):
    block_ids = jnp.arange(NB, dtype=jnp.int32)
    nearby = jnp.abs(block_ids[:, None] - block_ids[None, :]) <= 1
    chosen = jnp.any(random_blocks[:, :, :, None] == block_ids[None, None, None, :], axis=2)
    marked = jnp.any(global_blocks[:, None] == block_ids[None, :], axis=0)
    block_table = nearby[None] | chosen | marked[None, None, :] | marked[None, :, None]
    return jnp.repeat(jnp.repeat(block_table, BLK, axis=1), BLK, axis=2)


def seq_logits(seq_queries, seq_keys, labels, pattern):
    same_doc = (labels[:, None] == labels[None, :]) & (labels[None, :] != 0)
    raw_scores = jnp.einsum(
        "qhd,khd->hqk", seq_queries, seq_keys, preferred_element_type=jnp.float32
    )
    return jnp.where(pattern & same_doc[None], raw_scores * (1.0 / math.sqrt(HD)), -1000000000.0)


def attend_plain(queries, key_block, value_block, segments, pattern):

    def one_seq(pieces):
        seq_queries, seq_keys, seq_values, labels = pieces
        logits = seq_logits(seq_queries, seq_keys, labels, pattern)
        row_peak = jnp.max(logits, axis=2, keepdims=True)
        exp_terms = jnp.exp(logits - row_peak)
        row_total = jnp.sum(exp_terms, axis=2, keepdims=True)
        softmax = (exp_terms / row_total).astype(jnp.bfloat16)
        attended = jnp.einsum(
            "hqk,khd->qhd", softmax, seq_values, preferred_element_type=jnp.float32
        )
        live_rows = (labels != 0).astype(jnp.float32)
        return (attended * live_rows[:, None, None], (row_peak + jnp.log(row_total))[:, :, 0])

    return lax.map(one_seq, (queries, key_block, value_block, segments))


def attend_plain_backward(queries, key_block, value_block, segments, pattern, grad_heads, log_total):

    def one_seq(pieces):
        seq_queries, seq_keys, seq_values, labels, seq_grads, seq_log = pieces
        logits = seq_logits(seq_queries, seq_keys, labels, pattern)
        softmax = jnp.exp(logits - seq_log[:, :, None])
        grad_probs = jnp.einsum(
            "qhd,khd->hqk", seq_grads, seq_values, preferred_element_type=jnp.float32
        )
        grad_values = jnp.einsum(
            "hqk,qhd->khd",
            softmax.astype(jnp.bfloat16),
            seq_grads,
            preferred_element_type=jnp.float32,
        )
        inner_sum = jnp.sum(softmax * grad_probs, axis=2, keepdims=True)
        grad_raw = (softmax * (grad_probs - inner_sum) * (1.0 / math.sqrt(HD))).astype(jnp.bfloat16)
        grad_queries = jnp.einsum(
            "hqk,khd->qhd", grad_raw, seq_keys, preferred_element_type=jnp.float32
        )
        grad_keys = jnp.einsum(
            "hqk,qhd->khd", grad_raw, seq_queries, preferred_element_type=jnp.float32
        )
        return (grad_queries, grad_keys, grad_values)

    return lax.map(one_seq, (queries, key_block, value_block, segments, grad_heads, log_total))


def gelu_tanh(values):
    return jax.nn.gelu(values, approximate=True)


def weight_grad(left, right):
    return lax.dot_general(
        left, right, (((0,), (0,)), ((), ())), preferred_element_type=jnp.float32
    )


def body(
    inputs,
    gain_first,
    shift_first,
    w_query,
    w_key,
    w_value,
    w_output,
    gain_second,
    shift_second,
    w_up,
    bias_up,
    w_down,
    bias_down,
    segments,
    random_blocks,
    global_blocks,
    cotangent,
):
    seq_count, seq_len = segments.shape
    head_width = w_query.shape[1]
    heads_here = random_blocks.shape[0]
    seq_shape = (seq_count, seq_len, heads_here, HD)
    pattern = head_masks(random_blocks, global_blocks)
    live_tokens = (segments != 0).reshape(-1)
    x_first = inputs.astype(jnp.float32)
    first_full, normed_one, inverse_one = norm_forward(x_first, gain_first, shift_first)
    first_low = first_full.astype(jnp.bfloat16)
    stacked = jnp.concatenate((w_query, w_key, w_value), axis=1)
    projected, first_all = to_columns(first_low, stacked, False)
    proj_low = projected.astype(jnp.bfloat16)
    queries = proj_low[:, :head_width].reshape(seq_shape)
    key_block = proj_low[:, head_width : 2 * head_width].reshape(seq_shape)
    value_block = proj_low[:, 2 * head_width :].reshape(seq_shape)
    heads_out, log_total = attend_plain(queries, key_block, value_block, segments, pattern)
    heads_low = heads_out.reshape(-1, head_width).astype(jnp.bfloat16)
    mixed_out, heads_all = to_rows(heads_low, w_output, False)
    residual = x_first + mixed_out
    second_full, normed_two, inverse_two = norm_forward(residual, gain_second, shift_second)
    second_low = second_full.astype(jnp.bfloat16)
    upward, second_all = to_columns(second_low, w_up, False)
    upward = upward + bias_up
    hidden_low = gelu_tanh(upward).astype(jnp.bfloat16)
    downward, hidden_all = to_rows(hidden_low, w_down, False)
    layer_out = (residual + (downward + bias_down)).astype(jnp.bfloat16)
    grad_hidden, cotangent_all = to_columns(cotangent, w_down, True)
    activated, pull_back = jax.vjp(gelu_tanh, upward)
    grad_upward = pull_back(grad_hidden)[0].astype(jnp.bfloat16)
    grad_second, grad_upward_all = to_rows(grad_upward, w_up, True)
    grad_residual = cotangent.astype(jnp.float32) + norm_backward(
        grad_second, normed_two, inverse_two, gain_second
    )
    grad_mixed = grad_residual.astype(jnp.bfloat16)
    grad_heads, grad_mixed_all = to_columns(grad_mixed, w_output, True)
    grad_heads = jnp.where(live_tokens[:, None], grad_heads, 0.0).astype(jnp.bfloat16)
    grad_queries, grad_keys, grad_values = attend_plain_backward(
        queries, key_block, value_block, segments, pattern, grad_heads.reshape(seq_shape), log_total
    )
    grad_proj = jnp.concatenate(
        (
            grad_queries.reshape(-1, head_width),
            grad_keys.reshape(-1, head_width),
            grad_values.reshape(-1, head_width),
        ),
        axis=1,
    ).astype(jnp.bfloat16)
    grad_first, grad_proj_all = to_rows(grad_proj, stacked, True)
    grad_inputs = grad_residual + norm_backward(grad_first, normed_one, inverse_one, gain_first)
    grad_stacked = weight_grad(first_all, grad_proj_all)
    grad_out_weight = weight_grad(heads_all, grad_mixed_all)
    grad_up_weight = weight_grad(second_all, grad_upward_all)
    grad_down_weight = weight_grad(hidden_all, cotangent_all)
    grad_up_bias = jnp.sum(grad_upward_all, axis=0, dtype=jnp.float32)
    grad_down_bias = jnp.sum(cotangent_all, axis=0, dtype=jnp.float32)
    gain_terms = lax.psum(
        (
            jnp.sum(grad_first * normed_one, axis=0),
            jnp.sum(grad_first, axis=0),
            jnp.sum(grad_second * normed_two, axis=0),
            jnp.sum(grad_second, axis=0),
        ),
        ("dp", "col"),
    )
    summed = (
        lax.psum(grad_stacked.astype(jnp.bfloat16), "dp").astype(jnp.float32),
        lax.psum(grad_out_weight.astype(jnp.bfloat16), "dp").astype(jnp.float32),
        lax.psum(grad_up_weight.astype(jnp.bfloat16), "dp").astype(jnp.float32),
        lax.psum(grad_down_weight.astype(jnp.bfloat16), "dp").astype(jnp.float32),
        lax.psum(grad_up_bias.astype(jnp.bfloat16), "dp").astype(jnp.float32),
        lax.psum(grad_down_bias.astype(jnp.bfloat16), "dp").astype(jnp.float32),
    )
    return (
        layer_out,
        grad_inputs,
        gain_terms[0],
        gain_terms[1],
        summed[0][:, :head_width],
        summed[0][:, head_width : 2 * head_width],
        summed[0][:, 2 * head_width :],
        summed[1],
        gain_terms[2],
        gain_terms[3],
        summed[2],
        summed[4],
        summed[3],
        summed[5],
    )


SWAP = [(0, 1), (1, 0)]
LOW = jnp.bfloat16
FULL = jnp.float32
TILE = 256
BIG = 1e30


def swap(array, axis):
    return lax.ppermute(array, axis, SWAP)


def dot_nn(left, right):
    return lax.dot_general(left, right, (((1,), (0,)), ((), ())), preferred_element_type=FULL)


def dot_nt(left, right):
    return lax.dot_general(left, right, (((1,), (1,)), ((), ())), preferred_element_type=FULL)


def dot_tn(left, right):
    return lax.dot_general(left, right, (((0,), (0,)), ((), ())), preferred_element_type=FULL)


def attention_extras(labels, random_blocks, global_blocks):
    length = labels.shape[0]
    blocks = length // BLK
    block_ids = jnp.arange(blocks, dtype=jnp.int32)
    nearby = jnp.abs(block_ids[:, None] - block_ids[None, :]) <= 1
    chosen = jnp.any(random_blocks[:, :, :, None] == block_ids[None, None, None, :], axis=2)
    marked = jnp.any(global_blocks[:, None] == block_ids[None, :], axis=0)
    table = nearby[None] | chosen | marked[None, None, :] | marked[None, :, None]
    heads = table.shape[0]
    lane = jnp.arange(HD, dtype=jnp.int32)
    place = jnp.arange(length, dtype=jnp.int32) // BLK
    doc_lane = blocks + jnp.where(labels == 0, 4, labels - 1)
    row_extra = ((lane[None, :] == place[:, None]) | (lane[None, :] == doc_lane[:, None])).astype(LOW)
    table_keys = jnp.pad(jnp.swapaxes(table, 1, 2), ((0, 0), (0, 0), (0, HD - blocks)), constant_values=True)
    table_keys = jnp.repeat(table_keys, BLK, axis=1)
    is_doc = (lane >= blocks) & (lane <= blocks + 4)
    doc_bad = is_doc[None, :] & (lane[None, :] != doc_lane[:, None])
    doc_bad = doc_bad | (lane[None, :] == blocks + 4)
    key_extra = jnp.where(table_keys & ~doc_bad[None], 0.0, -BIG)
    key_extra = jnp.where((lane >= blocks + 5) & (lane <= blocks + 7), 1.0, key_extra).astype(LOW)
    rows = jnp.stack((jnp.pad(row_extra, ((0, 0), (HD, 0))), jnp.pad(row_extra, ((0, 0), (0, HD)))))
    even = jnp.pad(key_extra[0::2], ((0, 0), (0, 0), (HD, 0)))
    odd = jnp.pad(key_extra[1::2], ((0, 0), (0, 0), (0, HD)))
    keys = jnp.stack((even, odd), axis=1).reshape(heads, length, 2 * HD)
    tiles = length // TILE
    known = labels[None, :] == jnp.arange(1, 5, dtype=jnp.int32)[:, None]
    present = jnp.any(known.reshape(4, tiles, TILE), axis=2)
    wanted = jnp.any(present[:, :, None] & known[:, None, :], axis=0)
    spots = jnp.arange(length, dtype=jnp.int32)
    first = jnp.min(jnp.where(wanted, spots[None, :], length - 1), axis=1)
    last = jnp.max(jnp.where(wanted, spots[None, :], 0), axis=1)
    start = first // 128
    count = jnp.maximum((last + 1 - start * 128 + 255) // 256, 1)
    start = jnp.minimum(start, length // 128 - 2 * count)
    return rows, keys, jnp.stack((start, count)).astype(jnp.int32)


def attend_forward_kernel(where_ref, q_ref, k_ref, v_ref, rows_ref, keys_ref, out_ref, kept_ref, kk, vv):
    length = q_ref.shape[0]
    lane = lax.broadcasted_iota(jnp.int32, (length, 2 * HD), 1)
    for e in range(2):
        data = (lane < HD) if e == 0 else (lane >= HD)
        kk[e] = jnp.where(data, k_ref[...], keys_ref[e])
        vv[e] = jnp.where(data, v_ref[...], jnp.ones_like(v_ref[...]))
    tile_lane = lax.broadcasted_iota(jnp.int32, (TILE, 2 * HD), 1)

    def one_tile(t, carry):
        rows = pl.ds(pl.multiple_of(t * TILE, TILE), TILE)
        start = pl.multiple_of(where_ref[0, t] * 128, 128)
        count = where_ref[1, t]
        q_pair = q_ref[rows, :] * jnp.bfloat16(1.0 / math.sqrt(HD))
        for n in range(1, length // TILE + 1):

            @pl.when(count == n)
            def _():
                span = pl.ds(start, n * TILE)
                outs = []
                for e in range(2):
                    data = (tile_lane < HD) if e == 0 else (tile_lane >= HD)
                    base = HD if e == 0 else 0
                    extra = rows_ref[e, rows, :]
                    q_one = jnp.where(data, q_pair, extra)
                    logits = dot_nt(q_one, kk[e, span, :])
                    peak = jnp.max(logits, axis=1, keepdims=True)
                    terms = jnp.exp(logits - peak)
                    mixed = dot_nn(terms.astype(LOW), vv[e, span, :])
                    total = pltpu.roll(mixed, HD, 1)
                    outs.append(mixed / total)
                    total_one = jnp.max(jnp.where(data, total, 0.0), axis=1, keepdims=True)
                    padded = jnp.max(
                        jnp.where(tile_lane == base + 20, extra.astype(FULL), 0.0), axis=1, keepdims=True
                    )
                    log_total = jnp.where(padded > 0.5, 0.0, -(peak + jnp.log(total_one)))
                    high = log_total.astype(LOW).astype(FULL)
                    middle = (log_total - high).astype(LOW).astype(FULL)
                    low = log_total - high - middle
                    packed = jnp.where(tile_lane == base + 21, high, q_one.astype(FULL))
                    packed = jnp.where(tile_lane == base + 22, middle, packed)
                    packed = jnp.where(tile_lane == base + 23, low, packed)
                    kept_ref[e, rows, :] = packed.astype(LOW)
                joined = jnp.where(tile_lane < HD, outs[0], outs[1])
                out_ref[rows, :] = jnp.where(padded > 0.5, 0.0, joined).astype(LOW)

        return carry

    lax.fori_loop(0, length // TILE, one_tile, 0)


def attend_forward(qkv, rows_extra, keys_extra, where_table):
    length, width = qkv.shape
    pairs = width // (3 * 2 * HD)
    wide = 2 * HD
    return pl.pallas_call(
        attend_forward_kernel,
        out_shape=(
            jax.ShapeDtypeStruct((length, width // 3), LOW),
            jax.ShapeDtypeStruct((2 * pairs, length, wide), LOW),
        ),
        grid_spec=pltpu.PrefetchScalarGridSpec(
            num_scalar_prefetch=1,
            grid=(pairs,),
            in_specs=[
                pl.BlockSpec((length, wide), lambda p, w: (0, p)),
                pl.BlockSpec((length, wide), lambda p, w: (0, pairs + p)),
                pl.BlockSpec((length, wide), lambda p, w: (0, 2 * pairs + p)),
                pl.BlockSpec((2, length, wide), lambda p, w: (0, 0, 0)),
                pl.BlockSpec((2, length, wide), lambda p, w: (p, 0, 0)),
            ],
            out_specs=(
                pl.BlockSpec((length, wide), lambda p, w: (0, p)),
                pl.BlockSpec((2, length, wide), lambda p, w: (p, 0, 0)),
            ),
            scratch_shapes=[pltpu.VMEM((2, length, wide), LOW), pltpu.VMEM((2, length, wide), LOW)],
        ),
        name="attend_forward",
        cost_estimate=pl.CostEstimate(
            flops=8 * pairs * length * length * HD, bytes_accessed=16 * length * width, transcendentals=0
        ),
    )(where_table, qkv, qkv, qkv, rows_extra, keys_extra)


def attend_backward_kernel(
    where_ref, kept_ref, k_ref, v_ref, keys_ref, heads_ref, grads_ref, dq_ref, dk_ref, dv_ref, kk, va, dk_sum, dv_sum
):
    length = k_ref.shape[0]
    lane = lax.broadcasted_iota(jnp.int32, (length, 2 * HD), 1)
    for e in range(2):
        data = (lane < HD) if e == 0 else (lane >= HD)
        base = HD if e == 0 else 0
        kk[e] = jnp.where(data, k_ref[...], keys_ref[e])
        ones = jnp.where((lane == base) | (lane == base + 1), 1.0, 0.0).astype(LOW)
        va[e] = jnp.where(data, v_ref[...], ones)
    dk_sum[...] = jnp.zeros_like(dk_sum)
    dv_sum[...] = jnp.zeros_like(dv_sum)
    tile_lane = lax.broadcasted_iota(jnp.int32, (TILE, 2 * HD), 1)

    def one_tile(t, carry):
        rows = pl.ds(pl.multiple_of(t * TILE, TILE), TILE)
        start = pl.multiple_of(where_ref[0, t] * 128, 128)
        count = where_ref[1, t]
        grads = grads_ref[rows, :]
        both = grads.astype(FULL) * heads_ref[rows, :].astype(FULL)
        for n in range(1, length // TILE + 1):

            @pl.when(count == n)
            def _():
                span = pl.ds(start, n * TILE)
                outs = []
                for e in range(2):
                    data = (tile_lane < HD) if e == 0 else (tile_lane >= HD)
                    base = HD if e == 0 else 0
                    inner = -jnp.sum(jnp.where(data, both, 0.0), axis=1, keepdims=True)
                    high = inner.astype(LOW).astype(FULL)
                    only = jnp.where(data, grads, jnp.zeros_like(grads))
                    packed = jnp.where(tile_lane == base, high, only.astype(FULL))
                    packed = jnp.where(tile_lane == base + 1, inner - high, packed).astype(LOW)
                    q_one = kept_ref[e, rows, :]
                    q_only = jnp.where(data, q_one, jnp.zeros_like(q_one))
                    probs = jnp.exp(dot_nt(kk[e, span, :], q_one))
                    grad_raw = (probs * dot_nt(va[e, span, :], packed)).astype(LOW)
                    dv_sum[span, :] += dot_nn(probs.astype(LOW), only)
                    dk_sum[span, :] += dot_nn(grad_raw, q_only)
                    outs.append(dot_tn(grad_raw, kk[e, span, :]))
                joined = jnp.where(tile_lane < HD, outs[0], outs[1])
                dq_ref[rows, :] = (joined * (1.0 / math.sqrt(HD))).astype(LOW)

        return carry

    lax.fori_loop(0, length // TILE, one_tile, 0)
    dk_ref[...] = dk_sum[...].astype(LOW)
    dv_ref[...] = dv_sum[...].astype(LOW)


def attend_backward(kept, qkv, keys_extra, heads, grads, where_table):
    length, width = qkv.shape
    pairs = width // (3 * 2 * HD)
    wide = 2 * HD
    one = jax.ShapeDtypeStruct((length, width // 3), LOW)
    lanes = pl.BlockSpec((length, wide), lambda p, w: (0, p))
    stacked = pl.BlockSpec((2, length, wide), lambda p, w: (p, 0, 0))
    return pl.pallas_call(
        attend_backward_kernel,
        out_shape=(one, one, one),
        grid_spec=pltpu.PrefetchScalarGridSpec(
            num_scalar_prefetch=1,
            grid=(pairs,),
            in_specs=[
                stacked,
                pl.BlockSpec((length, wide), lambda p, w: (0, pairs + p)),
                pl.BlockSpec((length, wide), lambda p, w: (0, 2 * pairs + p)),
                stacked,
                lanes,
                lanes,
            ],
            out_specs=(lanes, lanes, lanes),
            scratch_shapes=[
                pltpu.VMEM((2, length, wide), LOW),
                pltpu.VMEM((2, length, wide), LOW),
                pltpu.VMEM((length, wide), FULL),
                pltpu.VMEM((length, wide), FULL),
            ],
        ),
        name="attend_backward",
        cost_estimate=pl.CostEstimate(
            flops=20 * pairs * length * length * HD, bytes_accessed=20 * length * width, transcendentals=0
        ),
    )(where_table, kept, qkv, qkv, keys_extra, heads, grads)


def swap_features(part):
    got = swap(part, "core")
    n = got.shape[1] // 4
    return jnp.concatenate((got[:, n : 2 * n], got[:, :n], got[:, 3 * n :], got[:, 2 * n : 3 * n]), axis=1)


def pick(pair, index):
    return lax.dynamic_index_in_dim(pair, index, 0, keepdims=False)


def ordered(own, other, index):
    flip = index == 0
    return jnp.stack((jnp.where(flip, own, other), jnp.where(flip, other, own)))


def plane_gather(block, first_axis, second_axis):
    near = {first_axis: swap(block, first_axis), second_axis: swap(block, second_axis)}
    across = swap(near[first_axis], second_axis)
    return block, near["col"], near["y"], across


def plane_reduce(own, at_col, at_y, across, first_axis, second_axis):
    near = {"col": at_col, "y": at_y}
    arrived = swap(across, first_axis)
    direct = swap(near[first_axis], first_axis)
    onward = (near[second_axis].astype(FULL) + arrived.astype(FULL)).astype(LOW)
    last = swap(onward, second_axis)
    return (own.astype(FULL) + direct.astype(FULL) + last.astype(FULL)).astype(LOW)


def fast_body(
    inputs, gain_first, shift_first, w_query, w_key, w_value, w_output, gain_second, shift_second,
    w_up, bias_up, w_down, bias_down, segments, random_blocks, global_blocks, cotangent,
):
    y_at, core_at, col_at = (lax.axis_index(name) for name in ("y", "core", "col"))
    length = segments.shape[1]
    narrow = inputs.shape[1]
    inputs_pair = inputs.reshape(2, length, narrow)
    cot_pair = cotangent.reshape(2, length, narrow)
    x_own = pick(inputs_pair, y_at)
    x_y = swap(pick(inputs_pair, 1 - y_at), "y")

    def half(weight, axis, index):
        size = weight.shape[axis] // 2
        return lax.dynamic_slice_in_dim(weight, index * size, size, axis)

    def chip_block(weights, axis, join):
        mine = jnp.concatenate([half(w, axis, core_at) for w in weights], axis=axis)
        theirs = swap(jnp.concatenate([half(w, axis, 1 - core_at) for w in weights], axis=axis), "core")
        return jnp.concatenate((mine, theirs), axis=join)

    qkv_block = chip_block((w_query, w_key, w_value), 1, 0)
    qkv_own, qkv_x, qkv_y, qkv_xy = plane_gather(qkv_block, "y", "col")
    x_core, x_ycore = swap(x_own, "core"), swap(x_y, "core")

    vectors = jnp.stack((gain_first, shift_first, gain_second, shift_second, bias_down))
    vectors = jnp.concatenate((vectors, swap(vectors, "core")), axis=1)
    vectors = jnp.concatenate((vectors, swap(vectors, "y")), axis=1)
    gain_one, shift_one, gain_two, shift_two, bias_low = (vectors[i] for i in range(5))
    heads_half = half(random_blocks, 0, core_at)
    hidden_bias = half(bias_up, 0, core_at)
    small = jnp.concatenate((hidden_bias, heads_half.astype(FULL).reshape(-1)))
    small = swap(small, "col")
    hidden_bias_x = small[: hidden_bias.shape[0]]
    heads_half_x = small[hidden_bias.shape[0] :].reshape(heads_half.shape).astype(jnp.int32)
    moves = []
    for y in range(2):
        for core in range(2):
            for col in range(2):
                moves.append(((col * 2 + y) * 2 + core, (y * 2 + core) * 2 + col))
    labels = lax.ppermute(segments, ("y", "core", "col"), moves)[0]
    all_heads = jnp.concatenate((heads_half, heads_half_x), axis=0)
    rows_extra, keys_extra, where_table = attention_extras(labels, all_heads, global_blocks)
    near_heads = heads_half.shape[0]
    live = (labels != 0)[:, None]

    out_block = chip_block((w_output,), 0, 1)
    up_block = chip_block((w_up,), 1, 0)
    down_block = chip_block((w_down,), 0, 1)
    out_own, out_x, out_y, out_xy = plane_gather(out_block, "col", "y")
    up_own, up_x, up_y, up_xy = plane_gather(up_block, "col", "y")
    down_own, down_x, down_y, down_xy = plane_gather(down_block, "y", "col")
    cot_own = pick(cot_pair, y_at)
    cot_y = swap(pick(cot_pair, 1 - y_at), "y")
    cot = jnp.concatenate((cot_own, swap(cot_own, "core"), cot_y, swap(cot_y, "core")), axis=1)

    x_full = jnp.concatenate((x_own, x_core, x_y, x_ycore), axis=1).astype(FULL)

    def norm_stats(moving):
        center = jnp.mean(moving, axis=1, keepdims=True)
        spread = jnp.mean(moving * moving, axis=1, keepdims=True) - center * center
        return center, lax.rsqrt(spread + EPS)

    center_one, inverse_one = norm_stats(x_full)
    normed_one = (x_full - center_one) * inverse_one
    first = (normed_one * gain_one + shift_one).astype(LOW)

    w_qkv = (jnp.concatenate((qkv_own, qkv_y), axis=0), jnp.concatenate((qkv_x, qkv_xy), axis=0))
    qkv = [dot_nn(first, w).astype(LOW) for w in w_qkv]
    keys_of = (keys_extra[:near_heads], keys_extra[near_heads:])
    heads, kept = zip(*[attend_forward(qkv[i], rows_extra, keys_of[i], where_table) for i in range(2)])
    w_out = (jnp.concatenate((out_own, out_y), axis=1), jnp.concatenate((out_x, out_xy), axis=1))
    mixed_part = (dot_nn(heads[0], w_out[0]) + dot_nn(heads[1], w_out[1])).astype(LOW)
    mixed = mixed_part.astype(FULL) + swap_features(mixed_part).astype(FULL)
    residual = x_full + mixed
    center_two, inverse_two = norm_stats(residual)
    normed_two = (residual - center_two) * inverse_two
    second = (normed_two * gain_two + shift_two).astype(LOW)

    w_ups = (jnp.concatenate((up_own, up_y), axis=0), jnp.concatenate((up_x, up_xy), axis=0))
    w_downs = (jnp.concatenate((down_own, down_y), axis=1), jnp.concatenate((down_x, down_xy), axis=1))
    biases = (hidden_bias, hidden_bias_x)
    low_part, second_part = 0.0, 0.0
    up_grads, down_grads, bias_grads = [], [], []
    for i in range(2):
        upward = dot_nn(second, w_ups[i]) + biases[i]
        activated, pull_back = jax.vjp(gelu_tanh, upward)
        hidden = activated.astype(LOW)
        grad_upward = pull_back(dot_nt(cot, w_downs[i]))[0].astype(LOW)
        low_part = low_part + dot_nn(hidden, w_downs[i])
        second_part = second_part + dot_nt(grad_upward, w_ups[i])
        up_grads.append(dot_tn(second, grad_upward).astype(LOW))
        down_grads.append(dot_tn(hidden, cot).astype(LOW))
        bias_grads.append(jnp.sum(grad_upward, axis=0, dtype=FULL))

    def own_columns(part):
        low = part.astype(LOW)
        n = narrow
        mine = jnp.concatenate((low[:, :n], low[:, 2 * n : 3 * n]), axis=1)
        theirs = swap(jnp.concatenate((low[:, n : 2 * n], low[:, 3 * n :]), axis=1), "core")
        return mine.astype(FULL) + theirs.astype(FULL)

    def mine_of(array):
        return jnp.concatenate((array[..., :narrow], array[..., 2 * narrow : 3 * narrow]), axis=-1)

    low_own = mine_of(residual) + own_columns(low_part) + mine_of(bias_low)

    def to_shard(columns, dtype):
        back = swap(columns[:, narrow:].astype(LOW), "y")
        return ordered(columns[:, :narrow].astype(dtype), back.astype(dtype), y_at).reshape(2 * length, narrow)

    layer_out = to_shard(low_own, LOW)

    second_low = second_part.astype(LOW)
    grad_second = second_low.astype(FULL) + swap_features(second_low).astype(FULL)
    scaled = grad_second * gain_two
    mean_one = jnp.mean(scaled, axis=1, keepdims=True)
    mean_two = jnp.mean(scaled * normed_two, axis=1, keepdims=True)
    grad_residual = cot.astype(FULL) + inverse_two * (scaled - mean_one - normed_two * mean_two)
    grad_gain_two = jnp.sum(mine_of(grad_second * normed_two), axis=0)
    grad_shift_two = jnp.sum(mine_of(grad_second), axis=0)
    grad_mixed = grad_residual.astype(LOW)
    grads = [jnp.where(live, dot_nt(grad_mixed, w), 0.0).astype(LOW) for w in w_out]
    out_grads = [dot_tn(heads[i], grad_mixed).astype(LOW) for i in range(2)]
    qkv_grads, first_part = [], 0.0
    for i in range(2):
        pieces = attend_backward(kept[i], qkv[i], keys_of[i], heads[i], grads[i], where_table)
        joined = jnp.concatenate(pieces, axis=1)
        qkv_grads.append(dot_tn(first, joined).astype(LOW))
        first_part = first_part + dot_nt(joined, w_qkv[i])
    scaled_part = first_part * gain_one
    sums = jnp.stack((jnp.sum(scaled_part, axis=1), jnp.sum(scaled_part * normed_one, axis=1)))
    sums = (sums + swap(sums, "core")) / (4 * narrow)
    grad_first = own_columns(first_part)
    normed_mine = mine_of(normed_one)
    grad_x = inverse_one * (grad_first * mine_of(gain_one) - sums[0][:, None] - normed_mine * sums[1][:, None])
    grad_inputs = to_shard(mine_of(grad_residual) + grad_x, FULL)
    grad_gain_one = jnp.sum(grad_first * normed_mine, axis=0)
    grad_shift_one = jnp.sum(grad_first, axis=0)

    gains = jnp.stack((grad_gain_one, grad_shift_one, grad_gain_two, grad_shift_two)).reshape(4, 2, narrow)
    down_bias = jnp.sum(cotangent, axis=0, dtype=FULL)
    gains = jnp.stack([ordered(gains[i, 0], gains[i, 1], y_at) for i in range(4)])
    bias_pair = ordered(down_bias, jnp.zeros_like(down_bias), y_at)
    gains = jnp.concatenate((gains, bias_pair[None]), axis=0)
    gains = jnp.stack((jnp.where(core_at == 0, gains, 0.0), jnp.where(core_at == 0, 0.0, gains)))
    ups = ordered(bias_grads[0], bias_grads[1], col_at)
    ups = jnp.stack((jnp.where(core_at == 0, ups, 0.0), jnp.where(core_at == 0, 0.0, ups)), axis=1)
    flat = lax.psum(jnp.concatenate((gains.reshape(-1), ups.reshape(-1))), ("dp", "y", "core", "col"))
    gains = flat[: gains.size].reshape(gains.shape)
    gains = pick(pick(gains, core_at).swapaxes(0, 1), y_at)
    grad_up_bias = pick(flat[gains.size * 4 :].reshape(2, -1), col_at)

    h = narrow * 2

    def finish(total, axis):
        total = lax.psum(total, "dp")
        size = total.shape[axis] // 2
        keep = lax.slice_in_dim(total, 0, size, axis=axis)
        got = swap(lax.slice_in_dim(total, size, 2 * size, axis=axis), "core")
        return keep, got

    def reduce_rows(pair, order):
        return plane_reduce(pair[0][:h], pair[1][:h], pair[0][h:], pair[1][h:], *order)

    def reduce_columns(pair, order):
        return plane_reduce(pair[0][:, :h], pair[1][:, :h], pair[0][:, h:], pair[1][:, h:], *order)

    def across_cores(keep, got, parts, axis):
        out = []
        size = keep.shape[axis] // parts
        for i in range(parts):
            a = lax.slice_in_dim(keep, i * size, (i + 1) * size, axis=axis)
            b = lax.slice_in_dim(got, i * size, (i + 1) * size, axis=axis)
            flip = core_at == 0
            out.append(jnp.concatenate((jnp.where(flip, a, b), jnp.where(flip, b, a)), axis=axis).astype(FULL))
        return out

    (grad_down,) = across_cores(*finish(reduce_columns(down_grads, ("y", "col")), 1), 1, 0)
    (grad_up,) = across_cores(*finish(reduce_rows(up_grads, ("col", "y")), 0), 1, 1)
    (grad_out,) = across_cores(*finish(reduce_columns(out_grads, ("y", "col")), 1), 1, 0)
    grad_qkv = across_cores(*finish(reduce_rows(qkv_grads, ("col", "y")), 0), 3, 1)
    return (
        layer_out, grad_inputs, gains[0], gains[1], *grad_qkv, grad_out, gains[2], gains[3],
        grad_up, grad_up_bias, grad_down, gains[4],
    )


def whole_sequences(mesh):
    return mesh.shape["row"] == 4 and mesh.shape["col"] == 2


def placements(row):
    tokens = P(("dp", "col"), row)
    rows = P(row)
    weight = P(row, "col")
    turned = P("col", row)
    placed = (
        tokens, rows, rows, weight, weight, weight, turned, rows, rows, weight, P("col"), turned, rows,
        P(("dp", *row), None), P("col", None, None), P(), tokens,
    )
    given = (
        tokens, tokens, rows, rows, weight, weight, weight, turned, rows, rows, weight, P("col"), turned, rows,
    )
    return placed, given


def solution(mesh):
    sizes = mesh.shape
    split = jax.sharding.Mesh(
        mesh.devices.reshape(sizes["dp"], sizes["row"] // 2, 2, sizes["col"]), ("dp", "y", "core", "col")
    )

    def run(*arrays):
        tokens, length = arrays[0].shape[0], arrays[13].shape[1]
        if whole_sequences(mesh) and tokens == sizes["dp"] * sizes["col"] * 2 * length:
            placed, given = placements(("y", "core"))
            step = jax.shard_map(fast_body, mesh=split, in_specs=placed, out_specs=given, check_vma=False)
        else:
            placed, given = placements(("row",))
            step = jax.shard_map(body, mesh=mesh, in_specs=placed, out_specs=given, check_vma=False)
        return step(*arrays)

    return run
```

```python
import math

import jax
import jax.numpy as jnp
from jax import lax
from jax.experimental import pallas as pl
from jax.experimental.pallas import tpu as pltpu
from jax.sharding import PartitionSpec as P

D = 1024
HD = 64
BLK = 64
NB = 16


EPS = 1e-05


def product(picked, weight, flipped):
    if flipped:
        return lax.dot_general(
            picked, weight, (((1,), (1,)), ((), ())), preferred_element_type=jnp.float32
        )
    return jnp.dot(picked, weight, preferred_element_type=jnp.float32)


def to_columns(moving, weight, flipped):
    gathered = lax.all_gather(moving, "col", axis=0, tiled=True)
    row_count = gathered.shape[0] // lax.axis_size("row")

    def term_rows(first_row, how_many):
        return product(gathered, weight, flipped)

    result = lax.psum_scatter(
        term_rows(jnp.int32(0), lax.axis_size("row") * row_count),
        "row",
        scatter_dimension=0,
        tiled=True,
    )
    return (result, gathered)


def to_rows(moving, weight, flipped):
    gathered = lax.all_gather(moving, "row", axis=0, tiled=True)
    row_count = gathered.shape[0] // lax.axis_size("col")

    def term_rows(first_row, how_many):
        return product(gathered, weight, flipped)

    return (
        lax.psum_scatter(
            term_rows(jnp.int32(0), lax.axis_size("col") * row_count),
            "col",
            scatter_dimension=0,
            tiled=True,
        ),
        gathered,
    )


def norm_sums(first_sum, second_sum):
    return lax.psum((first_sum, second_sum), "row")


def norm_forward(moving, gain_row, shift_row):
    totals, squares = norm_sums(jnp.sum(moving, axis=1), jnp.sum(moving * moving, axis=1))
    center = totals / D
    spread = squares / D - center * center
    inverse = lax.rsqrt(spread + EPS)
    normed = (moving - center[:, None]) * inverse[:, None]
    return (normed * gain_row + shift_row, normed, inverse)


def norm_backward(upstream, normed, inverse, gain_row):
    scaled = upstream * gain_row
    first_sum, second_sum = norm_sums(jnp.sum(scaled, axis=1), jnp.sum(scaled * normed, axis=1))
    return inverse[:, None] * (scaled - first_sum[:, None] / D - normed * (second_sum[:, None] / D))


def head_masks(random_blocks, global_blocks):
    block_ids = jnp.arange(NB, dtype=jnp.int32)
    nearby = jnp.abs(block_ids[:, None] - block_ids[None, :]) <= 1
    chosen = jnp.any(random_blocks[:, :, :, None] == block_ids[None, None, None, :], axis=2)
    marked = jnp.any(global_blocks[:, None] == block_ids[None, :], axis=0)
    block_table = nearby[None] | chosen | marked[None, None, :] | marked[None, :, None]
    return jnp.repeat(jnp.repeat(block_table, BLK, axis=1), BLK, axis=2)


def seq_logits(seq_queries, seq_keys, labels, pattern):
    same_doc = (labels[:, None] == labels[None, :]) & (labels[None, :] != 0)
    raw_scores = jnp.einsum(
        "qhd,khd->hqk", seq_queries, seq_keys, preferred_element_type=jnp.float32
    )
    return jnp.where(pattern & same_doc[None], raw_scores * (1.0 / math.sqrt(HD)), -1000000000.0)


def attend_plain(queries, key_block, value_block, segments, pattern):

    def one_seq(pieces):
        seq_queries, seq_keys, seq_values, labels = pieces
        logits = seq_logits(seq_queries, seq_keys, labels, pattern)
        row_peak = jnp.max(logits, axis=2, keepdims=True)
        exp_terms = jnp.exp(logits - row_peak)
        row_total = jnp.sum(exp_terms, axis=2, keepdims=True)
        softmax = (exp_terms / row_total).astype(jnp.bfloat16)
        attended = jnp.einsum(
            "hqk,khd->qhd", softmax, seq_values, preferred_element_type=jnp.float32
        )
        live_rows = (labels != 0).astype(jnp.float32)
        return (attended * live_rows[:, None, None], (row_peak + jnp.log(row_total))[:, :, 0])

    return lax.map(one_seq, (queries, key_block, value_block, segments))


def attend_plain_backward(queries, key_block, value_block, segments, pattern, grad_heads, log_total):

    def one_seq(pieces):
        seq_queries, seq_keys, seq_values, labels, seq_grads, seq_log = pieces
        logits = seq_logits(seq_queries, seq_keys, labels, pattern)
        softmax = jnp.exp(logits - seq_log[:, :, None])
        grad_probs = jnp.einsum(
            "qhd,khd->hqk", seq_grads, seq_values, preferred_element_type=jnp.float32
        )
        grad_values = jnp.einsum(
            "hqk,qhd->khd",
            softmax.astype(jnp.bfloat16),
            seq_grads,
            preferred_element_type=jnp.float32,
        )
        inner_sum = jnp.sum(softmax * grad_probs, axis=2, keepdims=True)
        grad_raw = (softmax * (grad_probs - inner_sum) * (1.0 / math.sqrt(HD))).astype(jnp.bfloat16)
        grad_queries = jnp.einsum(
            "hqk,khd->qhd", grad_raw, seq_keys, preferred_element_type=jnp.float32
        )
        grad_keys = jnp.einsum(
            "hqk,qhd->khd", grad_raw, seq_queries, preferred_element_type=jnp.float32
        )
        return (grad_queries, grad_keys, grad_values)

    return lax.map(one_seq, (queries, key_block, value_block, segments, grad_heads, log_total))


def gelu_tanh(values):
    return jax.nn.gelu(values, approximate=True)


def weight_grad(left, right):
    return lax.dot_general(
        left, right, (((0,), (0,)), ((), ())), preferred_element_type=jnp.float32
    )


def body(
    inputs,
    gain_first,
    shift_first,
    w_query,
    w_key,
    w_value,
    w_output,
    gain_second,
    shift_second,
    w_up,
    bias_up,
    w_down,
    bias_down,
    segments,
    random_blocks,
    global_blocks,
    cotangent,
):
    seq_count, seq_len = segments.shape
    head_width = w_query.shape[1]
    heads_here = random_blocks.shape[0]
    seq_shape = (seq_count, seq_len, heads_here, HD)
    pattern = head_masks(random_blocks, global_blocks)
    live_tokens = (segments != 0).reshape(-1)
    x_first = inputs.astype(jnp.float32)
    first_full, normed_one, inverse_one = norm_forward(x_first, gain_first, shift_first)
    first_low = first_full.astype(jnp.bfloat16)
    stacked = jnp.concatenate((w_query, w_key, w_value), axis=1)
    projected, first_all = to_columns(first_low, stacked, False)
    proj_low = projected.astype(jnp.bfloat16)
    queries = proj_low[:, :head_width].reshape(seq_shape)
    key_block = proj_low[:, head_width : 2 * head_width].reshape(seq_shape)
    value_block = proj_low[:, 2 * head_width :].reshape(seq_shape)
    heads_out, log_total = attend_plain(queries, key_block, value_block, segments, pattern)
    heads_low = heads_out.reshape(-1, head_width).astype(jnp.bfloat16)
    mixed_out, heads_all = to_rows(heads_low, w_output, False)
    residual = x_first + mixed_out
    second_full, normed_two, inverse_two = norm_forward(residual, gain_second, shift_second)
    second_low = second_full.astype(jnp.bfloat16)
    upward, second_all = to_columns(second_low, w_up, False)
    upward = upward + bias_up
    hidden_low = gelu_tanh(upward).astype(jnp.bfloat16)
    downward, hidden_all = to_rows(hidden_low, w_down, False)
    layer_out = (residual + (downward + bias_down)).astype(jnp.bfloat16)
    grad_hidden, cotangent_all = to_columns(cotangent, w_down, True)
    activated, pull_back = jax.vjp(gelu_tanh, upward)
    grad_upward = pull_back(grad_hidden)[0].astype(jnp.bfloat16)
    grad_second, grad_upward_all = to_rows(grad_upward, w_up, True)
    grad_residual = cotangent.astype(jnp.float32) + norm_backward(
        grad_second, normed_two, inverse_two, gain_second
    )
    grad_mixed = grad_residual.astype(jnp.bfloat16)
    grad_heads, grad_mixed_all = to_columns(grad_mixed, w_output, True)
    grad_heads = jnp.where(live_tokens[:, None], grad_heads, 0.0).astype(jnp.bfloat16)
    grad_queries, grad_keys, grad_values = attend_plain_backward(
        queries, key_block, value_block, segments, pattern, grad_heads.reshape(seq_shape), log_total
    )
    grad_proj = jnp.concatenate(
        (
            grad_queries.reshape(-1, head_width),
            grad_keys.reshape(-1, head_width),
            grad_values.reshape(-1, head_width),
        ),
        axis=1,
    ).astype(jnp.bfloat16)
    grad_first, grad_proj_all = to_rows(grad_proj, stacked, True)
    grad_inputs = grad_residual + norm_backward(grad_first, normed_one, inverse_one, gain_first)
    grad_stacked = weight_grad(first_all, grad_proj_all)
    grad_out_weight = weight_grad(heads_all, grad_mixed_all)
    grad_up_weight = weight_grad(second_all, grad_upward_all)
    grad_down_weight = weight_grad(hidden_all, cotangent_all)
    grad_up_bias = jnp.sum(grad_upward_all, axis=0, dtype=jnp.float32)
    grad_down_bias = jnp.sum(cotangent_all, axis=0, dtype=jnp.float32)
    gain_terms = lax.psum(
        (
            jnp.sum(grad_first * normed_one, axis=0),
            jnp.sum(grad_first, axis=0),
            jnp.sum(grad_second * normed_two, axis=0),
            jnp.sum(grad_second, axis=0),
        ),
        ("dp", "col"),
    )
    summed = (
        lax.psum(grad_stacked.astype(jnp.bfloat16), "dp").astype(jnp.float32),
        lax.psum(grad_out_weight.astype(jnp.bfloat16), "dp").astype(jnp.float32),
        lax.psum(grad_up_weight.astype(jnp.bfloat16), "dp").astype(jnp.float32),
        lax.psum(grad_down_weight.astype(jnp.bfloat16), "dp").astype(jnp.float32),
        lax.psum(grad_up_bias.astype(jnp.bfloat16), "dp").astype(jnp.float32),
        lax.psum(grad_down_bias.astype(jnp.bfloat16), "dp").astype(jnp.float32),
    )
    return (
        layer_out,
        grad_inputs,
        gain_terms[0],
        gain_terms[1],
        summed[0][:, :head_width],
        summed[0][:, head_width : 2 * head_width],
        summed[0][:, 2 * head_width :],
        summed[1],
        gain_terms[2],
        gain_terms[3],
        summed[2],
        summed[4],
        summed[3],
        summed[5],
    )


SWAP = [(0, 1), (1, 0)]
LOW = jnp.bfloat16
FULL = jnp.float32
TILE = 256
BIG = 1e30


def swap(array, axis):
    return lax.ppermute(array, axis, SWAP)


def dot_nn(left, right):
    return lax.dot_general(left, right, (((1,), (0,)), ((), ())), preferred_element_type=FULL)


def dot_nt(left, right):
    return lax.dot_general(left, right, (((1,), (1,)), ((), ())), preferred_element_type=FULL)


def dot_tn(left, right):
    return lax.dot_general(left, right, (((0,), (0,)), ((), ())), preferred_element_type=FULL)


def attention_extras(labels, random_blocks, global_blocks):
    length = labels.shape[0]
    blocks = length // BLK
    block_ids = jnp.arange(blocks, dtype=jnp.int32)
    nearby = jnp.abs(block_ids[:, None] - block_ids[None, :]) <= 1
    chosen = jnp.any(random_blocks[:, :, :, None] == block_ids[None, None, None, :], axis=2)
    marked = jnp.any(global_blocks[:, None] == block_ids[None, :], axis=0)
    table = nearby[None] | chosen | marked[None, None, :] | marked[None, :, None]
    heads = table.shape[0]
    lane = jnp.arange(HD, dtype=jnp.int32)
    place = jnp.arange(length, dtype=jnp.int32) // BLK
    doc_lane = blocks + jnp.where(labels == 0, 4, labels - 1)
    row_extra = ((lane[None, :] == place[:, None]) | (lane[None, :] == doc_lane[:, None])).astype(LOW)
    table_keys = jnp.pad(jnp.swapaxes(table, 1, 2), ((0, 0), (0, 0), (0, HD - blocks)), constant_values=True)
    table_keys = jnp.repeat(table_keys, BLK, axis=1)
    is_doc = (lane >= blocks) & (lane <= blocks + 4)
    doc_bad = is_doc[None, :] & (lane[None, :] != doc_lane[:, None])
    doc_bad = doc_bad | (lane[None, :] == blocks + 4)
    key_extra = jnp.where(table_keys & ~doc_bad[None], 0.0, -BIG)
    key_extra = jnp.where((lane >= blocks + 5) & (lane <= blocks + 7), 1.0, key_extra).astype(LOW)
    rows = jnp.stack((jnp.pad(row_extra, ((0, 0), (HD, 0))), jnp.pad(row_extra, ((0, 0), (0, HD)))))
    even = jnp.pad(key_extra[0::2], ((0, 0), (0, 0), (HD, 0)))
    odd = jnp.pad(key_extra[1::2], ((0, 0), (0, 0), (0, HD)))
    keys = jnp.stack((even, odd), axis=1).reshape(heads, length, 2 * HD)
    tiles = length // TILE
    known = labels[None, :] == jnp.arange(1, 5, dtype=jnp.int32)[:, None]
    present = jnp.any(known.reshape(4, tiles, TILE), axis=2)
    wanted = jnp.any(present[:, :, None] & known[:, None, :], axis=0)
    spots = jnp.arange(length, dtype=jnp.int32)
    first = jnp.min(jnp.where(wanted, spots[None, :], length - 1), axis=1)
    last = jnp.max(jnp.where(wanted, spots[None, :], 0), axis=1)
    start = first // 128
    count = jnp.maximum((last + 1 - start * 128 + 255) // 256, 1)
    start = jnp.minimum(start, length // 128 - 2 * count)
    return rows, keys, jnp.stack((start, count)).astype(jnp.int32)


def attend_forward_kernel(where_ref, q_ref, k_ref, v_ref, rows_ref, keys_ref, out_ref, kept_ref, kk, vv):
    length = q_ref.shape[0]
    lane = lax.broadcasted_iota(jnp.int32, (length, 2 * HD), 1)
    for e in range(2):
        data = (lane < HD) if e == 0 else (lane >= HD)
        kk[e] = jnp.where(data, k_ref[...], keys_ref[e])
        vv[e] = jnp.where(data, v_ref[...], jnp.ones_like(v_ref[...]))
    tile_lane = lax.broadcasted_iota(jnp.int32, (TILE, 2 * HD), 1)

    def one_tile(t, carry):
        rows = pl.ds(pl.multiple_of(t * TILE, TILE), TILE)
        start = pl.multiple_of(where_ref[0, t] * 128, 128)
        count = where_ref[1, t]
        q_pair = q_ref[rows, :] * jnp.bfloat16(1.0 / math.sqrt(HD))
        for n in range(1, length // TILE + 1):

            @pl.when(count == n)
            def _():
                span = pl.ds(start, n * TILE)
                outs = []
                for e in range(2):
                    data = (tile_lane < HD) if e == 0 else (tile_lane >= HD)
                    base = HD if e == 0 else 0
                    extra = rows_ref[e, rows, :]
                    q_one = jnp.where(data, q_pair, extra)
                    logits = dot_nt(q_one, kk[e, span, :])
                    peak = jnp.max(logits, axis=1, keepdims=True)
                    terms = jnp.exp(logits - peak)
                    mixed = dot_nn(terms.astype(LOW), vv[e, span, :])
                    total = pltpu.roll(mixed, HD, 1)
                    outs.append(mixed / total)
                    total_one = jnp.max(jnp.where(data, total, 0.0), axis=1, keepdims=True)
                    padded = jnp.max(
                        jnp.where(tile_lane == base + 20, extra.astype(FULL), 0.0), axis=1, keepdims=True
                    )
                    log_total = jnp.where(padded > 0.5, 0.0, -(peak + jnp.log(total_one)))
                    high = log_total.astype(LOW).astype(FULL)
                    middle = (log_total - high).astype(LOW).astype(FULL)
                    low = log_total - high - middle
                    packed = jnp.where(tile_lane == base + 21, high, q_one.astype(FULL))
                    packed = jnp.where(tile_lane == base + 22, middle, packed)
                    packed = jnp.where(tile_lane == base + 23, low, packed)
                    kept_ref[e, rows, :] = packed.astype(LOW)
                joined = jnp.where(tile_lane < HD, outs[0], outs[1])
                out_ref[rows, :] = jnp.where(padded > 0.5, 0.0, joined).astype(LOW)

        return carry

    lax.fori_loop(0, length // TILE, one_tile, 0)


def attend_forward(qkv, rows_extra, keys_extra, where_table):
    length, width = qkv.shape
    pairs = width // (3 * 2 * HD)
    wide = 2 * HD
    return pl.pallas_call(
        attend_forward_kernel,
        out_shape=(
            jax.ShapeDtypeStruct((length, width // 3), LOW),
            jax.ShapeDtypeStruct((2 * pairs, length, wide), LOW),
        ),
        grid_spec=pltpu.PrefetchScalarGridSpec(
            num_scalar_prefetch=1,
            grid=(pairs,),
            in_specs=[
                pl.BlockSpec((length, wide), lambda p, w: (0, p)),
                pl.BlockSpec((length, wide), lambda p, w: (0, pairs + p)),
                pl.BlockSpec((length, wide), lambda p, w: (0, 2 * pairs + p)),
                pl.BlockSpec((2, length, wide), lambda p, w: (0, 0, 0)),
                pl.BlockSpec((2, length, wide), lambda p, w: (p, 0, 0)),
            ],
            out_specs=(
                pl.BlockSpec((length, wide), lambda p, w: (0, p)),
                pl.BlockSpec((2, length, wide), lambda p, w: (p, 0, 0)),
            ),
            scratch_shapes=[pltpu.VMEM((2, length, wide), LOW), pltpu.VMEM((2, length, wide), LOW)],
        ),
        name="attend_forward",
        cost_estimate=pl.CostEstimate(
            flops=8 * pairs * length * length * HD, bytes_accessed=16 * length * width, transcendentals=0
        ),
    )(where_table, qkv, qkv, qkv, rows_extra, keys_extra)


def attend_backward_kernel(
    where_ref, kept_ref, k_ref, v_ref, keys_ref, heads_ref, grads_ref, out_ref, kk, va, dk_sum, dv_sum
):
    length = k_ref.shape[0]
    wide = 2 * HD
    third = out_ref.shape[1] // 3
    pair = pl.program_id(0) * wide
    lane = lax.broadcasted_iota(jnp.int32, (length, wide), 1)
    for e in range(2):
        data = (lane < HD) if e == 0 else (lane >= HD)
        base = HD if e == 0 else 0
        kk[e] = jnp.where(data, k_ref[...], keys_ref[e])
        ones = jnp.where((lane == base) | (lane == base + 1), 1.0, 0.0).astype(LOW)
        va[e] = jnp.where(data, v_ref[...], ones)
    dk_sum[...] = jnp.zeros_like(dk_sum)
    dv_sum[...] = jnp.zeros_like(dv_sum)
    tile_lane = lax.broadcasted_iota(jnp.int32, (TILE, wide), 1)

    def one_tile(t, carry):
        rows = pl.ds(pl.multiple_of(t * TILE, TILE), TILE)
        start = pl.multiple_of(where_ref[0, t] * 128, 128)
        count = where_ref[1, t]
        grads = grads_ref[rows, :]
        both = grads.astype(FULL) * heads_ref[rows, :].astype(FULL)
        for n in range(1, length // TILE + 1):

            @pl.when(count == n)
            def _():
                span = pl.ds(start, n * TILE)
                outs = []
                for e in range(2):
                    data = (tile_lane < HD) if e == 0 else (tile_lane >= HD)
                    base = HD if e == 0 else 0
                    inner = -jnp.sum(jnp.where(data, both, 0.0), axis=1, keepdims=True)
                    high = inner.astype(LOW).astype(FULL)
                    only = jnp.where(data, grads, jnp.zeros_like(grads))
                    packed = jnp.where(tile_lane == base, high, only.astype(FULL))
                    packed = jnp.where(tile_lane == base + 1, inner - high, packed).astype(LOW)
                    q_one = kept_ref[e, rows, :]
                    q_only = jnp.where(data, q_one, jnp.zeros_like(q_one))
                    probs = jnp.exp(dot_nt(kk[e, span, :], q_one))
                    grad_raw = (probs * dot_nt(va[e, span, :], packed)).astype(LOW)
                    dv_sum[span, :] += dot_nn(probs.astype(LOW), only)
                    dk_sum[span, :] += dot_nn(grad_raw, q_only)
                    outs.append(dot_tn(grad_raw, kk[e, span, :]))
                joined = jnp.where(tile_lane < HD, outs[0], outs[1])
                lanes = pl.ds(pl.multiple_of(pair, wide), wide)
                out_ref[rows, lanes] = (joined * (1.0 / math.sqrt(HD))).astype(LOW)

        return carry

    lax.fori_loop(0, length // TILE, one_tile, 0)
    out_ref[:, pl.ds(pl.multiple_of(third + pair, wide), wide)] = dk_sum[...].astype(LOW)
    out_ref[:, pl.ds(pl.multiple_of(2 * third + pair, wide), wide)] = dv_sum[...].astype(LOW)


def attend_backward(kept, qkv, keys_extra, heads, grads, group, where_table):
    length, width = qkv.shape
    pairs = width // (3 * 2 * HD)
    wide = 2 * HD
    stacked = pl.BlockSpec((2, length, wide), lambda p, w: (p, 0, 0))
    return pl.pallas_call(
        attend_backward_kernel,
        out_shape=jax.ShapeDtypeStruct((length, width), LOW),
        grid_spec=pltpu.PrefetchScalarGridSpec(
            num_scalar_prefetch=1,
            grid=(pairs,),
            in_specs=[
                stacked,
                pl.BlockSpec((length, wide), lambda p, w: (0, pairs + p)),
                pl.BlockSpec((length, wide), lambda p, w: (0, 2 * pairs + p)),
                stacked,
                pl.BlockSpec((length, wide), lambda p, w: (0, p)),
                pl.BlockSpec((length, wide), lambda p, w: (0, group * pairs + p)),
            ],
            out_specs=pl.BlockSpec((length, width), lambda p, w: (0, 0)),
            scratch_shapes=[
                pltpu.VMEM((2, length, wide), LOW),
                pltpu.VMEM((2, length, wide), LOW),
                pltpu.VMEM((length, wide), FULL),
                pltpu.VMEM((length, wide), FULL),
            ],
        ),
        name="attend_backward",
        cost_estimate=pl.CostEstimate(
            flops=20 * pairs * length * length * HD, bytes_accessed=20 * length * width, transcendentals=0
        ),
    )(where_table, kept, qkv, qkv, keys_extra, heads, grads)


def row_tiles(count):
    def spec(width):
        return pl.BlockSpec((TILE, width), lambda t: (t, 0))

    return spec


def whole(shape):
    return pl.BlockSpec(shape, lambda t: (0,) * len(shape))


def cost(flops, moved):
    return pl.CostEstimate(flops=int(flops), bytes_accessed=int(moved), transcendentals=0)


def norm_parts(blocks):
    width = sum(b.shape[1] for b in blocks)
    total = sum(jnp.sum(b, axis=1, keepdims=True) for b in blocks)
    squares = sum(jnp.sum(b * b, axis=1, keepdims=True) for b in blocks)
    center = total / width
    return center, lax.rsqrt(squares / width - center * center + EPS)


def columns(ref, index, width):
    return ref[:, index * width : (index + 1) * width]


def first_norm_kernel(x0, x1, x2, x3, gain_ref, shift_ref, low_ref, high_ref):
    blocks = [x[...].astype(FULL) for x in (x0, x1, x2, x3)]
    n = blocks[0].shape[1]
    center, inverse = norm_parts(blocks)
    for i, block in enumerate(blocks):
        value = (block - center) * inverse * columns(gain_ref, i, n) + columns(shift_ref, i, n)
        (low_ref, high_ref)[i // 2][:, (i % 2) * n : (i % 2 + 1) * n] = value.astype(LOW)


def first_norm(blocks, gain, shift):
    length, n = blocks[0].shape
    rows = row_tiles(length)
    half = jax.ShapeDtypeStruct((length, 2 * n), LOW)
    return pl.pallas_call(
        first_norm_kernel,
        out_shape=(half, half),
        grid=(length // TILE,),
        in_specs=[rows(n)] * 4 + [whole((1, 4 * n))] * 2,
        out_specs=(rows(2 * n), rows(2 * n)),
        name="first_norm",
        cost_estimate=cost(20 * length * n, 16 * length * n),
    )(*blocks, gain, shift)


def second_norm_kernel(x0, x1, x2, x3, part_ref, got_ref, gain_ref, shift_ref, residual_ref, low_ref, high_ref):
    n = x0.shape[1]
    blocks = []
    for i, x in enumerate((x0, x1, x2, x3)):
        mixed = columns(part_ref, i, n).astype(FULL) + columns(got_ref, i ^ 1, n).astype(FULL)
        blocks.append(x[...].astype(FULL) + mixed)
    center, inverse = norm_parts(blocks)
    for i, block in enumerate(blocks):
        residual_ref[:, i * n : (i + 1) * n] = block
        value = (block - center) * inverse * columns(gain_ref, i, n) + columns(shift_ref, i, n)
        (low_ref, high_ref)[i // 2][:, (i % 2) * n : (i % 2 + 1) * n] = value.astype(LOW)


def second_norm(blocks, part, got, gain, shift):
    length, n = blocks[0].shape
    rows = row_tiles(length)
    half = jax.ShapeDtypeStruct((length, 2 * n), LOW)
    return pl.pallas_call(
        second_norm_kernel,
        out_shape=(jax.ShapeDtypeStruct((length, 4 * n), FULL), half, half),
        grid=(length // TILE,),
        in_specs=[rows(n)] * 4 + [rows(4 * n)] * 2 + [whole((1, 4 * n))] * 2,
        out_specs=(rows(4 * n), rows(2 * n), rows(2 * n)),
        name="second_norm",
        cost_estimate=cost(30 * length * n, 48 * length * n),
    )(*blocks, part, got, gain, shift)


def norm_gradient(blocks, part_ref, got_ref, gain_ref, sums_ref):
    n = blocks[0].shape[1]
    center, inverse = norm_parts(blocks)
    normed = [(b - center) * inverse for b in blocks]
    grads = [columns(part_ref, i, n).astype(FULL) + columns(got_ref, i ^ 1, n).astype(FULL) for i in range(4)]
    scaled = [g * columns(gain_ref, i, n) for i, g in enumerate(grads)]
    mean_one = sum(jnp.sum(s, axis=1, keepdims=True) for s in scaled) / (4 * n)
    mean_two = sum(jnp.sum(s * z, axis=1, keepdims=True) for s, z in zip(scaled, normed)) / (4 * n)

    @pl.when(pl.program_id(0) == 0)
    def _():
        sums_ref[...] = jnp.zeros_like(sums_ref)

    for slot, i in enumerate((0, 2)):
        place = slice(slot * n, (slot + 1) * n)
        sums_ref[0:1, place] += jnp.sum(grads[i] * normed[i], axis=0, keepdims=True)
        sums_ref[1:2, place] += jnp.sum(grads[i], axis=0, keepdims=True)
    return [inverse * (s - mean_one - z * mean_two) for s, z in zip(scaled, normed)]


def second_norm_back_kernel(
    residual_ref, part_ref, got_ref, low_ref, high_ref, gain_ref, own_ref, other_ref, mixed_ref, sums_ref
):
    n = residual_ref.shape[1] // 4
    blocks = [columns(residual_ref, i, n) for i in range(4)]
    for i, grad in enumerate(norm_gradient(blocks, part_ref, got_ref, gain_ref, sums_ref)):
        total = columns((low_ref, high_ref)[i // 2], i % 2, n).astype(FULL) + grad
        mixed_ref[:, i * n : (i + 1) * n] = total.astype(LOW)
        if i % 2 == 0:
            (own_ref, other_ref)[i // 2][...] = total


def second_norm_back(residual, part, got, low, high, gain):
    length, width = residual.shape
    n = width // 4
    rows = row_tiles(length)
    one = jax.ShapeDtypeStruct((length, n), FULL)
    return pl.pallas_call(
        second_norm_back_kernel,
        out_shape=(one, one, jax.ShapeDtypeStruct((length, width), LOW), jax.ShapeDtypeStruct((8, 2 * n), FULL)),
        grid=(length // TILE,),
        in_specs=[rows(width)] * 3 + [rows(2 * n)] * 2 + [whole((1, width))],
        out_specs=(rows(n), rows(n), rows(width), whole((8, 2 * n))),
        name="second_norm_back",
        cost_estimate=cost(60 * length * n, 64 * length * n),
    )(residual, part, got, low, high, gain)


def first_norm_back_kernel(
    x0, x1, x2, x3, part_ref, got_ref, own_ref, other_ref, gain_ref, mine_ref, theirs_ref, sums_ref
):
    blocks = [x[...].astype(FULL) for x in (x0, x1, x2, x3)]
    grads = norm_gradient(blocks, part_ref, got_ref, gain_ref, sums_ref)
    mine_ref[...] = own_ref[...] + grads[0]
    theirs_ref[...] = (other_ref[...] + grads[2]).astype(LOW)


def first_norm_back(blocks, part, got, own, other, gain):
    length, n = blocks[0].shape
    rows = row_tiles(length)
    return pl.pallas_call(
        first_norm_back_kernel,
        out_shape=(
            jax.ShapeDtypeStruct((length, n), FULL),
            jax.ShapeDtypeStruct((length, n), LOW),
            jax.ShapeDtypeStruct((8, 2 * n), FULL),
        ),
        grid=(length // TILE,),
        in_specs=[rows(n)] * 4 + [rows(4 * n)] * 2 + [rows(n)] * 2 + [whole((1, 4 * n))],
        out_specs=(rows(n), rows(n), whole((8, 2 * n))),
        name="first_norm_back",
        cost_estimate=cost(60 * length * n, 40 * length * n),
    )(*blocks, part, got, own, other, gain)


def mix_kernel(h0, h1, w0, w1, out_ref):
    out_ref[...] = (dot_nn(h0[...], w0[...]) + dot_nn(h1[...], w1[...])).astype(LOW)


def mix_heads(heads, weights):
    length, depth = heads[0].shape
    width = weights[0].shape[1]
    rows = row_tiles(length)
    return pl.pallas_call(
        mix_kernel,
        out_shape=jax.ShapeDtypeStruct((length, width), LOW),
        grid=(length // TILE,),
        in_specs=[rows(depth)] * 2 + [whole((depth, width))] * 2,
        out_specs=rows(width),
        name="mix_heads",
        cost_estimate=cost(4 * length * depth * width, 4 * length * (depth + width)),
    )(*heads, *weights)


ROOT = math.sqrt(2.0 / math.pi)


def feed_forward_kernel(
    at_ref, s_low, s_high, c_low, c_high, u_low, u_high, d_low, d_high, bias_ref,
    part_ref, hidden0, hidden1, grad0, grad1, bias_sum, low_sum, high_sum,
):
    step = pl.program_id(0)
    steps = pl.num_programs(0)
    first = step < steps // 2

    @pl.when(step == 0)
    def _():
        low_sum[...] = jnp.zeros_like(low_sum)
        high_sum[...] = jnp.zeros_like(high_sum)

    totals = 0.0
    for t in range(s_low.shape[0] // TILE):
        rows = slice(t * TILE, (t + 1) * TILE)
        upward = dot_nn(s_low[rows, :], u_low[0]) + dot_nn(s_high[rows, :], u_high[0]) + bias_ref[0]
        grad_hidden = dot_nt(c_low[rows, :], d_low[0]) + dot_nt(c_high[rows, :], d_high[0])
        square = upward * upward
        bent = jnp.tanh(upward * (ROOT + (ROOT * 0.044715) * square))
        lifted = 0.5 + 0.5 * bent
        slope = lifted + (0.5 * upward) * (1.0 - bent * bent) * (ROOT + (ROOT * 3 * 0.044715) * square)
        hidden = (upward * lifted).astype(LOW)
        grad = grad_hidden * slope
        totals = totals + jnp.sum(grad, axis=0, keepdims=True)
        grad = grad.astype(LOW)

        @pl.when(first)
        def _():
            hidden0[rows, :] = hidden
            grad0[rows, :] = grad

        @pl.when(jnp.logical_not(first))
        def _():
            hidden1[rows, :] = hidden
            grad1[rows, :] = grad

        low_sum[rows, :] += dot_nt(grad, u_low[0])
        high_sum[rows, :] += dot_nt(grad, u_high[0])
    bias_sum[0] = jnp.broadcast_to(totals, bias_sum.shape[1:])

    @pl.when(step == steps - 1)
    def _():
        n = low_sum.shape[1]
        part_ref[:, :n] = low_sum[...].astype(LOW)
        part_ref[:, n:] = high_sum[...].astype(LOW)


def feed_forward(at, seconds, cots, ups, downs, biases):
    length, h = seconds[0].shape
    each = ups.shape[2]
    tiles = each // TILE
    keep = pl.BlockSpec((length, h), lambda i, at: (0, 0))

    def up_spec(flip):
        return pl.BlockSpec(
            (1, h, TILE), lambda i, at: ((at[0] ^ flip) * 2 + (at[1] ^ (i // tiles)), 0, lax.rem(i, tiles))
        )

    def down_spec(flip):
        return pl.BlockSpec(
            (1, TILE, h), lambda i, at: ((at[0] ^ flip) * 2 + (at[1] ^ (i // tiles)), lax.rem(i, tiles), 0)
        )

    early = pl.BlockSpec((length, TILE), lambda i, at: (0, jnp.minimum(i, tiles - 1)))
    late = pl.BlockSpec((length, TILE), lambda i, at: (0, jnp.maximum(i - tiles, 0)))
    one = jax.ShapeDtypeStruct((length, each), LOW)
    return pl.pallas_call(
        feed_forward_kernel,
        out_shape=(
            jax.ShapeDtypeStruct((length, 2 * h), LOW), one, one, one, one,
            jax.ShapeDtypeStruct((2 * tiles, 8, TILE), FULL),
        ),
        grid_spec=pltpu.PrefetchScalarGridSpec(
            num_scalar_prefetch=1,
            grid=(2 * tiles,),
            in_specs=[keep] * 4
            + [up_spec(0), up_spec(1), down_spec(0), down_spec(1)]
            + [pl.BlockSpec((1, 1, TILE), lambda i, at: (i, 0, 0))],
            out_specs=(
                pl.BlockSpec((length, 2 * h), lambda i, at: (0, 0)), early, late, early, late,
                pl.BlockSpec((1, 8, TILE), lambda i, at: (i, 0, 0)),
            ),
            scratch_shapes=[pltpu.VMEM((length, h), FULL), pltpu.VMEM((length, h), FULL)],
        ),
        name="feed_forward",
        cost_estimate=cost(12 * length * 2 * h * each, 8 * length * h + 16 * h * each + 16 * length * each),
    )(at, *seconds, *cots, ups, ups, downs, downs, biases.reshape(2 * tiles, 1, TILE))


def layer_end_kernel(at_ref, h0, h1, w00, w01, w10, w11, own_ref, theirs_ref):
    n = own_ref.shape[1] // 2
    for j, (a, b) in enumerate(((w00, w01), (w10, w11))):
        part = dot_nn(h0[...], a[0]) + dot_nn(h1[...], b[0])
        own_ref[:, j * n : (j + 1) * n] = part[:, :n]
        theirs_ref[:, j * n : (j + 1) * n] = part[:, n:].astype(LOW)


def layer_end(at, hiddens, downs):
    length, each = hiddens[0].shape
    h = downs.shape[2]
    rows = pl.BlockSpec((TILE, each), lambda t, at: (t, 0))
    out = pl.BlockSpec((TILE, h), lambda t, at: (t, 0))

    def weight(y, col):
        return pl.BlockSpec((1, each, h), lambda t, at: ((at[0] ^ y) * 2 + (at[1] ^ col), 0, 0))

    return pl.pallas_call(
        layer_end_kernel,
        out_shape=(jax.ShapeDtypeStruct((length, h), FULL), jax.ShapeDtypeStruct((length, h), LOW)),
        grid_spec=pltpu.PrefetchScalarGridSpec(
            num_scalar_prefetch=1,
            grid=(length // TILE,),
            in_specs=[rows, rows, weight(0, 0), weight(0, 1), weight(1, 0), weight(1, 1)],
            out_specs=(out, out),
        ),
        name="layer_end",
        cost_estimate=cost(8 * length * h * each, 8 * h * each + 12 * length * h),
    )(at, *hiddens, downs, downs, downs, downs)


def pick(pair, index):
    return lax.dynamic_index_in_dim(pair, index, 0, keepdims=False)


def ordered(own, other, index):
    flip = index == 0
    return jnp.stack((jnp.where(flip, own, other), jnp.where(flip, other, own)))


def swap_across(array):
    return lax.ppermute(array, ("y", "col"), [(0, 3), (3, 0), (1, 2), (2, 1)])


def plane_gather(block):
    return block, swap(block, "y"), swap(block, "col"), swap_across(block)


def plane_reduce(own, at_y, at_col, across):
    got = (swap(at_y, "y"), swap(at_col, "col"), swap_across(across))
    return (own.astype(FULL) + sum(g.astype(FULL) for g in got)).astype(LOW)


def depth_sum(array, index):
    near = array + lax.ppermute(array, "dp", [(0, 1), (3, 2)])
    both = near + lax.ppermute(near, "dp", [(1, 2), (2, 1)])
    back = lax.ppermute(both, "dp", [(1, 0), (2, 3)])
    return jnp.where((index == 0) | (index == 3), back, both)


def half(weight, axis, index):
    size = weight.shape[axis] // 2
    return lax.dynamic_slice_in_dim(weight, index * size, size, axis)


def fast_body(
    inputs, gain_first, shift_first, w_query, w_key, w_value, w_output, gain_second, shift_second,
    w_up, bias_up, w_down, bias_down, segments, random_blocks, global_blocks, cotangent,
):
    depth_at, y_at, core_at, col_at = (lax.axis_index(name) for name in ("dp", "y", "core", "col"))
    length = segments.shape[1]
    n = inputs.shape[1]
    h = 2 * n
    at = jnp.stack((y_at, col_at)).astype(jnp.int32)

    def chip_block(weights, axis, join):
        mine = jnp.concatenate([half(w, axis, core_at) for w in weights], axis=axis)
        theirs = swap(jnp.concatenate([half(w, axis, 1 - core_at) for w in weights], axis=axis), "core")
        return jnp.concatenate((mine, theirs), axis=join)

    inputs_pair = inputs.reshape(2, length, n)
    cot_pair = cotangent.reshape(2, length, n)
    x_own = pick(inputs_pair, y_at)
    x_y = swap(pick(inputs_pair, 1 - y_at), "y")
    qkv_own, qkv_y, qkv_x, qkv_xy = plane_gather(chip_block((w_query, w_key, w_value), 1, 0))
    xs = (x_own, swap(x_own, "core"), x_y, swap(x_y, "core"))
    out_own, out_y, out_x, out_xy = plane_gather(chip_block((w_output,), 0, 1))
    ups = lax.all_gather(chip_block((w_up,), 1, 0), ("y", "col"), axis=0, tiled=False)
    downs = lax.all_gather(chip_block((w_down,), 0, 1), ("y", "col"), axis=0, tiled=False)

    vectors = jnp.stack((gain_first, shift_first, gain_second, shift_second, bias_down))
    vectors = jnp.concatenate((vectors, swap(vectors, "core")), axis=1)
    vectors = jnp.concatenate((vectors, swap(vectors, "y")), axis=1)
    gain_one, shift_one, gain_two, shift_two, bias_low = (vectors[i : i + 1] for i in range(5))
    heads_half = half(random_blocks, 0, core_at)
    hidden_bias = half(bias_up, 0, core_at)
    each = hidden_bias.shape[0]
    small = swap(jnp.concatenate((hidden_bias, heads_half.astype(FULL).reshape(-1))), "col")
    biases = jnp.concatenate((hidden_bias, small[:each]))
    heads_half_x = small[each:].reshape(heads_half.shape).astype(jnp.int32)
    moves = []
    for y in range(2):
        for core in range(2):
            for col in range(2):
                moves.append(((col * 2 + y) * 2 + core, (y * 2 + core) * 2 + col))
    labels = lax.ppermute(segments, ("y", "core", "col"), moves)[0]
    all_heads = jnp.concatenate((heads_half, heads_half_x), axis=0)
    rows_extra, keys_extra, where_table = attention_extras(labels, all_heads, global_blocks)
    near_heads = heads_half.shape[0]
    keys_of = (keys_extra[:near_heads], keys_extra[near_heads:])
    live = (labels != 0)[:, None]

    cot_own = pick(cot_pair, y_at)
    cot_y = swap(pick(cot_pair, 1 - y_at), "y")
    cots = tuple(jnp.concatenate((c, swap(c, "core")), axis=1) for c in (cot_own, cot_y))

    firsts = first_norm(xs, gain_one, shift_one)
    w_qkv = (jnp.concatenate((qkv_own, qkv_y), axis=0), jnp.concatenate((qkv_x, qkv_xy), axis=0))
    first = jnp.concatenate(firsts, axis=1)
    w_out = (jnp.concatenate((out_own, out_y), axis=1), jnp.concatenate((out_x, out_xy), axis=1))
    qkv, heads, kept = [], [], []
    for i in range(2):
        qkv.append(dot_nn(first, w_qkv[i]).astype(LOW))
        done, saved = attend_forward(qkv[i], rows_extra, keys_of[i], where_table)
        heads.append(done)
        kept.append(saved)
    mixed_part = mix_heads(heads, w_out)
    residual, *seconds = second_norm(xs, mixed_part, swap(mixed_part, "core"), gain_two, shift_two)

    second_part, hidden0, hidden1, grad0, grad1, bias_sum = feed_forward(at, seconds, cots, ups, downs, biases)
    hiddens, up_sides = (hidden0, hidden1), (grad0, grad1)
    second_got = swap(second_part, "core")
    down_grads = [[dot_tn(hid, c).astype(LOW) for c in cots] for hid in hiddens]
    up_grads = [[dot_tn(s, g).astype(LOW) for s in seconds] for g in up_sides]
    down_total = plane_reduce(down_grads[0][0], down_grads[0][1], down_grads[1][0], down_grads[1][1])
    up_total = plane_reduce(up_grads[0][0], up_grads[0][1], up_grads[1][0], up_grads[1][1])

    grad_own, grad_other, grad_mixed, sums_two = second_norm_back(residual, second_part, second_got, *cots, gain_two)
    grads = jnp.where(live, dot_nt(grad_mixed, jnp.concatenate(w_out, axis=0)), 0.0).astype(LOW)
    out_grads = [dot_tn(head, grad_mixed).astype(LOW) for head in heads]
    out_total = plane_reduce(out_grads[0][:, :h], out_grads[0][:, h:], out_grads[1][:, :h], out_grads[1][:, h:])
    qkv_sides, qkv_grads = [None, None], [None, None]
    for i in (1, 0):
        qkv_sides[i] = attend_backward(kept[i], qkv[i], keys_of[i], heads[i], grads, i, where_table)
        qkv_grads[i] = [dot_tn(f, qkv_sides[i]).astype(LOW) for f in firsts]
    qkv_total = plane_reduce(qkv_grads[0][0], qkv_grads[0][1], qkv_grads[1][0], qkv_grads[1][1])
    first_part = dot_nt(jnp.concatenate(qkv_sides, axis=1), jnp.concatenate(w_qkv, axis=1)).astype(LOW)
    mine, theirs, sums_one = first_norm_back(xs, first_part, swap(first_part, "core"), grad_own, grad_other, gain_one)
    grad_inputs = ordered(mine, swap(theirs, "y").astype(FULL), y_at).reshape(2 * length, n)

    ends_own, ends_other = layer_end(at, hiddens, downs)
    kept_two = jnp.concatenate((residual[:, :n], residual[:, 2 * n : 3 * n]), axis=1)
    bias_two = jnp.concatenate((bias_low[:, :n], bias_low[:, 2 * n : 3 * n]), axis=1)
    ends = (kept_two + ends_own + swap(ends_other, "core").astype(FULL) + bias_two).astype(LOW)
    layer_out = ordered(ends[:, :n], swap(ends[:, n:], "y"), y_at).reshape(2 * length, n)

    gains = jnp.concatenate((sums_one[:2, :n], sums_two[:2, :n])).reshape(-1)
    gains_y = jnp.concatenate((sums_one[:2, n:], sums_two[:2, n:])).reshape(-1)
    up_bias = bias_sum[:, 0, :].reshape(-1)
    got = swap(jnp.concatenate((gains_y, up_bias)), "y")
    gains = gains + got[: 4 * n]
    up_bias = up_bias + got[4 * n :]
    near = jnp.concatenate((gains, jnp.sum(cotangent, axis=0, dtype=FULL), up_bias[:each]))
    near = near + swap(jnp.concatenate((near[: 5 * n], up_bias[each:])), "col")
    near = near + lax.ppermute(near, "dp", [(0, 1), (1, 0), (2, 3), (3, 2)])
    near = near + lax.ppermute(near, "dp", [(0, 2), (2, 0), (1, 3), (3, 1)])
    gains = near[: 5 * n].reshape(5, n)
    up_bias = ordered(near[5 * n :], swap(near[5 * n :], "core"), core_at).reshape(-1)

    def finish(total, axis, parts):
        total = depth_sum(total, depth_at)
        keep = lax.slice_in_dim(total, 0, n, axis=axis)
        got = swap(lax.slice_in_dim(total, n, 2 * n, axis=axis), "core")
        size = keep.shape[1 - axis] // parts
        flip = core_at == 0
        out = []
        for i in range(parts):
            a, b = (lax.slice_in_dim(z, i * size, (i + 1) * size, axis=1 - axis) for z in (keep, got))
            out.append(jnp.concatenate((jnp.where(flip, a, b), jnp.where(flip, b, a)), axis=1 - axis).astype(FULL))
        return out

    (grad_down,) = finish(down_total, 1, 1)
    (grad_up,) = finish(up_total, 0, 1)
    (grad_out,) = finish(out_total, 1, 1)
    grad_query, grad_key, grad_value = finish(qkv_total, 0, 3)
    return (
        layer_out, grad_inputs, gains[0], gains[1], grad_query, grad_key, grad_value, grad_out, gains[2], gains[3],
        grad_up, up_bias, grad_down, gains[4],
    )


def whole_sequences(mesh):
    return mesh.shape["row"] == 4 and mesh.shape["col"] == 2 and mesh.shape["dp"] == 4


def placements(row):
    tokens = P(("dp", "col"), row)
    rows = P(row)
    weight = P(row, "col")
    turned = P("col", row)
    placed = (
        tokens, rows, rows, weight, weight, weight, turned, rows, rows, weight, P("col"), turned, rows,
        P(("dp", *row), None), P("col", None, None), P(), tokens,
    )
    given = (
        tokens, tokens, rows, rows, weight, weight, weight, turned, rows, rows, weight, P("col"), turned, rows,
    )
    return placed, given


def solution(mesh):
    sizes = mesh.shape
    split = jax.sharding.Mesh(
        mesh.devices.reshape(sizes["dp"], sizes["row"] // 2, 2, sizes["col"]), ("dp", "y", "core", "col")
    )

    def run(*arrays):
        tokens, length = arrays[0].shape[0], arrays[13].shape[1]
        if whole_sequences(mesh) and tokens == sizes["dp"] * sizes["col"] * 2 * length:
            placed, given = placements(("y", "core"))
            step = jax.shard_map(fast_body, mesh=split, in_specs=placed, out_specs=given, check_vma=False)
        else:
            placed, given = placements(("row",))
            step = jax.shard_map(body, mesh=mesh, in_specs=placed, out_specs=given, check_vma=False)
        return step(*arrays)

    return run
```

```python
import math

import jax
import jax.numpy as jnp
from jax import lax
from jax.experimental import pallas as pl
from jax.experimental.pallas import tpu as pltpu
from jax.sharding import PartitionSpec as P

D = 1024
HD = 64
BLK = 64
NB = 16


EPS = 1e-05


def product(picked, weight, flipped):
    if flipped:
        return lax.dot_general(
            picked, weight, (((1,), (1,)), ((), ())), preferred_element_type=jnp.float32
        )
    return jnp.dot(picked, weight, preferred_element_type=jnp.float32)


def to_columns(moving, weight, flipped):
    gathered = lax.all_gather(moving, "col", axis=0, tiled=True)
    row_count = gathered.shape[0] // lax.axis_size("row")

    def term_rows(first_row, how_many):
        return product(gathered, weight, flipped)

    result = lax.psum_scatter(
        term_rows(jnp.int32(0), lax.axis_size("row") * row_count),
        "row",
        scatter_dimension=0,
        tiled=True,
    )
    return (result, gathered)


def to_rows(moving, weight, flipped):
    gathered = lax.all_gather(moving, "row", axis=0, tiled=True)
    row_count = gathered.shape[0] // lax.axis_size("col")

    def term_rows(first_row, how_many):
        return product(gathered, weight, flipped)

    return (
        lax.psum_scatter(
            term_rows(jnp.int32(0), lax.axis_size("col") * row_count),
            "col",
            scatter_dimension=0,
            tiled=True,
        ),
        gathered,
    )


def norm_sums(first_sum, second_sum):
    return lax.psum((first_sum, second_sum), "row")


def norm_forward(moving, gain_row, shift_row):
    totals, squares = norm_sums(jnp.sum(moving, axis=1), jnp.sum(moving * moving, axis=1))
    center = totals / D
    spread = squares / D - center * center
    inverse = lax.rsqrt(spread + EPS)
    normed = (moving - center[:, None]) * inverse[:, None]
    return (normed * gain_row + shift_row, normed, inverse)


def norm_backward(upstream, normed, inverse, gain_row):
    scaled = upstream * gain_row
    first_sum, second_sum = norm_sums(jnp.sum(scaled, axis=1), jnp.sum(scaled * normed, axis=1))
    return inverse[:, None] * (scaled - first_sum[:, None] / D - normed * (second_sum[:, None] / D))


def head_masks(random_blocks, global_blocks):
    block_ids = jnp.arange(NB, dtype=jnp.int32)
    nearby = jnp.abs(block_ids[:, None] - block_ids[None, :]) <= 1
    chosen = jnp.any(random_blocks[:, :, :, None] == block_ids[None, None, None, :], axis=2)
    marked = jnp.any(global_blocks[:, None] == block_ids[None, :], axis=0)
    block_table = nearby[None] | chosen | marked[None, None, :] | marked[None, :, None]
    return jnp.repeat(jnp.repeat(block_table, BLK, axis=1), BLK, axis=2)


def seq_logits(seq_queries, seq_keys, labels, pattern):
    same_doc = (labels[:, None] == labels[None, :]) & (labels[None, :] != 0)
    raw_scores = jnp.einsum(
        "qhd,khd->hqk", seq_queries, seq_keys, preferred_element_type=jnp.float32
    )
    return jnp.where(pattern & same_doc[None], raw_scores * (1.0 / math.sqrt(HD)), -1000000000.0)


def attend_plain(queries, key_block, value_block, segments, pattern):

    def one_seq(pieces):
        seq_queries, seq_keys, seq_values, labels = pieces
        logits = seq_logits(seq_queries, seq_keys, labels, pattern)
        row_peak = jnp.max(logits, axis=2, keepdims=True)
        exp_terms = jnp.exp(logits - row_peak)
        row_total = jnp.sum(exp_terms, axis=2, keepdims=True)
        softmax = (exp_terms / row_total).astype(jnp.bfloat16)
        attended = jnp.einsum(
            "hqk,khd->qhd", softmax, seq_values, preferred_element_type=jnp.float32
        )
        live_rows = (labels != 0).astype(jnp.float32)
        return (attended * live_rows[:, None, None], (row_peak + jnp.log(row_total))[:, :, 0])

    return lax.map(one_seq, (queries, key_block, value_block, segments))


def attend_plain_backward(queries, key_block, value_block, segments, pattern, grad_heads, log_total):

    def one_seq(pieces):
        seq_queries, seq_keys, seq_values, labels, seq_grads, seq_log = pieces
        logits = seq_logits(seq_queries, seq_keys, labels, pattern)
        softmax = jnp.exp(logits - seq_log[:, :, None])
        grad_probs = jnp.einsum(
            "qhd,khd->hqk", seq_grads, seq_values, preferred_element_type=jnp.float32
        )
        grad_values = jnp.einsum(
            "hqk,qhd->khd",
            softmax.astype(jnp.bfloat16),
            seq_grads,
            preferred_element_type=jnp.float32,
        )
        inner_sum = jnp.sum(softmax * grad_probs, axis=2, keepdims=True)
        grad_raw = (softmax * (grad_probs - inner_sum) * (1.0 / math.sqrt(HD))).astype(jnp.bfloat16)
        grad_queries = jnp.einsum(
            "hqk,khd->qhd", grad_raw, seq_keys, preferred_element_type=jnp.float32
        )
        grad_keys = jnp.einsum(
            "hqk,qhd->khd", grad_raw, seq_queries, preferred_element_type=jnp.float32
        )
        return (grad_queries, grad_keys, grad_values)

    return lax.map(one_seq, (queries, key_block, value_block, segments, grad_heads, log_total))


def gelu_tanh(values):
    return jax.nn.gelu(values, approximate=True)


def weight_grad(left, right):
    return lax.dot_general(
        left, right, (((0,), (0,)), ((), ())), preferred_element_type=jnp.float32
    )


def body(
    inputs,
    gain_first,
    shift_first,
    w_query,
    w_key,
    w_value,
    w_output,
    gain_second,
    shift_second,
    w_up,
    bias_up,
    w_down,
    bias_down,
    segments,
    random_blocks,
    global_blocks,
    cotangent,
):
    seq_count, seq_len = segments.shape
    head_width = w_query.shape[1]
    heads_here = random_blocks.shape[0]
    seq_shape = (seq_count, seq_len, heads_here, HD)
    pattern = head_masks(random_blocks, global_blocks)
    live_tokens = (segments != 0).reshape(-1)
    x_first = inputs.astype(jnp.float32)
    first_full, normed_one, inverse_one = norm_forward(x_first, gain_first, shift_first)
    first_low = first_full.astype(jnp.bfloat16)
    stacked = jnp.concatenate((w_query, w_key, w_value), axis=1)
    projected, first_all = to_columns(first_low, stacked, False)
    proj_low = projected.astype(jnp.bfloat16)
    queries = proj_low[:, :head_width].reshape(seq_shape)
    key_block = proj_low[:, head_width : 2 * head_width].reshape(seq_shape)
    value_block = proj_low[:, 2 * head_width :].reshape(seq_shape)
    heads_out, log_total = attend_plain(queries, key_block, value_block, segments, pattern)
    heads_low = heads_out.reshape(-1, head_width).astype(jnp.bfloat16)
    mixed_out, heads_all = to_rows(heads_low, w_output, False)
    residual = x_first + mixed_out
    second_full, normed_two, inverse_two = norm_forward(residual, gain_second, shift_second)
    second_low = second_full.astype(jnp.bfloat16)
    upward, second_all = to_columns(second_low, w_up, False)
    upward = upward + bias_up
    hidden_low = gelu_tanh(upward).astype(jnp.bfloat16)
    downward, hidden_all = to_rows(hidden_low, w_down, False)
    layer_out = (residual + (downward + bias_down)).astype(jnp.bfloat16)
    grad_hidden, cotangent_all = to_columns(cotangent, w_down, True)
    activated, pull_back = jax.vjp(gelu_tanh, upward)
    grad_upward = pull_back(grad_hidden)[0].astype(jnp.bfloat16)
    grad_second, grad_upward_all = to_rows(grad_upward, w_up, True)
    grad_residual = cotangent.astype(jnp.float32) + norm_backward(
        grad_second, normed_two, inverse_two, gain_second
    )
    grad_mixed = grad_residual.astype(jnp.bfloat16)
    grad_heads, grad_mixed_all = to_columns(grad_mixed, w_output, True)
    grad_heads = jnp.where(live_tokens[:, None], grad_heads, 0.0).astype(jnp.bfloat16)
    grad_queries, grad_keys, grad_values = attend_plain_backward(
        queries, key_block, value_block, segments, pattern, grad_heads.reshape(seq_shape), log_total
    )
    grad_proj = jnp.concatenate(
        (
            grad_queries.reshape(-1, head_width),
            grad_keys.reshape(-1, head_width),
            grad_values.reshape(-1, head_width),
        ),
        axis=1,
    ).astype(jnp.bfloat16)
    grad_first, grad_proj_all = to_rows(grad_proj, stacked, True)
    grad_inputs = grad_residual + norm_backward(grad_first, normed_one, inverse_one, gain_first)
    grad_stacked = weight_grad(first_all, grad_proj_all)
    grad_out_weight = weight_grad(heads_all, grad_mixed_all)
    grad_up_weight = weight_grad(second_all, grad_upward_all)
    grad_down_weight = weight_grad(hidden_all, cotangent_all)
    grad_up_bias = jnp.sum(grad_upward_all, axis=0, dtype=jnp.float32)
    grad_down_bias = jnp.sum(cotangent_all, axis=0, dtype=jnp.float32)
    gain_terms = lax.psum(
        (
            jnp.sum(grad_first * normed_one, axis=0),
            jnp.sum(grad_first, axis=0),
            jnp.sum(grad_second * normed_two, axis=0),
            jnp.sum(grad_second, axis=0),
        ),
        ("dp", "col"),
    )
    summed = (
        lax.psum(grad_stacked.astype(jnp.bfloat16), "dp").astype(jnp.float32),
        lax.psum(grad_out_weight.astype(jnp.bfloat16), "dp").astype(jnp.float32),
        lax.psum(grad_up_weight.astype(jnp.bfloat16), "dp").astype(jnp.float32),
        lax.psum(grad_down_weight.astype(jnp.bfloat16), "dp").astype(jnp.float32),
        lax.psum(grad_up_bias.astype(jnp.bfloat16), "dp").astype(jnp.float32),
        lax.psum(grad_down_bias.astype(jnp.bfloat16), "dp").astype(jnp.float32),
    )
    return (
        layer_out,
        grad_inputs,
        gain_terms[0],
        gain_terms[1],
        summed[0][:, :head_width],
        summed[0][:, head_width : 2 * head_width],
        summed[0][:, 2 * head_width :],
        summed[1],
        gain_terms[2],
        gain_terms[3],
        summed[2],
        summed[4],
        summed[3],
        summed[5],
    )


SWAP = [(0, 1), (1, 0)]
LOW = jnp.bfloat16
FULL = jnp.float32
TILE = 256
BIG = 1e30


def swap(array, axis):
    return lax.ppermute(array, axis, SWAP)


def dot_nn(left, right):
    return lax.dot_general(left, right, (((1,), (0,)), ((), ())), preferred_element_type=FULL)


def dot_nt(left, right):
    return lax.dot_general(left, right, (((1,), (1,)), ((), ())), preferred_element_type=FULL)


def dot_tn(left, right):
    return lax.dot_general(left, right, (((0,), (0,)), ((), ())), preferred_element_type=FULL)


def attention_extras(labels, random_blocks, global_blocks):
    length = labels.shape[0]
    blocks = length // BLK
    block_ids = jnp.arange(blocks, dtype=jnp.int32)
    nearby = jnp.abs(block_ids[:, None] - block_ids[None, :]) <= 1
    chosen = jnp.any(random_blocks[:, :, :, None] == block_ids[None, None, None, :], axis=2)
    marked = jnp.any(global_blocks[:, None] == block_ids[None, :], axis=0)
    table = nearby[None] | chosen | marked[None, None, :] | marked[None, :, None]
    heads = table.shape[0]
    lane = jnp.arange(HD, dtype=jnp.int32)
    place = jnp.arange(length, dtype=jnp.int32) // BLK
    doc_lane = blocks + jnp.where(labels == 0, 4, labels - 1)
    row_extra = ((lane[None, :] == place[:, None]) | (lane[None, :] == doc_lane[:, None])).astype(LOW)
    table_keys = jnp.pad(jnp.swapaxes(table, 1, 2), ((0, 0), (0, 0), (0, HD - blocks)), constant_values=True)
    table_keys = jnp.repeat(table_keys, BLK, axis=1)
    is_doc = (lane >= blocks) & (lane <= blocks + 4)
    doc_bad = is_doc[None, :] & (lane[None, :] != doc_lane[:, None])
    doc_bad = doc_bad | (lane[None, :] == blocks + 4)
    key_extra = jnp.where(table_keys & ~doc_bad[None], 0.0, -BIG)
    key_extra = jnp.where((lane >= blocks + 5) & (lane <= blocks + 7), 1.0, key_extra).astype(LOW)
    rows = jnp.stack((jnp.pad(row_extra, ((0, 0), (HD, 0))), jnp.pad(row_extra, ((0, 0), (0, HD)))))
    even = jnp.pad(key_extra[0::2], ((0, 0), (0, 0), (HD, 0)))
    odd = jnp.pad(key_extra[1::2], ((0, 0), (0, 0), (0, HD)))
    keys = jnp.stack((even, odd), axis=1).reshape(heads, length, 2 * HD)
    tiles = length // TILE
    known = labels[None, :] == jnp.arange(1, 5, dtype=jnp.int32)[:, None]
    present = jnp.any(known.reshape(4, tiles, TILE), axis=2)
    wanted = jnp.any(present[:, :, None] & known[:, None, :], axis=0)
    spots = jnp.arange(length, dtype=jnp.int32)
    first = jnp.min(jnp.where(wanted, spots[None, :], length - 1), axis=1)
    last = jnp.max(jnp.where(wanted, spots[None, :], 0), axis=1)
    start = first // 128
    count = jnp.maximum((last + 1 - start * 128 + 255) // 256, 1)
    start = jnp.minimum(start, length // 128 - 2 * count)
    return rows, keys, jnp.stack((start, count)).astype(jnp.int32)


def attend_forward_kernel(where_ref, q_ref, k_ref, v_ref, rows_ref, keys_ref, out_ref, kept_ref, kk, vv):
    length = q_ref.shape[0]
    lane = lax.broadcasted_iota(jnp.int32, (length, 2 * HD), 1)
    for e in range(2):
        data = (lane < HD) if e == 0 else (lane >= HD)
        kk[e] = jnp.where(data, k_ref[...], keys_ref[e])
        vv[e] = jnp.where(data, v_ref[...], jnp.ones_like(v_ref[...]))
    tile_lane = lax.broadcasted_iota(jnp.int32, (TILE, 2 * HD), 1)

    def one_tile(t, carry):
        rows = pl.ds(pl.multiple_of(t * TILE, TILE), TILE)
        start = pl.multiple_of(where_ref[0, t] * 128, 128)
        count = where_ref[1, t]
        q_pair = q_ref[rows, :] * jnp.bfloat16(1.0 / math.sqrt(HD))
        for n in range(1, length // TILE + 1):

            @pl.when(count == n)
            def _():
                span = pl.ds(start, n * TILE)
                outs = []
                for e in range(2):
                    data = (tile_lane < HD) if e == 0 else (tile_lane >= HD)
                    base = HD if e == 0 else 0
                    extra = rows_ref[e, rows, :]
                    q_one = jnp.where(data, q_pair, extra)
                    logits = dot_nt(q_one, kk[e, span, :])
                    peak = jnp.max(logits, axis=1, keepdims=True)
                    terms = jnp.exp(logits - peak)
                    mixed = dot_nn(terms.astype(LOW), vv[e, span, :])
                    total = pltpu.roll(mixed, HD, 1)
                    outs.append(mixed / total)
                    total_one = jnp.max(jnp.where(data, total, 0.0), axis=1, keepdims=True)
                    padded = jnp.max(
                        jnp.where(tile_lane == base + 20, extra.astype(FULL), 0.0), axis=1, keepdims=True
                    )
                    log_total = jnp.where(padded > 0.5, 0.0, -(peak + jnp.log(total_one)))
                    high = log_total.astype(LOW).astype(FULL)
                    middle = (log_total - high).astype(LOW).astype(FULL)
                    low = log_total - high - middle
                    packed = jnp.where(tile_lane == base + 21, high, q_one.astype(FULL))
                    packed = jnp.where(tile_lane == base + 22, middle, packed)
                    packed = jnp.where(tile_lane == base + 23, low, packed)
                    kept_ref[e, rows, :] = packed.astype(LOW)
                joined = jnp.where(tile_lane < HD, outs[0], outs[1])
                out_ref[rows, :] = jnp.where(padded > 0.5, 0.0, joined).astype(LOW)

        return carry

    lax.fori_loop(0, length // TILE, one_tile, 0)


def attend_forward(qkv, rows_extra, keys_extra, where_table):
    length, width = qkv.shape
    pairs = width // (3 * 2 * HD)
    wide = 2 * HD
    return pl.pallas_call(
        attend_forward_kernel,
        out_shape=(
            jax.ShapeDtypeStruct((length, width // 3), LOW),
            jax.ShapeDtypeStruct((2 * pairs, length, wide), LOW),
        ),
        grid_spec=pltpu.PrefetchScalarGridSpec(
            num_scalar_prefetch=1,
            grid=(pairs,),
            in_specs=[
                pl.BlockSpec((length, wide), lambda p, w: (0, p)),
                pl.BlockSpec((length, wide), lambda p, w: (0, pairs + p)),
                pl.BlockSpec((length, wide), lambda p, w: (0, 2 * pairs + p)),
                pl.BlockSpec((2, length, wide), lambda p, w: (0, 0, 0)),
                pl.BlockSpec((2, length, wide), lambda p, w: (p, 0, 0)),
            ],
            out_specs=(
                pl.BlockSpec((length, wide), lambda p, w: (0, p)),
                pl.BlockSpec((2, length, wide), lambda p, w: (p, 0, 0)),
            ),
            scratch_shapes=[pltpu.VMEM((2, length, wide), LOW), pltpu.VMEM((2, length, wide), LOW)],
        ),
        name="attend_forward",
        cost_estimate=pl.CostEstimate(
            flops=8 * pairs * length * length * HD, bytes_accessed=16 * length * width, transcendentals=0
        ),
    )(where_table, qkv, qkv, qkv, rows_extra, keys_extra)


def attend_backward_kernel(
    where_ref, kept_ref, k_ref, v_ref, keys_ref, heads_ref, grads_ref, out_ref, kk, va, dk_sum, dv_sum
):
    length = k_ref.shape[0]
    wide = 2 * HD
    third = out_ref.shape[1] // 3
    pair = pl.program_id(0) * wide
    lane = lax.broadcasted_iota(jnp.int32, (length, wide), 1)
    for e in range(2):
        data = (lane < HD) if e == 0 else (lane >= HD)
        base = HD if e == 0 else 0
        kk[e] = jnp.where(data, k_ref[...], keys_ref[e])
        ones = jnp.where((lane == base) | (lane == base + 1), 1.0, 0.0).astype(LOW)
        va[e] = jnp.where(data, v_ref[...], ones)
    dk_sum[...] = jnp.zeros_like(dk_sum)
    dv_sum[...] = jnp.zeros_like(dv_sum)
    tile_lane = lax.broadcasted_iota(jnp.int32, (TILE, wide), 1)

    def one_tile(t, carry):
        rows = pl.ds(pl.multiple_of(t * TILE, TILE), TILE)
        start = pl.multiple_of(where_ref[0, t] * 128, 128)
        count = where_ref[1, t]
        grads = grads_ref[rows, :]
        both = grads.astype(FULL) * heads_ref[rows, :].astype(FULL)
        for n in range(1, length // TILE + 1):

            @pl.when(count == n)
            def _():
                span = pl.ds(start, n * TILE)
                outs = []
                for e in range(2):
                    data = (tile_lane < HD) if e == 0 else (tile_lane >= HD)
                    base = HD if e == 0 else 0
                    inner = -jnp.sum(jnp.where(data, both, 0.0), axis=1, keepdims=True)
                    high = inner.astype(LOW).astype(FULL)
                    only = jnp.where(data, grads, jnp.zeros_like(grads))
                    packed = jnp.where(tile_lane == base, high, only.astype(FULL))
                    packed = jnp.where(tile_lane == base + 1, inner - high, packed).astype(LOW)
                    q_one = kept_ref[e, rows, :]
                    q_only = jnp.where(data, q_one, jnp.zeros_like(q_one))
                    probs = jnp.exp(dot_nt(kk[e, span, :], q_one))
                    grad_raw = (probs * dot_nt(va[e, span, :], packed)).astype(LOW)
                    dv_sum[span, :] += dot_nn(probs.astype(LOW), only)
                    dk_sum[span, :] += dot_nn(grad_raw, q_only)
                    outs.append(dot_tn(grad_raw, kk[e, span, :]))
                joined = jnp.where(tile_lane < HD, outs[0], outs[1])
                lanes = pl.ds(pl.multiple_of(pair, wide), wide)
                out_ref[rows, lanes] = (joined * (1.0 / math.sqrt(HD))).astype(LOW)

        return carry

    lax.fori_loop(0, length // TILE, one_tile, 0)
    out_ref[:, pl.ds(pl.multiple_of(third + pair, wide), wide)] = dk_sum[...].astype(LOW)
    out_ref[:, pl.ds(pl.multiple_of(2 * third + pair, wide), wide)] = dv_sum[...].astype(LOW)


def attend_backward(kept, qkv, keys_extra, heads, grads, group, where_table):
    length, width = qkv.shape
    pairs = width // (3 * 2 * HD)
    wide = 2 * HD
    stacked = pl.BlockSpec((2, length, wide), lambda p, w: (p, 0, 0))
    return pl.pallas_call(
        attend_backward_kernel,
        out_shape=jax.ShapeDtypeStruct((length, width), LOW),
        grid_spec=pltpu.PrefetchScalarGridSpec(
            num_scalar_prefetch=1,
            grid=(pairs,),
            in_specs=[
                stacked,
                pl.BlockSpec((length, wide), lambda p, w: (0, pairs + p)),
                pl.BlockSpec((length, wide), lambda p, w: (0, 2 * pairs + p)),
                stacked,
                pl.BlockSpec((length, wide), lambda p, w: (0, p)),
                pl.BlockSpec((length, wide), lambda p, w: (0, group * pairs + p)),
            ],
            out_specs=pl.BlockSpec((length, width), lambda p, w: (0, 0)),
            scratch_shapes=[
                pltpu.VMEM((2, length, wide), LOW),
                pltpu.VMEM((2, length, wide), LOW),
                pltpu.VMEM((length, wide), FULL),
                pltpu.VMEM((length, wide), FULL),
            ],
        ),
        name="attend_backward",
        cost_estimate=pl.CostEstimate(
            flops=20 * pairs * length * length * HD, bytes_accessed=20 * length * width, transcendentals=0
        ),
    )(where_table, kept, qkv, qkv, keys_extra, heads, grads)


def row_tiles(count):
    def spec(width):
        return pl.BlockSpec((TILE, width), lambda t: (t, 0))

    return spec


def whole(shape):
    return pl.BlockSpec(shape, lambda t: (0,) * len(shape))


def cost(flops, moved):
    return pl.CostEstimate(flops=int(flops), bytes_accessed=int(moved), transcendentals=0)


def norm_parts(blocks):
    width = sum(b.shape[1] for b in blocks)
    total = sum(jnp.sum(b, axis=1, keepdims=True) for b in blocks)
    squares = sum(jnp.sum(b * b, axis=1, keepdims=True) for b in blocks)
    center = total / width
    return center, lax.rsqrt(squares / width - center * center + EPS)


def columns(ref, index, width):
    return ref[:, index * width : (index + 1) * width]


def first_norm_kernel(x0, x1, x2, x3, gain_ref, shift_ref, low_ref, high_ref):
    blocks = [x[...].astype(FULL) for x in (x0, x1, x2, x3)]
    n = blocks[0].shape[1]
    center, inverse = norm_parts(blocks)
    for i, block in enumerate(blocks):
        value = (block - center) * inverse * columns(gain_ref, i, n) + columns(shift_ref, i, n)
        (low_ref, high_ref)[i // 2][:, (i % 2) * n : (i % 2 + 1) * n] = value.astype(LOW)


def first_norm(blocks, gain, shift):
    length, n = blocks[0].shape
    rows = row_tiles(length)
    half = jax.ShapeDtypeStruct((length, 2 * n), LOW)
    return pl.pallas_call(
        first_norm_kernel,
        out_shape=(half, half),
        grid=(length // TILE,),
        in_specs=[rows(n)] * 4 + [whole((1, 4 * n))] * 2,
        out_specs=(rows(2 * n), rows(2 * n)),
        name="first_norm",
        cost_estimate=cost(20 * length * n, 16 * length * n),
    )(*blocks, gain, shift)


def second_norm_kernel(x0, x1, x2, x3, part_ref, got_ref, gain_ref, shift_ref, residual_ref, second_ref):
    n = x0.shape[1]
    blocks = []
    for i, x in enumerate((x0, x1, x2, x3)):
        mixed = columns(part_ref, i, n).astype(FULL) + columns(got_ref, i ^ 1, n).astype(FULL)
        blocks.append(x[...].astype(FULL) + mixed)
    center, inverse = norm_parts(blocks)
    for i, block in enumerate(blocks):
        residual_ref[:, i * n : (i + 1) * n] = block
        value = (block - center) * inverse * columns(gain_ref, i, n) + columns(shift_ref, i, n)
        second_ref[i // 2, :, (i % 2) * n : (i % 2 + 1) * n] = value.astype(LOW)


def second_norm(blocks, part, got, gain, shift):
    length, n = blocks[0].shape
    rows = row_tiles(length)
    return pl.pallas_call(
        second_norm_kernel,
        out_shape=(jax.ShapeDtypeStruct((length, 4 * n), FULL), jax.ShapeDtypeStruct((2, length, 2 * n), LOW)),
        grid=(length // TILE,),
        in_specs=[rows(n)] * 4 + [rows(4 * n)] * 2 + [whole((1, 4 * n))] * 2,
        out_specs=(rows(4 * n), pl.BlockSpec((2, TILE, 2 * n), lambda t: (0, t, 0))),
        name="second_norm",
        cost_estimate=cost(30 * length * n, 48 * length * n),
    )(*blocks, part, got, gain, shift)


def norm_gradient(blocks, part_ref, got_ref, gain_ref, sums_ref):
    n = blocks[0].shape[1]
    center, inverse = norm_parts(blocks)
    normed = [(b - center) * inverse for b in blocks]
    grads = [columns(part_ref, i, n).astype(FULL) + columns(got_ref, i ^ 1, n).astype(FULL) for i in range(4)]
    scaled = [g * columns(gain_ref, i, n) for i, g in enumerate(grads)]
    mean_one = sum(jnp.sum(s, axis=1, keepdims=True) for s in scaled) / (4 * n)
    mean_two = sum(jnp.sum(s * z, axis=1, keepdims=True) for s, z in zip(scaled, normed)) / (4 * n)

    @pl.when(pl.program_id(0) == 0)
    def _():
        sums_ref[...] = jnp.zeros_like(sums_ref)

    for slot, i in enumerate((0, 2)):
        place = slice(slot * n, (slot + 1) * n)
        sums_ref[0:1, place] += jnp.sum(grads[i] * normed[i], axis=0, keepdims=True)
        sums_ref[1:2, place] += jnp.sum(grads[i], axis=0, keepdims=True)
    return [inverse * (s - mean_one - z * mean_two) for s, z in zip(scaled, normed)]


def second_norm_back_kernel(
    residual_ref, part_ref, got_ref, cots_ref, gain_ref, own_ref, other_ref, mixed_ref, sums_ref
):
    n = residual_ref.shape[1] // 4
    blocks = [columns(residual_ref, i, n) for i in range(4)]
    for i, grad in enumerate(norm_gradient(blocks, part_ref, got_ref, gain_ref, sums_ref)):
        total = cots_ref[i // 2, :, (i % 2) * n : (i % 2 + 1) * n].astype(FULL) + grad
        mixed_ref[:, i * n : (i + 1) * n] = total.astype(LOW)
        if i % 2 == 0:
            (own_ref, other_ref)[i // 2][...] = total


def second_norm_back(residual, part, got, cots, gain):
    length, width = residual.shape
    n = width // 4
    rows = row_tiles(length)
    one = jax.ShapeDtypeStruct((length, n), FULL)
    return pl.pallas_call(
        second_norm_back_kernel,
        out_shape=(one, one, jax.ShapeDtypeStruct((length, width), LOW), jax.ShapeDtypeStruct((8, 2 * n), FULL)),
        grid=(length // TILE,),
        in_specs=[rows(width)] * 3 + [pl.BlockSpec((2, TILE, 2 * n), lambda t: (0, t, 0)), whole((1, width))],
        out_specs=(rows(n), rows(n), rows(width), whole((8, 2 * n))),
        name="second_norm_back",
        cost_estimate=cost(60 * length * n, 64 * length * n),
    )(residual, part, got, cots, gain)


def first_norm_back_kernel(
    x0, x1, x2, x3, part_ref, got_ref, own_ref, other_ref, gain_ref, mine_ref, theirs_ref, sums_ref
):
    blocks = [x[...].astype(FULL) for x in (x0, x1, x2, x3)]
    grads = norm_gradient(blocks, part_ref, got_ref, gain_ref, sums_ref)
    mine_ref[...] = own_ref[...] + grads[0]
    theirs_ref[...] = (other_ref[...] + grads[2]).astype(LOW)


def first_norm_back(blocks, part, got, own, other, gain):
    length, n = blocks[0].shape
    rows = row_tiles(length)
    return pl.pallas_call(
        first_norm_back_kernel,
        out_shape=(
            jax.ShapeDtypeStruct((length, n), FULL),
            jax.ShapeDtypeStruct((length, n), LOW),
            jax.ShapeDtypeStruct((8, 2 * n), FULL),
        ),
        grid=(length // TILE,),
        in_specs=[rows(n)] * 4 + [rows(4 * n)] * 2 + [rows(n)] * 2 + [whole((1, 4 * n))],
        out_specs=(rows(n), rows(n), whole((8, 2 * n))),
        name="first_norm_back",
        cost_estimate=cost(60 * length * n, 40 * length * n),
    )(*blocks, part, got, own, other, gain)


def mix_kernel(h0, h1, w0, w1, out_ref):
    out_ref[...] = (dot_nn(h0[...], w0[...]) + dot_nn(h1[...], w1[...])).astype(LOW)


def mix_heads(heads, weights):
    length, depth = heads[0].shape
    width = weights[0].shape[1]
    rows = row_tiles(length)
    return pl.pallas_call(
        mix_kernel,
        out_shape=jax.ShapeDtypeStruct((length, width), LOW),
        grid=(length // TILE,),
        in_specs=[rows(depth)] * 2 + [whole((depth, width))] * 2,
        out_specs=rows(width),
        name="mix_heads",
        cost_estimate=cost(4 * length * depth * width, 4 * length * (depth + width)),
    )(*heads, *weights)


ROOT = math.sqrt(2.0 / math.pi)


def feed_forward_kernel(
    at_ref, s_ref, c_ref, u_low, u_high, d_low, d_high, bias_ref, part_ref, hidden_ref, grad_ref, bias_sum, low_sum, high_sum
):
    step = pl.program_id(0)

    @pl.when(step == 0)
    def _():
        low_sum[...] = jnp.zeros_like(low_sum)
        high_sum[...] = jnp.zeros_like(high_sum)

    totals = 0.0
    for t in range(s_ref.shape[1] // TILE):
        rows = slice(t * TILE, (t + 1) * TILE)
        upward = dot_nn(s_ref[0, rows, :], u_low[0]) + dot_nn(s_ref[1, rows, :], u_high[0]) + bias_ref[0]
        grad_hidden = dot_nt(c_ref[0, rows, :], d_low[0]) + dot_nt(c_ref[1, rows, :], d_high[0])
        square = upward * upward
        bent = jnp.tanh(upward * (ROOT + (ROOT * 0.044715) * square))
        lifted = 0.5 + 0.5 * bent
        slope = lifted + (0.5 * upward) * (1.0 - bent * bent) * (ROOT + (ROOT * 3 * 0.044715) * square)
        hidden_ref[0, rows, :] = (upward * lifted).astype(LOW)
        grad = grad_hidden * slope
        totals = totals + jnp.sum(grad, axis=0, keepdims=True)
        grad = grad.astype(LOW)
        grad_ref[0, rows, :] = grad
        low_sum[rows, :] += dot_nt(grad, u_low[0])
        high_sum[rows, :] += dot_nt(grad, u_high[0])
    bias_sum[0] = jnp.broadcast_to(totals, bias_sum.shape[1:])

    @pl.when(step == pl.num_programs(0) - 1)
    def _():
        n = low_sum.shape[1]
        part_ref[:, :n] = low_sum[...].astype(LOW)
        part_ref[:, n:] = high_sum[...].astype(LOW)


def feed_forward(at, seconds, cots, weights, biases):
    _, length, h = seconds.shape
    each = weights.shape[1] // 2
    tiles = each // TILE
    per = h // TILE
    keep = pl.BlockSpec((2, length, h), lambda i, at: (0, 0, 0))

    def up_spec(flip):
        return pl.BlockSpec(
            (1, h, TILE),
            lambda i, at: (
                (at[0] ^ flip) * 2 + (at[1] ^ (i // tiles)), lax.rem(i, tiles) // per, lax.rem(lax.rem(i, tiles), per)
            ),
        )

    def down_spec(flip):
        return pl.BlockSpec(
            (1, TILE, h), lambda i, at: ((at[0] ^ flip) * 2 + (at[1] ^ (i // tiles)), tiles + lax.rem(i, tiles), 0)
        )

    side = pl.BlockSpec((1, length, TILE), lambda i, at: (i // tiles, 0, lax.rem(i, tiles)))
    one = jax.ShapeDtypeStruct((2, length, each), LOW)
    return pl.pallas_call(
        feed_forward_kernel,
        out_shape=(
            jax.ShapeDtypeStruct((length, 2 * h), LOW), one, one, jax.ShapeDtypeStruct((2 * tiles, 8, TILE), FULL),
        ),
        grid_spec=pltpu.PrefetchScalarGridSpec(
            num_scalar_prefetch=1,
            grid=(2 * tiles,),
            in_specs=[keep] * 2
            + [up_spec(0), up_spec(1), down_spec(0), down_spec(1)]
            + [pl.BlockSpec((1, 1, TILE), lambda i, at: (i, 0, 0))],
            out_specs=(
                pl.BlockSpec((length, 2 * h), lambda i, at: (0, 0)), side, side,
                pl.BlockSpec((1, 8, TILE), lambda i, at: (i, 0, 0)),
            ),
            scratch_shapes=[pltpu.VMEM((length, h), FULL), pltpu.VMEM((length, h), FULL)],
        ),
        name="feed_forward",
        cost_estimate=cost(12 * length * 2 * h * each, 8 * length * h + 16 * h * each + 16 * length * each),
    )(at, seconds, cots, weights, weights, weights, weights, biases.reshape(2 * tiles, 1, TILE))


def up_grads_kernel(at_ref, s_ref, grad_ref, out_ref, turned):
    h = out_ref.shape[2]

    @pl.when(pl.program_id(1) == 0)
    def _():
        turned[...] = s_ref[0].T

    for i in range(out_ref.shape[1] // h):
        part = dot_nn(turned[...], grad_ref[0, :, i * h : (i + 1) * h])
        out_ref[0, i * h : (i + 1) * h, :] = part.astype(LOW)


def up_grads(at, seconds, grads):
    _, length, h = seconds.shape
    each = grads.shape[2]
    return pl.pallas_call(
        up_grads_kernel,
        out_shape=jax.ShapeDtypeStruct((4, each, h), LOW),
        grid_spec=pltpu.PrefetchScalarGridSpec(
            num_scalar_prefetch=1,
            grid=(2, 2),
            in_specs=[
                pl.BlockSpec((1, length, h), lambda y, c, at: (y, 0, 0)),
                pl.BlockSpec((1, length, each), lambda y, c, at: (c, 0, 0)),
            ],
            out_specs=pl.BlockSpec((1, each, h), lambda y, c, at: ((at[0] ^ y) * 2 + (at[1] ^ c), 0, 0)),
            scratch_shapes=[pltpu.VMEM((h, length), LOW)],
        ),
        name="up_grads",
        cost_estimate=cost(8 * length * h * each, 4 * length * each + 8 * h * each),
    )(at, seconds, grads)


def down_grads_kernel(at_ref, hidden_ref, c_ref, out_ref):
    turned = hidden_ref[0].T
    for y in range(2):
        out_ref[at_ref[0] ^ y, 0] = dot_nn(turned, c_ref[y]).astype(LOW)


def down_grads(at, hiddens, cots):
    _, length, h = cots.shape
    each = hiddens.shape[2]
    return pl.pallas_call(
        down_grads_kernel,
        out_shape=jax.ShapeDtypeStruct((2, 2, each, h), LOW),
        grid_spec=pltpu.PrefetchScalarGridSpec(
            num_scalar_prefetch=1,
            grid=(2, each // h),
            in_specs=[
                pl.BlockSpec((1, length, h), lambda c, b, at: (c, 0, b)),
                pl.BlockSpec((2, length, h), lambda c, b, at: (0, 0, 0)),
            ],
            out_specs=pl.BlockSpec((2, 1, h, h), lambda c, b, at: (0, at[1] ^ c, b, 0)),
        ),
        name="down_grads",
        cost_estimate=cost(8 * length * h * each, 4 * length * each + 8 * h * each),
    )(at, hiddens, cots)


def layer_end_kernel(at_ref, h0, h1, w00, w01, w10, w11, own_ref, theirs_ref):
    n = own_ref.shape[1] // 2
    for j, (a, b) in enumerate(((w00, w01), (w10, w11))):
        part = dot_nn(h0[0], a[0]) + dot_nn(h1[0], b[0])
        own_ref[:, j * n : (j + 1) * n] = part[:, :n]
        theirs_ref[:, j * n : (j + 1) * n] = part[:, n:].astype(LOW)


def layer_end(at, hiddens, weights):
    _, length, each = hiddens.shape
    h = weights.shape[2]
    out = pl.BlockSpec((TILE, h), lambda t, at: (t, 0))

    def rows(c):
        return pl.BlockSpec((1, TILE, each), lambda t, at: (c, t, 0))

    def weight(y, col):
        return pl.BlockSpec((1, each, h), lambda t, at: ((at[0] ^ y) * 2 + (at[1] ^ col), 1, 0))

    return pl.pallas_call(
        layer_end_kernel,
        out_shape=(jax.ShapeDtypeStruct((length, h), FULL), jax.ShapeDtypeStruct((length, h), LOW)),
        grid_spec=pltpu.PrefetchScalarGridSpec(
            num_scalar_prefetch=1,
            grid=(length // TILE,),
            in_specs=[rows(0), rows(1), weight(0, 0), weight(0, 1), weight(1, 0), weight(1, 1)],
            out_specs=(out, out),
        ),
        name="layer_end",
        cost_estimate=cost(8 * length * h * each, 8 * h * each + 12 * length * h),
    )(at, hiddens, hiddens, weights, weights, weights, weights)


def after(values, *late):
    return lax.optimization_barrier((values, late))[0]


def pick(pair, index):
    return lax.dynamic_index_in_dim(pair, index, 0, keepdims=False)


def ordered(own, other, index):
    flip = index == 0
    return jnp.stack((jnp.where(flip, own, other), jnp.where(flip, other, own)))


def swap_across(array):
    return lax.ppermute(array, ("y", "col"), [(0, 3), (3, 0), (1, 2), (2, 1)])


def plane_gather(block):
    return block, swap(block, "y"), swap(block, "col"), swap_across(block)


def plane_exchange(at_y, at_col, across):
    return swap(at_y, "y"), swap(at_col, "col"), swap_across(across)


def plane_sum(own, got):
    return (own.astype(FULL) + sum(g.astype(FULL) for g in got)).astype(LOW)


def add_low(left, right):
    return (left.astype(FULL) + right.astype(FULL)).astype(LOW)


PAIRS = [(0, 1), (1, 0), (2, 3), (3, 2)]
FAR = [(0, 2), (2, 0), (1, 3), (3, 1)]


def depth_pair(array, odd):
    halves = array.reshape(2, array.shape[0] // 2, array.shape[1])
    return add_low(pick(halves, odd), lax.ppermute(pick(halves, 1 - odd), "dp", PAIRS))


def depth_far(part):
    return add_low(part, lax.ppermute(part, "dp", FAR))


def depth_join(part, odd):
    return ordered(part, lax.ppermute(part, "dp", PAIRS), odd).reshape(-1, part.shape[1])


def half(weight, axis, index):
    size = weight.shape[axis] // 2
    return lax.dynamic_slice_in_dim(weight, index * size, size, axis)


def fast_body(
    inputs, gain_first, shift_first, w_query, w_key, w_value, w_output, gain_second, shift_second,
    w_up, bias_up, w_down, bias_down, segments, random_blocks, global_blocks, cotangent,
):
    depth_at, y_at, core_at, col_at = (lax.axis_index(name) for name in ("dp", "y", "core", "col"))
    length = segments.shape[1]
    n = inputs.shape[1]
    h = 2 * n
    at = jnp.stack((y_at, col_at)).astype(jnp.int32)

    def chip_block(weights, axis, join):
        mine = jnp.concatenate([half(w, axis, core_at) for w in weights], axis=axis)
        theirs = swap(jnp.concatenate([half(w, axis, 1 - core_at) for w in weights], axis=axis), "core")
        return jnp.concatenate((mine, theirs), axis=join)

    inputs_pair = inputs.reshape(2, length, n)
    x_own = pick(inputs_pair, y_at)
    x_y = swap(pick(inputs_pair, 1 - y_at), "y")
    qkv_block = chip_block((w_query, w_key, w_value), 1, 0)
    qkv_own, qkv_y, qkv_x, qkv_xy = plane_gather(qkv_block)
    xs = (x_own, swap(x_own, "core"), x_y, swap(x_y, "core"))
    w_up, w_down = after((w_up, w_down), qkv_block)
    up_block, down_block = chip_block((w_up,), 1, 0), chip_block((w_down,), 0, 1)
    ups = up_block.shape[1] // h
    ffn_block = jnp.concatenate([up_block[:, i * h : (i + 1) * h] for i in range(ups)] + [down_block])
    ffn_block, w_output, cotangent_late = after((ffn_block, w_output, cotangent), qkv_y, qkv_x)
    ffn = lax.all_gather(ffn_block, ("y", "col"), axis=0, tiled=False)
    out_own, out_y, out_x, out_xy = plane_gather(chip_block((w_output,), 0, 1))
    cot_pair = cotangent_late.reshape(2, length, n)

    vectors = jnp.stack((gain_first, shift_first, gain_second, shift_second, bias_down))
    vectors = jnp.concatenate((vectors, swap(vectors, "core")), axis=1)
    vectors = jnp.concatenate((vectors, swap(vectors, "y")), axis=1)
    gain_one, shift_one, gain_two, shift_two, bias_low = (vectors[i : i + 1] for i in range(5))
    heads_half = half(random_blocks, 0, core_at)
    hidden_bias = half(bias_up, 0, core_at)
    each = hidden_bias.shape[0]
    small = swap(jnp.concatenate((hidden_bias, heads_half.astype(FULL).reshape(-1))), "col")
    biases = jnp.concatenate((hidden_bias, small[:each]))
    heads_half_x = small[each:].reshape(heads_half.shape).astype(jnp.int32)
    moves = []
    for y in range(2):
        for core in range(2):
            for col in range(2):
                moves.append(((col * 2 + y) * 2 + core, (y * 2 + core) * 2 + col))
    labels = lax.ppermute(segments, ("y", "core", "col"), moves)[0]
    all_heads = jnp.concatenate((heads_half, heads_half_x), axis=0)
    rows_extra, keys_extra, where_table = attention_extras(labels, all_heads, global_blocks)
    near_heads = heads_half.shape[0]
    keys_of = (keys_extra[:near_heads], keys_extra[near_heads:])
    live = (labels != 0)[:, None]

    cot_own = pick(cot_pair, y_at)
    cot_y = swap(pick(cot_pair, 1 - y_at), "y")
    cot_swapped = swap(cot_y, "core")
    cots = jnp.stack([jnp.concatenate(c, axis=1) for c in ((cot_own, swap(cot_own, "core")), (cot_y, cot_swapped))])

    firsts = first_norm(xs, gain_one, shift_one)
    w_qkv = (jnp.concatenate((qkv_own, qkv_y), axis=0), jnp.concatenate((qkv_x, qkv_xy), axis=0))
    first = jnp.concatenate(firsts, axis=1)
    out_own = after(out_own, cot_y, cot_swapped)
    w_out = (jnp.concatenate((out_own, out_y), axis=1), jnp.concatenate((out_x, out_xy), axis=1))
    qkv, heads, kept = [], [], []
    for i in range(2):
        qkv.append(dot_nn(first, w_qkv[i]).astype(LOW))
        done, saved = attend_forward(qkv[i], rows_extra, keys_of[i], where_table)
        heads.append(done)
        kept.append(saved)
    mixed_part = mix_heads(heads, w_out)
    residual, seconds = second_norm(xs, mixed_part, swap(mixed_part, "core"), gain_two, shift_two)

    second_part, hiddens, up_sides, bias_sum = feed_forward(at, seconds, cots, ffn, biases)
    down_parts = down_grads(at, hiddens, cots).reshape(4, -1, h)
    down_scattered = lax.psum_scatter(down_parts, ("y", "col"), scatter_dimension=0, tiled=True)[0]
    up_parts = up_grads(at, seconds, after(up_sides, down_parts))
    up_scattered = lax.psum_scatter(up_parts, ("y", "col"), scatter_dimension=0, tiled=True)[0]
    second_got = after(swap(second_part, "core"), up_parts)

    grad_own, grad_other, grad_mixed, sums_two = second_norm_back(residual, second_part, second_got, cots, gain_two)
    grads = jnp.where(live, dot_nt(grad_mixed, jnp.concatenate(w_out, axis=0)), 0.0).astype(LOW)
    out_grads = [[dot_tn(grad_mixed[:, j * h : (j + 1) * h], head).astype(LOW) for j in range(2)] for head in heads]
    qkv_sides, qkv_grads = [None, None], [None, None]
    for i in (1, 0):
        qkv_sides[i] = attend_backward(kept[i], qkv[i], keys_of[i], heads[i], grads, i, where_table)
        qkv_grads[i] = [dot_tn(f, qkv_sides[i]).astype(LOW) for f in firsts]
    odd = lax.rem(depth_at, 2)
    out_got = plane_exchange(out_grads[0][1], out_grads[1][0], out_grads[1][1])
    qkv_got = plane_exchange(qkv_grads[0][1], qkv_grads[1][0], qkv_grads[1][1])
    qkv_sides = after(qkv_sides, qkv_grads)
    first_part = dot_nt(jnp.concatenate(qkv_sides, axis=1), jnp.concatenate(w_qkv, axis=1)).astype(LOW)
    first_part = after(first_part, out_got)
    mine, theirs, sums_one = first_norm_back(xs, first_part, swap(first_part, "core"), grad_own, grad_other, gain_one)
    grad_inputs = ordered(mine, swap(theirs, "y").astype(FULL), y_at).reshape(2 * length, n)
    down_part = depth_pair(after(down_scattered, qkv_grads[0]), odd)

    ends_own, ends_other = layer_end(at, after(hiddens, sums_one, down_part), ffn)
    residual, up_scattered, down_part = lax.optimization_barrier((residual, up_scattered, down_part, ends_own))[:3]
    up_total = lax.psum(up_scattered, "dp")
    down_part = depth_far(down_part)
    kept_two = jnp.concatenate((residual[:, :n], residual[:, 2 * n : 3 * n]), axis=1)
    bias_two = jnp.concatenate((bias_low[:, :n], bias_low[:, 2 * n : 3 * n]), axis=1)
    ends = (kept_two + ends_own + swap(ends_other, "core").astype(FULL) + bias_two).astype(LOW)
    layer_out = ordered(ends[:, :n], swap(ends[:, n:], "y"), y_at).reshape(2 * length, n)

    gains = jnp.concatenate((sums_one[:2, :n], sums_two[:2, :n])).reshape(-1)
    gains_y = jnp.concatenate((sums_one[:2, n:], sums_two[:2, n:])).reshape(-1)
    up_bias = bias_sum[:, 0, :].reshape(-1)
    got = swap(jnp.concatenate((gains_y, up_bias)), "y")
    gains = gains + got[: 4 * n]
    up_bias = up_bias + got[4 * n :]
    near = jnp.concatenate((gains, jnp.sum(cotangent, axis=0, dtype=FULL), up_bias[:each]))
    near = near + swap(jnp.concatenate((near[: 5 * n], up_bias[each:])), "col")
    near = near + lax.ppermute(near, "dp", [(0, 1), (1, 0), (2, 3), (3, 2)])
    near = near + lax.ppermute(near, "dp", [(0, 2), (2, 0), (1, 3), (3, 1)])
    gains = near[: 5 * n].reshape(5, n)
    up_bias = ordered(near[5 * n :], swap(near[5 * n :], "core"), core_at).reshape(-1)

    def finish(total, axis, parts):
        keep = lax.slice_in_dim(total, 0, n, axis=axis)
        got = swap(lax.slice_in_dim(total, n, 2 * n, axis=axis), "core")
        size = keep.shape[1 - axis] // parts
        flip = core_at == 0
        out = []
        for i in range(parts):
            a, b = (lax.slice_in_dim(z, i * size, (i + 1) * size, axis=1 - axis) for z in (keep, got))
            out.append(jnp.concatenate((jnp.where(flip, a, b), jnp.where(flip, b, a)), axis=1 - axis).astype(FULL))
        return out

    four = jnp.concatenate(
        (plane_sum(after(qkv_grads[0][0], up_scattered), qkv_got), plane_sum(out_grads[0][0], out_got)), axis=1
    )
    four = depth_pair(four, odd)
    down_total = depth_join(after(down_part, four), odd)
    four = depth_join(depth_far(four), odd)
    grad_query, grad_key, grad_value, grad_out = finish(four, 0, 4)
    (grad_down,) = finish(down_total, 1, 1)
    (grad_up,) = finish(jnp.concatenate([up_total[i * h : (i + 1) * h] for i in range(ups)], axis=1), 0, 1)
    return (
        layer_out, grad_inputs, gains[0], gains[1], grad_query, grad_key, grad_value, grad_out.T, gains[2], gains[3],
        grad_up, up_bias, grad_down, gains[4],
    )


def whole_sequences(mesh):
    return mesh.shape["row"] == 4 and mesh.shape["col"] == 2 and mesh.shape["dp"] == 4


def placements(row):
    tokens = P(("dp", "col"), row)
    rows = P(row)
    weight = P(row, "col")
    turned = P("col", row)
    placed = (
        tokens, rows, rows, weight, weight, weight, turned, rows, rows, weight, P("col"), turned, rows,
        P(("dp", *row), None), P("col", None, None), P(), tokens,
    )
    given = (
        tokens, tokens, rows, rows, weight, weight, weight, turned, rows, rows, weight, P("col"), turned, rows,
    )
    return placed, given


def solution(mesh):
    sizes = mesh.shape
    split = jax.sharding.Mesh(
        mesh.devices.reshape(sizes["dp"], sizes["row"] // 2, 2, sizes["col"]), ("dp", "y", "core", "col")
    )

    def run(*arrays):
        tokens, length = arrays[0].shape[0], arrays[13].shape[1]
        if whole_sequences(mesh) and tokens == sizes["dp"] * sizes["col"] * 2 * length:
            placed, given = placements(("y", "core"))
            step = jax.shard_map(fast_body, mesh=split, in_specs=placed, out_specs=given, check_vma=False)
        else:
            placed, given = placements(("row",))
            step = jax.shard_map(body, mesh=mesh, in_specs=placed, out_specs=given, check_vma=False)
        return step(*arrays)

    return run
```

```python
import math

import jax
import jax.numpy as jnp
from jax import lax
from jax.experimental import pallas as pl
from jax.experimental.pallas import tpu as pltpu
from jax.sharding import PartitionSpec as P

D = 1024
HD = 64
BLK = 64
NB = 16


EPS = 1e-05


def product(picked, weight, flipped):
    if flipped:
        return lax.dot_general(
            picked, weight, (((1,), (1,)), ((), ())), preferred_element_type=jnp.float32
        )
    return jnp.dot(picked, weight, preferred_element_type=jnp.float32)


def to_columns(moving, weight, flipped):
    gathered = lax.all_gather(moving, "col", axis=0, tiled=True)
    row_count = gathered.shape[0] // lax.axis_size("row")

    def term_rows(first_row, how_many):
        return product(gathered, weight, flipped)

    result = lax.psum_scatter(
        term_rows(jnp.int32(0), lax.axis_size("row") * row_count),
        "row",
        scatter_dimension=0,
        tiled=True,
    )
    return (result, gathered)


def to_rows(moving, weight, flipped):
    gathered = lax.all_gather(moving, "row", axis=0, tiled=True)
    row_count = gathered.shape[0] // lax.axis_size("col")

    def term_rows(first_row, how_many):
        return product(gathered, weight, flipped)

    return (
        lax.psum_scatter(
            term_rows(jnp.int32(0), lax.axis_size("col") * row_count),
            "col",
            scatter_dimension=0,
            tiled=True,
        ),
        gathered,
    )


def norm_sums(first_sum, second_sum):
    return lax.psum((first_sum, second_sum), "row")


def norm_forward(moving, gain_row, shift_row):
    totals, squares = norm_sums(jnp.sum(moving, axis=1), jnp.sum(moving * moving, axis=1))
    center = totals / D
    spread = squares / D - center * center
    inverse = lax.rsqrt(spread + EPS)
    normed = (moving - center[:, None]) * inverse[:, None]
    return (normed * gain_row + shift_row, normed, inverse)


def norm_backward(upstream, normed, inverse, gain_row):
    scaled = upstream * gain_row
    first_sum, second_sum = norm_sums(jnp.sum(scaled, axis=1), jnp.sum(scaled * normed, axis=1))
    return inverse[:, None] * (scaled - first_sum[:, None] / D - normed * (second_sum[:, None] / D))


def head_masks(random_blocks, global_blocks):
    block_ids = jnp.arange(NB, dtype=jnp.int32)
    nearby = jnp.abs(block_ids[:, None] - block_ids[None, :]) <= 1
    chosen = jnp.any(random_blocks[:, :, :, None] == block_ids[None, None, None, :], axis=2)
    marked = jnp.any(global_blocks[:, None] == block_ids[None, :], axis=0)
    block_table = nearby[None] | chosen | marked[None, None, :] | marked[None, :, None]
    return jnp.repeat(jnp.repeat(block_table, BLK, axis=1), BLK, axis=2)


def seq_logits(seq_queries, seq_keys, labels, pattern):
    same_doc = (labels[:, None] == labels[None, :]) & (labels[None, :] != 0)
    raw_scores = jnp.einsum(
        "qhd,khd->hqk", seq_queries, seq_keys, preferred_element_type=jnp.float32
    )
    return jnp.where(pattern & same_doc[None], raw_scores * (1.0 / math.sqrt(HD)), -1000000000.0)


def attend_plain(queries, key_block, value_block, segments, pattern):

    def one_seq(pieces):
        seq_queries, seq_keys, seq_values, labels = pieces
        logits = seq_logits(seq_queries, seq_keys, labels, pattern)
        row_peak = jnp.max(logits, axis=2, keepdims=True)
        exp_terms = jnp.exp(logits - row_peak)
        row_total = jnp.sum(exp_terms, axis=2, keepdims=True)
        softmax = (exp_terms / row_total).astype(jnp.bfloat16)
        attended = jnp.einsum(
            "hqk,khd->qhd", softmax, seq_values, preferred_element_type=jnp.float32
        )
        live_rows = (labels != 0).astype(jnp.float32)
        return (attended * live_rows[:, None, None], (row_peak + jnp.log(row_total))[:, :, 0])

    return lax.map(one_seq, (queries, key_block, value_block, segments))


def attend_plain_backward(queries, key_block, value_block, segments, pattern, grad_heads, log_total):

    def one_seq(pieces):
        seq_queries, seq_keys, seq_values, labels, seq_grads, seq_log = pieces
        logits = seq_logits(seq_queries, seq_keys, labels, pattern)
        softmax = jnp.exp(logits - seq_log[:, :, None])
        grad_probs = jnp.einsum(
            "qhd,khd->hqk", seq_grads, seq_values, preferred_element_type=jnp.float32
        )
        grad_values = jnp.einsum(
            "hqk,qhd->khd",
            softmax.astype(jnp.bfloat16),
            seq_grads,
            preferred_element_type=jnp.float32,
        )
        inner_sum = jnp.sum(softmax * grad_probs, axis=2, keepdims=True)
        grad_raw = (softmax * (grad_probs - inner_sum) * (1.0 / math.sqrt(HD))).astype(jnp.bfloat16)
        grad_queries = jnp.einsum(
            "hqk,khd->qhd", grad_raw, seq_keys, preferred_element_type=jnp.float32
        )
        grad_keys = jnp.einsum(
            "hqk,qhd->khd", grad_raw, seq_queries, preferred_element_type=jnp.float32
        )
        return (grad_queries, grad_keys, grad_values)

    return lax.map(one_seq, (queries, key_block, value_block, segments, grad_heads, log_total))


def gelu_tanh(values):
    return jax.nn.gelu(values, approximate=True)


def weight_grad(left, right):
    return lax.dot_general(
        left, right, (((0,), (0,)), ((), ())), preferred_element_type=jnp.float32
    )


def body(
    inputs,
    gain_first,
    shift_first,
    w_query,
    w_key,
    w_value,
    w_output,
    gain_second,
    shift_second,
    w_up,
    bias_up,
    w_down,
    bias_down,
    segments,
    random_blocks,
    global_blocks,
    cotangent,
):
    seq_count, seq_len = segments.shape
    head_width = w_query.shape[1]
    heads_here = random_blocks.shape[0]
    seq_shape = (seq_count, seq_len, heads_here, HD)
    pattern = head_masks(random_blocks, global_blocks)
    live_tokens = (segments != 0).reshape(-1)
    x_first = inputs.astype(jnp.float32)
    first_full, normed_one, inverse_one = norm_forward(x_first, gain_first, shift_first)
    first_low = first_full.astype(jnp.bfloat16)
    stacked = jnp.concatenate((w_query, w_key, w_value), axis=1)
    projected, first_all = to_columns(first_low, stacked, False)
    proj_low = projected.astype(jnp.bfloat16)
    queries = proj_low[:, :head_width].reshape(seq_shape)
    key_block = proj_low[:, head_width : 2 * head_width].reshape(seq_shape)
    value_block = proj_low[:, 2 * head_width :].reshape(seq_shape)
    heads_out, log_total = attend_plain(queries, key_block, value_block, segments, pattern)
    heads_low = heads_out.reshape(-1, head_width).astype(jnp.bfloat16)
    mixed_out, heads_all = to_rows(heads_low, w_output, False)
    residual = x_first + mixed_out
    second_full, normed_two, inverse_two = norm_forward(residual, gain_second, shift_second)
    second_low = second_full.astype(jnp.bfloat16)
    upward, second_all = to_columns(second_low, w_up, False)
    upward = upward + bias_up
    hidden_low = gelu_tanh(upward).astype(jnp.bfloat16)
    downward, hidden_all = to_rows(hidden_low, w_down, False)
    layer_out = (residual + (downward + bias_down)).astype(jnp.bfloat16)
    grad_hidden, cotangent_all = to_columns(cotangent, w_down, True)
    activated, pull_back = jax.vjp(gelu_tanh, upward)
    grad_upward = pull_back(grad_hidden)[0].astype(jnp.bfloat16)
    grad_second, grad_upward_all = to_rows(grad_upward, w_up, True)
    grad_residual = cotangent.astype(jnp.float32) + norm_backward(
        grad_second, normed_two, inverse_two, gain_second
    )
    grad_mixed = grad_residual.astype(jnp.bfloat16)
    grad_heads, grad_mixed_all = to_columns(grad_mixed, w_output, True)
    grad_heads = jnp.where(live_tokens[:, None], grad_heads, 0.0).astype(jnp.bfloat16)
    grad_queries, grad_keys, grad_values = attend_plain_backward(
        queries, key_block, value_block, segments, pattern, grad_heads.reshape(seq_shape), log_total
    )
    grad_proj = jnp.concatenate(
        (
            grad_queries.reshape(-1, head_width),
            grad_keys.reshape(-1, head_width),
            grad_values.reshape(-1, head_width),
        ),
        axis=1,
    ).astype(jnp.bfloat16)
    grad_first, grad_proj_all = to_rows(grad_proj, stacked, True)
    grad_inputs = grad_residual + norm_backward(grad_first, normed_one, inverse_one, gain_first)
    grad_stacked = weight_grad(first_all, grad_proj_all)
    grad_out_weight = weight_grad(heads_all, grad_mixed_all)
    grad_up_weight = weight_grad(second_all, grad_upward_all)
    grad_down_weight = weight_grad(hidden_all, cotangent_all)
    grad_up_bias = jnp.sum(grad_upward_all, axis=0, dtype=jnp.float32)
    grad_down_bias = jnp.sum(cotangent_all, axis=0, dtype=jnp.float32)
    gain_terms = lax.psum(
        (
            jnp.sum(grad_first * normed_one, axis=0),
            jnp.sum(grad_first, axis=0),
            jnp.sum(grad_second * normed_two, axis=0),
            jnp.sum(grad_second, axis=0),
        ),
        ("dp", "col"),
    )
    summed = (
        lax.psum(grad_stacked.astype(jnp.bfloat16), "dp").astype(jnp.float32),
        lax.psum(grad_out_weight.astype(jnp.bfloat16), "dp").astype(jnp.float32),
        lax.psum(grad_up_weight.astype(jnp.bfloat16), "dp").astype(jnp.float32),
        lax.psum(grad_down_weight.astype(jnp.bfloat16), "dp").astype(jnp.float32),
        lax.psum(grad_up_bias.astype(jnp.bfloat16), "dp").astype(jnp.float32),
        lax.psum(grad_down_bias.astype(jnp.bfloat16), "dp").astype(jnp.float32),
    )
    return (
        layer_out,
        grad_inputs,
        gain_terms[0],
        gain_terms[1],
        summed[0][:, :head_width],
        summed[0][:, head_width : 2 * head_width],
        summed[0][:, 2 * head_width :],
        summed[1],
        gain_terms[2],
        gain_terms[3],
        summed[2],
        summed[4],
        summed[3],
        summed[5],
    )


SWAP = [(0, 1), (1, 0)]
LOW = jnp.bfloat16
FULL = jnp.float32
TILE = 256
BIG = 1e30


def swap(array, axis):
    return lax.ppermute(array, axis, SWAP)


def dot_nn(left, right):
    return lax.dot_general(left, right, (((1,), (0,)), ((), ())), preferred_element_type=FULL)


def dot_nt(left, right):
    return lax.dot_general(left, right, (((1,), (1,)), ((), ())), preferred_element_type=FULL)


def dot_tn(left, right):
    return lax.dot_general(left, right, (((0,), (0,)), ((), ())), preferred_element_type=FULL)


def attention_extras(labels, random_blocks, global_blocks):
    length = labels.shape[0]
    blocks = length // BLK
    block_ids = jnp.arange(blocks, dtype=jnp.int32)
    nearby = jnp.abs(block_ids[:, None] - block_ids[None, :]) <= 1
    chosen = jnp.any(random_blocks[:, :, :, None] == block_ids[None, None, None, :], axis=2)
    marked = jnp.any(global_blocks[:, None] == block_ids[None, :], axis=0)
    table = nearby[None] | chosen | marked[None, None, :] | marked[None, :, None]
    heads = table.shape[0]
    lane = jnp.arange(HD, dtype=jnp.int32)
    place = jnp.arange(length, dtype=jnp.int32) // BLK
    doc_lane = blocks + jnp.where(labels == 0, 4, labels - 1)
    row_extra = ((lane[None, :] == place[:, None]) | (lane[None, :] == doc_lane[:, None])).astype(LOW)
    table_keys = jnp.pad(jnp.swapaxes(table, 1, 2), ((0, 0), (0, 0), (0, HD - blocks)), constant_values=True)
    table_keys = jnp.repeat(table_keys, BLK, axis=1)
    is_doc = (lane >= blocks) & (lane <= blocks + 4)
    doc_bad = is_doc[None, :] & (lane[None, :] != doc_lane[:, None])
    doc_bad = doc_bad | (lane[None, :] == blocks + 4)
    key_extra = jnp.where(table_keys & ~doc_bad[None], 0.0, -BIG)
    key_extra = jnp.where((lane >= blocks + 5) & (lane <= blocks + 7), 1.0, key_extra).astype(LOW)
    rows = jnp.stack((jnp.pad(row_extra, ((0, 0), (HD, 0))), jnp.pad(row_extra, ((0, 0), (0, HD)))))
    even = jnp.pad(key_extra[0::2], ((0, 0), (0, 0), (HD, 0)))
    odd = jnp.pad(key_extra[1::2], ((0, 0), (0, 0), (0, HD)))
    keys = jnp.stack((even, odd), axis=1).reshape(heads, length, 2 * HD)
    tiles = length // TILE
    known = labels[None, :] == jnp.arange(1, 5, dtype=jnp.int32)[:, None]
    present = jnp.any(known.reshape(4, tiles, TILE), axis=2)
    wanted = jnp.any(present[:, :, None] & known[:, None, :], axis=0)
    spots = jnp.arange(length, dtype=jnp.int32)
    first = jnp.min(jnp.where(wanted, spots[None, :], length - 1), axis=1)
    last = jnp.max(jnp.where(wanted, spots[None, :], 0), axis=1)
    start = first // 128
    count = jnp.maximum((last + 1 - start * 128 + 255) // 256, 1)
    start = jnp.minimum(start, length // 128 - 2 * count)
    return rows, keys, jnp.stack((start, count)).astype(jnp.int32)


def attend_forward_kernel(where_ref, q_ref, k_ref, v_ref, rows_ref, keys_ref, out_ref, kept_ref, kk, vv):
    length = q_ref.shape[0]
    lane = lax.broadcasted_iota(jnp.int32, (length, 2 * HD), 1)
    for e in range(2):
        data = (lane < HD) if e == 0 else (lane >= HD)
        kk[e] = jnp.where(data, k_ref[...], keys_ref[e])
        vv[e] = jnp.where(data, v_ref[...], jnp.ones_like(v_ref[...]))
    tile_lane = lax.broadcasted_iota(jnp.int32, (TILE, 2 * HD), 1)

    def one_tile(t, carry):
        rows = pl.ds(pl.multiple_of(t * TILE, TILE), TILE)
        start = pl.multiple_of(where_ref[0, t] * 128, 128)
        count = where_ref[1, t]
        q_pair = q_ref[rows, :] * jnp.bfloat16(1.0 / math.sqrt(HD))
        for n in range(1, length // TILE + 1):

            @pl.when(count == n)
            def _():
                span = pl.ds(start, n * TILE)
                outs = []
                for e in range(2):
                    data = (tile_lane < HD) if e == 0 else (tile_lane >= HD)
                    base = HD if e == 0 else 0
                    extra = rows_ref[e, rows, :]
                    q_one = jnp.where(data, q_pair, extra)
                    logits = dot_nt(q_one, kk[e, span, :])
                    peak = jnp.max(logits, axis=1, keepdims=True)
                    terms = jnp.exp(logits - peak)
                    mixed = dot_nn(terms.astype(LOW), vv[e, span, :])
                    total = pltpu.roll(mixed, HD, 1)
                    outs.append(mixed / total)
                    total_one = jnp.max(jnp.where(data, total, 0.0), axis=1, keepdims=True)
                    padded = jnp.max(
                        jnp.where(tile_lane == base + 20, extra.astype(FULL), 0.0), axis=1, keepdims=True
                    )
                    log_total = jnp.where(padded > 0.5, 0.0, -(peak + jnp.log(total_one)))
                    high = log_total.astype(LOW).astype(FULL)
                    middle = (log_total - high).astype(LOW).astype(FULL)
                    low = log_total - high - middle
                    packed = jnp.where(tile_lane == base + 21, high, q_one.astype(FULL))
                    packed = jnp.where(tile_lane == base + 22, middle, packed)
                    packed = jnp.where(tile_lane == base + 23, low, packed)
                    kept_ref[e, rows, :] = packed.astype(LOW)
                joined = jnp.where(tile_lane < HD, outs[0], outs[1])
                out_ref[rows, :] = jnp.where(padded > 0.5, 0.0, joined).astype(LOW)

        return carry

    lax.fori_loop(0, length // TILE, one_tile, 0)


def attend_forward(qkv, rows_extra, keys_extra, where_table):
    length, width = qkv.shape
    pairs = width // (3 * 2 * HD)
    wide = 2 * HD
    return pl.pallas_call(
        attend_forward_kernel,
        out_shape=(
            jax.ShapeDtypeStruct((length, width // 3), LOW),
            jax.ShapeDtypeStruct((2 * pairs, length, wide), LOW),
        ),
        grid_spec=pltpu.PrefetchScalarGridSpec(
            num_scalar_prefetch=1,
            grid=(pairs,),
            in_specs=[
                pl.BlockSpec((length, wide), lambda p, w: (0, p)),
                pl.BlockSpec((length, wide), lambda p, w: (0, pairs + p)),
                pl.BlockSpec((length, wide), lambda p, w: (0, 2 * pairs + p)),
                pl.BlockSpec((2, length, wide), lambda p, w: (0, 0, 0)),
                pl.BlockSpec((2, length, wide), lambda p, w: (p, 0, 0)),
            ],
            out_specs=(
                pl.BlockSpec((length, wide), lambda p, w: (0, p)),
                pl.BlockSpec((2, length, wide), lambda p, w: (p, 0, 0)),
            ),
            scratch_shapes=[pltpu.VMEM((2, length, wide), LOW), pltpu.VMEM((2, length, wide), LOW)],
        ),
        name="attend_forward",
        cost_estimate=pl.CostEstimate(
            flops=8 * pairs * length * length * HD, bytes_accessed=16 * length * width, transcendentals=0
        ),
    )(where_table, qkv, qkv, qkv, rows_extra, keys_extra)


def attend_backward_kernel(
    where_ref, kept_ref, k_ref, v_ref, keys_ref, heads_ref, grads_ref, out_ref, kk, va, dk_sum, dv_sum
):
    length = k_ref.shape[0]
    wide = 2 * HD
    third = out_ref.shape[1] // 3
    pair = pl.program_id(0) * wide
    lane = lax.broadcasted_iota(jnp.int32, (length, wide), 1)
    for e in range(2):
        data = (lane < HD) if e == 0 else (lane >= HD)
        base = HD if e == 0 else 0
        kk[e] = jnp.where(data, k_ref[...], keys_ref[e])
        ones = jnp.where((lane == base) | (lane == base + 1), 1.0, 0.0).astype(LOW)
        va[e] = jnp.where(data, v_ref[...], ones)
    dk_sum[...] = jnp.zeros_like(dk_sum)
    dv_sum[...] = jnp.zeros_like(dv_sum)
    tile_lane = lax.broadcasted_iota(jnp.int32, (TILE, wide), 1)

    def one_tile(t, carry):
        rows = pl.ds(pl.multiple_of(t * TILE, TILE), TILE)
        start = pl.multiple_of(where_ref[0, t] * 128, 128)
        count = where_ref[1, t]
        grads = grads_ref[rows, :]
        both = grads.astype(FULL) * heads_ref[rows, :].astype(FULL)
        for n in range(1, length // TILE + 1):

            @pl.when(count == n)
            def _():
                span = pl.ds(start, n * TILE)
                outs = []
                for e in range(2):
                    data = (tile_lane < HD) if e == 0 else (tile_lane >= HD)
                    base = HD if e == 0 else 0
                    inner = -jnp.sum(jnp.where(data, both, 0.0), axis=1, keepdims=True)
                    high = inner.astype(LOW).astype(FULL)
                    only = jnp.where(data, grads, jnp.zeros_like(grads))
                    packed = jnp.where(tile_lane == base, high, only.astype(FULL))
                    packed = jnp.where(tile_lane == base + 1, inner - high, packed).astype(LOW)
                    q_one = kept_ref[e, rows, :]
                    q_only = jnp.where(data, q_one, jnp.zeros_like(q_one))
                    probs = jnp.exp(dot_nt(kk[e, span, :], q_one))
                    grad_raw = (probs * dot_nt(va[e, span, :], packed)).astype(LOW)
                    dv_sum[span, :] += dot_nn(probs.astype(LOW), only)
                    dk_sum[span, :] += dot_nn(grad_raw, q_only)
                    outs.append(dot_tn(grad_raw, kk[e, span, :]))
                joined = jnp.where(tile_lane < HD, outs[0], outs[1])
                lanes = pl.ds(pl.multiple_of(pair, wide), wide)
                out_ref[rows, lanes] = (joined * (1.0 / math.sqrt(HD))).astype(LOW)

        return carry

    lax.fori_loop(0, length // TILE, one_tile, 0)
    out_ref[:, pl.ds(pl.multiple_of(third + pair, wide), wide)] = dk_sum[...].astype(LOW)
    out_ref[:, pl.ds(pl.multiple_of(2 * third + pair, wide), wide)] = dv_sum[...].astype(LOW)


def attend_backward(kept, qkv, keys_extra, heads, grads, group, where_table):
    length, width = qkv.shape
    pairs = width // (3 * 2 * HD)
    wide = 2 * HD
    stacked = pl.BlockSpec((2, length, wide), lambda p, w: (p, 0, 0))
    return pl.pallas_call(
        attend_backward_kernel,
        out_shape=jax.ShapeDtypeStruct((length, width), LOW),
        grid_spec=pltpu.PrefetchScalarGridSpec(
            num_scalar_prefetch=1,
            grid=(pairs,),
            in_specs=[
                stacked,
                pl.BlockSpec((length, wide), lambda p, w: (0, pairs + p)),
                pl.BlockSpec((length, wide), lambda p, w: (0, 2 * pairs + p)),
                stacked,
                pl.BlockSpec((length, wide), lambda p, w: (0, p)),
                pl.BlockSpec((length, wide), lambda p, w: (0, group * pairs + p)),
            ],
            out_specs=pl.BlockSpec((length, width), lambda p, w: (0, 0)),
            scratch_shapes=[
                pltpu.VMEM((2, length, wide), LOW),
                pltpu.VMEM((2, length, wide), LOW),
                pltpu.VMEM((length, wide), FULL),
                pltpu.VMEM((length, wide), FULL),
            ],
        ),
        name="attend_backward",
        cost_estimate=pl.CostEstimate(
            flops=20 * pairs * length * length * HD, bytes_accessed=20 * length * width, transcendentals=0
        ),
    )(where_table, kept, qkv, qkv, keys_extra, heads, grads)


def row_tiles(count):
    def spec(width):
        return pl.BlockSpec((TILE, width), lambda t: (t, 0))

    return spec


def whole(shape):
    return pl.BlockSpec(shape, lambda t: (0,) * len(shape))


def cost(flops, moved):
    return pl.CostEstimate(flops=int(flops), bytes_accessed=int(moved), transcendentals=0)


def norm_parts(blocks):
    width = sum(b.shape[1] for b in blocks)
    total = sum(jnp.sum(b, axis=1, keepdims=True) for b in blocks)
    squares = sum(jnp.sum(b * b, axis=1, keepdims=True) for b in blocks)
    center = total / width
    return center, lax.rsqrt(squares / width - center * center + EPS)


def columns(ref, index, width):
    return ref[:, index * width : (index + 1) * width]


def first_norm_kernel(x0, x1, x2, x3, gain_ref, shift_ref, low_ref, high_ref):
    blocks = [x[...].astype(FULL) for x in (x0, x1, x2, x3)]
    n = blocks[0].shape[1]
    center, inverse = norm_parts(blocks)
    for i, block in enumerate(blocks):
        value = (block - center) * inverse * columns(gain_ref, i, n) + columns(shift_ref, i, n)
        (low_ref, high_ref)[i // 2][:, (i % 2) * n : (i % 2 + 1) * n] = value.astype(LOW)


def first_norm(blocks, gain, shift):
    length, n = blocks[0].shape
    rows = row_tiles(length)
    half = jax.ShapeDtypeStruct((length, 2 * n), LOW)
    return pl.pallas_call(
        first_norm_kernel,
        out_shape=(half, half),
        grid=(length // TILE,),
        in_specs=[rows(n)] * 4 + [whole((1, 4 * n))] * 2,
        out_specs=(rows(2 * n), rows(2 * n)),
        name="first_norm",
        cost_estimate=cost(20 * length * n, 16 * length * n),
    )(*blocks, gain, shift)


def second_norm_kernel(x0, x1, x2, x3, part_ref, got_ref, gain_ref, shift_ref, residual_ref, second_ref):
    n = x0.shape[1]
    blocks = []
    for i, x in enumerate((x0, x1, x2, x3)):
        mixed = columns(part_ref, i, n).astype(FULL) + columns(got_ref, i ^ 1, n).astype(FULL)
        blocks.append(x[...].astype(FULL) + mixed)
    center, inverse = norm_parts(blocks)
    for i, block in enumerate(blocks):
        residual_ref[:, i * n : (i + 1) * n] = block
        value = (block - center) * inverse * columns(gain_ref, i, n) + columns(shift_ref, i, n)
        second_ref[i // 2, :, (i % 2) * n : (i % 2 + 1) * n] = value.astype(LOW)


def second_norm(blocks, part, got, gain, shift):
    length, n = blocks[0].shape
    rows = row_tiles(length)
    return pl.pallas_call(
        second_norm_kernel,
        out_shape=(jax.ShapeDtypeStruct((length, 4 * n), FULL), jax.ShapeDtypeStruct((2, length, 2 * n), LOW)),
        grid=(length // TILE,),
        in_specs=[rows(n)] * 4 + [rows(4 * n)] * 2 + [whole((1, 4 * n))] * 2,
        out_specs=(rows(4 * n), pl.BlockSpec((2, TILE, 2 * n), lambda t: (0, t, 0))),
        name="second_norm",
        cost_estimate=cost(30 * length * n, 48 * length * n),
    )(*blocks, part, got, gain, shift)


def norm_gradient(blocks, part_ref, got_ref, gain_ref, sums_ref):
    n = blocks[0].shape[1]
    center, inverse = norm_parts(blocks)
    normed = [(b - center) * inverse for b in blocks]
    grads = [columns(part_ref, i, n).astype(FULL) + columns(got_ref, i ^ 1, n).astype(FULL) for i in range(4)]
    scaled = [g * columns(gain_ref, i, n) for i, g in enumerate(grads)]
    mean_one = sum(jnp.sum(s, axis=1, keepdims=True) for s in scaled) / (4 * n)
    mean_two = sum(jnp.sum(s * z, axis=1, keepdims=True) for s, z in zip(scaled, normed)) / (4 * n)

    @pl.when(pl.program_id(0) == 0)
    def _():
        sums_ref[...] = jnp.zeros_like(sums_ref)

    for slot, i in enumerate((0, 2)):
        place = slice(slot * n, (slot + 1) * n)
        sums_ref[0:1, place] += jnp.sum(grads[i] * normed[i], axis=0, keepdims=True)
        sums_ref[1:2, place] += jnp.sum(grads[i], axis=0, keepdims=True)
    return [inverse * (s - mean_one - z * mean_two) for s, z in zip(scaled, normed)]


def second_norm_back_kernel(
    residual_ref, part_ref, got_ref, cots_ref, gain_ref, own_ref, other_ref, mixed_ref, sums_ref
):
    n = residual_ref.shape[1] // 4
    blocks = [columns(residual_ref, i, n) for i in range(4)]
    for i, grad in enumerate(norm_gradient(blocks, part_ref, got_ref, gain_ref, sums_ref)):
        total = cots_ref[i // 2, :, (i % 2) * n : (i % 2 + 1) * n].astype(FULL) + grad
        mixed_ref[:, i * n : (i + 1) * n] = total.astype(LOW)
        if i % 2 == 0:
            (own_ref, other_ref)[i // 2][...] = total


def second_norm_back(residual, part, got, cots, gain):
    length, width = residual.shape
    n = width // 4
    rows = row_tiles(length)
    one = jax.ShapeDtypeStruct((length, n), FULL)
    return pl.pallas_call(
        second_norm_back_kernel,
        out_shape=(one, one, jax.ShapeDtypeStruct((length, width), LOW), jax.ShapeDtypeStruct((8, 2 * n), FULL)),
        grid=(length // TILE,),
        in_specs=[rows(width)] * 3 + [pl.BlockSpec((2, TILE, 2 * n), lambda t: (0, t, 0)), whole((1, width))],
        out_specs=(rows(n), rows(n), rows(width), whole((8, 2 * n))),
        name="second_norm_back",
        cost_estimate=cost(60 * length * n, 64 * length * n),
    )(residual, part, got, cots, gain)


def first_norm_back_kernel(
    x0, x1, x2, x3, part_ref, got_ref, own_ref, other_ref, gain_ref, mine_ref, theirs_ref, sums_ref
):
    blocks = [x[...].astype(FULL) for x in (x0, x1, x2, x3)]
    grads = norm_gradient(blocks, part_ref, got_ref, gain_ref, sums_ref)
    mine_ref[...] = own_ref[...] + grads[0]
    theirs_ref[...] = (other_ref[...] + grads[2]).astype(LOW)


def first_norm_back(blocks, part, got, own, other, gain):
    length, n = blocks[0].shape
    rows = row_tiles(length)
    return pl.pallas_call(
        first_norm_back_kernel,
        out_shape=(
            jax.ShapeDtypeStruct((length, n), FULL),
            jax.ShapeDtypeStruct((length, n), LOW),
            jax.ShapeDtypeStruct((8, 2 * n), FULL),
        ),
        grid=(length // TILE,),
        in_specs=[rows(n)] * 4 + [rows(4 * n)] * 2 + [rows(n)] * 2 + [whole((1, 4 * n))],
        out_specs=(rows(n), rows(n), whole((8, 2 * n))),
        name="first_norm_back",
        cost_estimate=cost(60 * length * n, 40 * length * n),
    )(*blocks, part, got, own, other, gain)


def mix_kernel(h0, h1, w0, w1, out_ref):
    out_ref[...] = (dot_nn(h0[...], w0[...]) + dot_nn(h1[...], w1[...])).astype(LOW)


def mix_heads(heads, weights):
    length, depth = heads[0].shape
    width = weights[0].shape[1]
    rows = row_tiles(length)
    return pl.pallas_call(
        mix_kernel,
        out_shape=jax.ShapeDtypeStruct((length, width), LOW),
        grid=(length // TILE,),
        in_specs=[rows(depth)] * 2 + [whole((depth, width))] * 2,
        out_specs=rows(width),
        name="mix_heads",
        cost_estimate=cost(4 * length * depth * width, 4 * length * (depth + width)),
    )(*heads, *weights)


ROOT = math.sqrt(2.0 / math.pi)


def feed_forward_kernel(
    at_ref, s_ref, c_ref, u_low, u_high, d_low, d_high, bias_ref, part_ref, hidden_ref, grad_ref, bias_sum, low_sum, high_sum
):
    step = pl.program_id(0)

    @pl.when(step == 0)
    def _():
        low_sum[...] = jnp.zeros_like(low_sum)
        high_sum[...] = jnp.zeros_like(high_sum)

    totals = 0.0
    for t in range(s_ref.shape[1] // TILE):
        rows = slice(t * TILE, (t + 1) * TILE)
        upward = dot_nn(s_ref[0, rows, :], u_low[0]) + dot_nn(s_ref[1, rows, :], u_high[0]) + bias_ref[0]
        grad_hidden = dot_nt(c_ref[0, rows, :], d_low[0]) + dot_nt(c_ref[1, rows, :], d_high[0])
        square = upward * upward
        bent = jnp.tanh(upward * (ROOT + (ROOT * 0.044715) * square))
        lifted = 0.5 + 0.5 * bent
        slope = lifted + (0.5 * upward) * (1.0 - bent * bent) * (ROOT + (ROOT * 3 * 0.044715) * square)
        hidden_ref[0, rows, :] = (upward * lifted).astype(LOW)
        grad = grad_hidden * slope
        totals = totals + jnp.sum(grad, axis=0, keepdims=True)
        grad = grad.astype(LOW)
        grad_ref[0, rows, :] = grad
        low_sum[rows, :] += dot_nt(grad, u_low[0])
        high_sum[rows, :] += dot_nt(grad, u_high[0])
    bias_sum[0] = jnp.broadcast_to(totals, bias_sum.shape[1:])

    @pl.when(step == pl.num_programs(0) - 1)
    def _():
        n = low_sum.shape[1]
        part_ref[:, :n] = low_sum[...].astype(LOW)
        part_ref[:, n:] = high_sum[...].astype(LOW)


def feed_forward(at, seconds, cots, weights, biases):
    _, length, h = seconds.shape
    each = weights.shape[1] // 2
    tiles = each // TILE
    per = h // TILE
    keep = pl.BlockSpec((2, length, h), lambda i, at: (0, 0, 0))

    def up_spec(flip):
        return pl.BlockSpec(
            (1, h, TILE),
            lambda i, at: (
                (at[0] ^ flip) * 2 + (at[1] ^ (i // tiles)), lax.rem(i, tiles) // per, lax.rem(lax.rem(i, tiles), per)
            ),
        )

    def down_spec(flip):
        return pl.BlockSpec(
            (1, TILE, h), lambda i, at: ((at[0] ^ flip) * 2 + (at[1] ^ (i // tiles)), tiles + lax.rem(i, tiles), 0)
        )

    side = pl.BlockSpec((1, length, TILE), lambda i, at: (i // tiles, 0, lax.rem(i, tiles)))
    one = jax.ShapeDtypeStruct((2, length, each), LOW)
    return pl.pallas_call(
        feed_forward_kernel,
        out_shape=(
            jax.ShapeDtypeStruct((length, 2 * h), LOW), one, one, jax.ShapeDtypeStruct((2 * tiles, 8, TILE), FULL),
        ),
        grid_spec=pltpu.PrefetchScalarGridSpec(
            num_scalar_prefetch=1,
            grid=(2 * tiles,),
            in_specs=[keep] * 2
            + [up_spec(0), up_spec(1), down_spec(0), down_spec(1)]
            + [pl.BlockSpec((1, 1, TILE), lambda i, at: (i, 0, 0))],
            out_specs=(
                pl.BlockSpec((length, 2 * h), lambda i, at: (0, 0)), side, side,
                pl.BlockSpec((1, 8, TILE), lambda i, at: (i, 0, 0)),
            ),
            scratch_shapes=[pltpu.VMEM((length, h), FULL), pltpu.VMEM((length, h), FULL)],
        ),
        name="feed_forward",
        cost_estimate=cost(12 * length * 2 * h * each, 8 * length * h + 16 * h * each + 16 * length * each),
    )(at, seconds, cots, weights, weights, weights, weights, biases.reshape(2 * tiles, 1, TILE))


def up_grads_kernel(at_ref, s_ref, grad_ref, out_ref, turned):
    h = out_ref.shape[2]

    @pl.when(pl.program_id(1) == 0)
    def _():
        turned[...] = s_ref[0].T

    for i in range(out_ref.shape[1] // h):
        part = dot_nn(turned[...], grad_ref[0, :, i * h : (i + 1) * h])
        out_ref[0, i * h : (i + 1) * h, :] = part.astype(LOW)


def up_grads(at, seconds, grads):
    _, length, h = seconds.shape
    each = grads.shape[2]
    return pl.pallas_call(
        up_grads_kernel,
        out_shape=jax.ShapeDtypeStruct((4, each, h), LOW),
        grid_spec=pltpu.PrefetchScalarGridSpec(
            num_scalar_prefetch=1,
            grid=(2, 2),
            in_specs=[
                pl.BlockSpec((1, length, h), lambda y, c, at: (y, 0, 0)),
                pl.BlockSpec((1, length, each), lambda y, c, at: (c, 0, 0)),
            ],
            out_specs=pl.BlockSpec((1, each, h), lambda y, c, at: ((at[0] ^ y) * 2 + (at[1] ^ c), 0, 0)),
            scratch_shapes=[pltpu.VMEM((h, length), LOW)],
        ),
        name="up_grads",
        cost_estimate=cost(8 * length * h * each, 4 * length * each + 8 * h * each),
    )(at, seconds, grads)


def down_grads_kernel(at_ref, hidden_ref, c_ref, out_ref):
    turned = hidden_ref[0].T
    for y in range(2):
        out_ref[at_ref[0] ^ y, 0] = dot_nn(turned, c_ref[y]).astype(LOW)


def down_grads(at, hiddens, cots):
    _, length, h = cots.shape
    each = hiddens.shape[2]
    return pl.pallas_call(
        down_grads_kernel,
        out_shape=jax.ShapeDtypeStruct((2, 2, each, h), LOW),
        grid_spec=pltpu.PrefetchScalarGridSpec(
            num_scalar_prefetch=1,
            grid=(2, each // h),
            in_specs=[
                pl.BlockSpec((1, length, h), lambda c, b, at: (c, 0, b)),
                pl.BlockSpec((2, length, h), lambda c, b, at: (0, 0, 0)),
            ],
            out_specs=pl.BlockSpec((2, 1, h, h), lambda c, b, at: (0, at[1] ^ c, b, 0)),
        ),
        name="down_grads",
        cost_estimate=cost(8 * length * h * each, 4 * length * each + 8 * h * each),
    )(at, hiddens, cots)


def layer_end_kernel(at_ref, h0, h1, w00, w01, w10, w11, own_ref, theirs_ref):
    n = own_ref.shape[1] // 2
    for j, (a, b) in enumerate(((w00, w01), (w10, w11))):
        part = dot_nn(h0[0], a[0]) + dot_nn(h1[0], b[0])
        own_ref[:, j * n : (j + 1) * n] = part[:, :n]
        theirs_ref[:, j * n : (j + 1) * n] = part[:, n:].astype(LOW)


def layer_end(at, hiddens, weights):
    _, length, each = hiddens.shape
    h = weights.shape[2]
    out = pl.BlockSpec((TILE, h), lambda t, at: (t, 0))

    def rows(c):
        return pl.BlockSpec((1, TILE, each), lambda t, at: (c, t, 0))

    def weight(y, col):
        return pl.BlockSpec((1, each, h), lambda t, at: ((at[0] ^ y) * 2 + (at[1] ^ col), 1, 0))

    return pl.pallas_call(
        layer_end_kernel,
        out_shape=(jax.ShapeDtypeStruct((length, h), FULL), jax.ShapeDtypeStruct((length, h), LOW)),
        grid_spec=pltpu.PrefetchScalarGridSpec(
            num_scalar_prefetch=1,
            grid=(length // TILE,),
            in_specs=[rows(0), rows(1), weight(0, 0), weight(0, 1), weight(1, 0), weight(1, 1)],
            out_specs=(out, out),
        ),
        name="layer_end",
        cost_estimate=cost(8 * length * h * each, 8 * h * each + 12 * length * h),
    )(at, hiddens, hiddens, weights, weights, weights, weights)


def after(values, *late):
    return lax.optimization_barrier((values, late))[0]


def pick(pair, index):
    return lax.dynamic_index_in_dim(pair, index, 0, keepdims=False)


def ordered(own, other, index):
    flip = index == 0
    return jnp.stack((jnp.where(flip, own, other), jnp.where(flip, other, own)))


def swap_across(array):
    return lax.ppermute(array, ("y", "col"), [(0, 3), (3, 0), (1, 2), (2, 1)])


def plane_gather(block):
    return block, swap(block, "y"), swap(block, "col"), swap_across(block)


def plane_exchange(at_y, at_col, across):
    return swap(at_y, "y"), swap(at_col, "col"), swap_across(across)


def plane_sum(own, got):
    return (own.astype(FULL) + sum(g.astype(FULL) for g in got)).astype(LOW)


def add_low(left, right):
    return (left.astype(FULL) + right.astype(FULL)).astype(LOW)


PAIRS = [(0, 1), (1, 0), (2, 3), (3, 2)]
FAR = [(0, 2), (2, 0), (1, 3), (3, 1)]


def depth_pair(array, odd):
    halves = array.reshape(2, array.shape[0] // 2, array.shape[1])
    return add_low(pick(halves, odd), lax.ppermute(pick(halves, 1 - odd), "dp", PAIRS))


def depth_far(part):
    return add_low(part, lax.ppermute(part, "dp", FAR))


def depth_join(part, odd):
    return ordered(part, lax.ppermute(part, "dp", PAIRS), odd).reshape(-1, part.shape[1])


def half(weight, axis, index):
    size = weight.shape[axis] // 2
    return lax.dynamic_slice_in_dim(weight, index * size, size, axis)


def fast_body(
    inputs, gain_first, shift_first, w_query, w_key, w_value, w_output, gain_second, shift_second,
    w_up, bias_up, w_down, bias_down, segments, random_blocks, global_blocks, cotangent,
):
    depth_at, y_at, core_at, col_at = (lax.axis_index(name) for name in ("dp", "y", "core", "col"))
    length = segments.shape[1]
    n = inputs.shape[1]
    h = 2 * n
    at = jnp.stack((y_at, col_at)).astype(jnp.int32)

    def chip_block(weights, axis, join):
        mine = jnp.concatenate([half(w, axis, core_at) for w in weights], axis=axis)
        theirs = swap(jnp.concatenate([half(w, axis, 1 - core_at) for w in weights], axis=axis), "core")
        return jnp.concatenate((mine, theirs), axis=join)

    inputs_pair = inputs.reshape(2, length, n)
    x_own = pick(inputs_pair, y_at)
    x_y = swap(pick(inputs_pair, 1 - y_at), "y")
    qkv_block = chip_block((w_query, w_key, w_value), 1, 0)
    qkv_own, qkv_y, qkv_x, qkv_xy = plane_gather(qkv_block)
    xs = (x_own, swap(x_own, "core"), x_y, swap(x_y, "core"))
    w_up, w_down = after((w_up, w_down), qkv_block)
    up_block, down_block = chip_block((w_up,), 1, 0), chip_block((w_down,), 0, 1)
    ups = up_block.shape[1] // h
    ffn_block = jnp.concatenate([up_block[:, i * h : (i + 1) * h] for i in range(ups)] + [down_block])
    ffn_block, w_output, cotangent_late = after((ffn_block, w_output, cotangent), qkv_y, qkv_x)
    ffn = lax.all_gather(ffn_block, ("y", "col"), axis=0, tiled=False)
    out_own, out_y, out_x, out_xy = plane_gather(chip_block((w_output,), 0, 1))
    cot_pair = cotangent_late.reshape(2, length, n)

    vectors = jnp.stack((gain_first, shift_first, gain_second, shift_second, bias_down))
    vectors = jnp.concatenate((vectors, swap(vectors, "core")), axis=1)
    vectors = jnp.concatenate((vectors, swap(vectors, "y")), axis=1)
    gain_one, shift_one, gain_two, shift_two, bias_low = (vectors[i : i + 1] for i in range(5))
    heads_half = half(random_blocks, 0, core_at)
    hidden_bias = half(bias_up, 0, core_at)
    each = hidden_bias.shape[0]
    small = swap(jnp.concatenate((hidden_bias, heads_half.astype(FULL).reshape(-1))), "col")
    biases = jnp.concatenate((hidden_bias, small[:each]))
    heads_half_x = small[each:].reshape(heads_half.shape).astype(jnp.int32)
    moves = []
    for y in range(2):
        for core in range(2):
            for col in range(2):
                moves.append(((col * 2 + y) * 2 + core, (y * 2 + core) * 2 + col))
    labels = lax.ppermute(segments, ("y", "core", "col"), moves)[0]
    all_heads = jnp.concatenate((heads_half, heads_half_x), axis=0)
    rows_extra, keys_extra, where_table = attention_extras(labels, all_heads, global_blocks)
    near_heads = heads_half.shape[0]
    keys_of = (keys_extra[:near_heads], keys_extra[near_heads:])
    live = (labels != 0)[:, None]

    cot_own = pick(cot_pair, y_at)
    cot_y = swap(pick(cot_pair, 1 - y_at), "y")
    cot_swapped = swap(cot_y, "core")
    cots = jnp.stack([jnp.concatenate(c, axis=1) for c in ((cot_own, swap(cot_own, "core")), (cot_y, cot_swapped))])

    firsts = first_norm(after(xs, qkv_xy), gain_one, shift_one)
    qkv_x = after(qkv_x, out_y, out_x, out_xy, cot_y)
    w_qkv = (jnp.concatenate((qkv_own, qkv_y), axis=0), jnp.concatenate((qkv_x, qkv_xy), axis=0))
    first = jnp.concatenate(firsts, axis=1)
    out_own = after(out_own, cots)
    w_out = (jnp.concatenate((out_own, out_y), axis=1), jnp.concatenate((out_x, out_xy), axis=1))
    qkv, heads, kept = [], [], []
    for i in range(2):
        qkv.append(dot_nn(first, w_qkv[i]).astype(LOW))
        done, saved = attend_forward(qkv[i], rows_extra, keys_of[i], where_table)
        heads.append(done)
        kept.append(saved)
    mixed_part = mix_heads(heads, w_out)
    residual, seconds = second_norm(xs, mixed_part, swap(mixed_part, "core"), gain_two, shift_two)

    second_part, hiddens, up_sides, bias_sum = feed_forward(at, seconds, cots, ffn, biases)
    down_parts = down_grads(at, hiddens, cots).reshape(4, -1, h)
    down_scattered = lax.psum_scatter(down_parts, ("y", "col"), scatter_dimension=0, tiled=True)[0]
    up_parts = up_grads(at, seconds, after(up_sides, down_parts))
    up_scattered = lax.psum_scatter(up_parts, ("y", "col"), scatter_dimension=0, tiled=True)[0]
    second_got = after(swap(second_part, "core"), up_parts)

    grad_own, grad_other, grad_mixed, sums_two = second_norm_back(residual, second_part, second_got, cots, gain_two)
    grads = jnp.where(live, dot_nt(grad_mixed, jnp.concatenate(w_out, axis=0)), 0.0).astype(LOW)
    out_grads = [[dot_tn(grad_mixed[:, j * h : (j + 1) * h], head).astype(LOW) for j in range(2)] for head in heads]
    qkv_sides, qkv_grads = [None, None], [None, None]
    for i in (1, 0):
        qkv_sides[i] = attend_backward(kept[i], qkv[i], keys_of[i], heads[i], grads, i, where_table)
        qkv_grads[i] = [dot_tn(f, qkv_sides[i]).astype(LOW) for f in firsts]
    odd = lax.rem(depth_at, 2)
    out_got = plane_exchange(out_grads[0][1], out_grads[1][0], out_grads[1][1])
    qkv_sides = after(qkv_sides, qkv_grads)
    first_part = dot_nt(jnp.concatenate(qkv_sides, axis=1), jnp.concatenate(w_qkv, axis=1)).astype(LOW)
    down_part = depth_pair(after(down_scattered, qkv_sides[0]), odd)
    down_part = depth_far(down_part)
    first_part = after(first_part, out_got, down_part)
    mine, theirs, sums_one = first_norm_back(xs, first_part, swap(first_part, "core"), grad_own, grad_other, gain_one)
    theirs = swap(theirs, "y")
    grad_inputs = ordered(mine, theirs.astype(FULL), y_at).reshape(2 * length, n)

    up_scattered = after(up_scattered, sums_one)
    up_part = depth_pair(up_scattered, odd)
    qkv_got = plane_exchange(*after((qkv_grads[0][1], qkv_grads[1][0], qkv_grads[1][1]), up_scattered))
    ends_own, ends_other = layer_end(at, after(hiddens, up_scattered), ffn)
    up_far = depth_far(after(up_part, ends_own))
    down_total = depth_join(after(down_part, ends_own), odd)
    kept_two = jnp.concatenate((residual[:, :n], residual[:, 2 * n : 3 * n]), axis=1)
    bias_two = jnp.concatenate((bias_low[:, :n], bias_low[:, 2 * n : 3 * n]), axis=1)
    ends = (kept_two + ends_own + swap(ends_other, "core").astype(FULL) + bias_two).astype(LOW)
    ends_got = swap(ends[:, n:], "y")
    layer_out = ordered(ends[:, :n], ends_got, y_at).reshape(2 * length, n)

    gains = jnp.concatenate((sums_one[:2, :n], sums_two[:2, :n])).reshape(-1)
    gains_y = jnp.concatenate((sums_one[:2, n:], sums_two[:2, n:])).reshape(-1)
    up_bias = bias_sum[:, 0, :].reshape(-1)
    got = swap(jnp.concatenate((gains_y, up_bias)), "y")
    gains = gains + got[: 4 * n]
    up_bias = up_bias + got[4 * n :]
    near = jnp.concatenate((gains, jnp.sum(cotangent, axis=0, dtype=FULL), up_bias[:each]))
    near = near + swap(jnp.concatenate((near[: 5 * n], up_bias[each:])), "col")
    near = near + lax.ppermute(near, "dp", [(0, 1), (1, 0), (2, 3), (3, 2)])
    near = near + lax.ppermute(near, "dp", [(0, 2), (2, 0), (1, 3), (3, 1)])
    gains = near[: 5 * n].reshape(5, n)
    up_bias = ordered(near[5 * n :], swap(near[5 * n :], "core"), core_at).reshape(-1)

    def finish(total, axis, parts):
        keep = lax.slice_in_dim(total, 0, n, axis=axis)
        got = swap(lax.slice_in_dim(total, n, 2 * n, axis=axis), "core")
        size = keep.shape[1 - axis] // parts
        flip = core_at == 0
        out = []
        for i in range(parts):
            a, b = (lax.slice_in_dim(z, i * size, (i + 1) * size, axis=1 - axis) for z in (keep, got))
            out.append(jnp.concatenate((jnp.where(flip, a, b), jnp.where(flip, b, a)), axis=1 - axis).astype(FULL))
        return out

    four = jnp.concatenate(
        (plane_sum(after(qkv_grads[0][0], up_part), qkv_got), plane_sum(out_grads[0][0], out_got)), axis=1
    )
    four = depth_pair(after(four, up_far, near), odd)
    up_total = depth_join(up_far, odd)
    four = depth_far(after(four, theirs, ends))
    four = depth_join(after(four, ends_got), odd)
    grad_query, grad_key, grad_value, grad_out = finish(four, 0, 4)
    (grad_down,) = finish(down_total, 1, 1)
    (grad_up,) = finish(jnp.concatenate([up_total[i * h : (i + 1) * h] for i in range(ups)], axis=1), 0, 1)
    return (
        layer_out, grad_inputs, gains[0], gains[1], grad_query, grad_key, grad_value, grad_out.T, gains[2], gains[3],
        grad_up, up_bias, grad_down, gains[4],
    )


def whole_sequences(mesh):
    return mesh.shape["row"] == 4 and mesh.shape["col"] == 2 and mesh.shape["dp"] == 4


def placements(row):
    tokens = P(("dp", "col"), row)
    rows = P(row)
    weight = P(row, "col")
    turned = P("col", row)
    placed = (
        tokens, rows, rows, weight, weight, weight, turned, rows, rows, weight, P("col"), turned, rows,
        P(("dp", *row), None), P("col", None, None), P(), tokens,
    )
    given = (
        tokens, tokens, rows, rows, weight, weight, weight, turned, rows, rows, weight, P("col"), turned, rows,
    )
    return placed, given


def solution(mesh):
    sizes = mesh.shape
    split = jax.sharding.Mesh(
        mesh.devices.reshape(sizes["dp"], sizes["row"] // 2, 2, sizes["col"]), ("dp", "y", "core", "col")
    )

    def run(*arrays):
        tokens, length = arrays[0].shape[0], arrays[13].shape[1]
        if whole_sequences(mesh) and tokens == sizes["dp"] * sizes["col"] * 2 * length:
            placed, given = placements(("y", "core"))
            step = jax.shard_map(fast_body, mesh=split, in_specs=placed, out_specs=given, check_vma=False)
        else:
            placed, given = placements(("row",))
            step = jax.shard_map(body, mesh=mesh, in_specs=placed, out_specs=given, check_vma=False)
        return step(*arrays)

    return run
```

```python
import math

import jax
import jax.numpy as jnp
from jax import lax
from jax.experimental import pallas as pl
from jax.experimental.pallas import tpu as pltpu
from jax.sharding import PartitionSpec as P

D = 1024
HD = 64
BLK = 64
NB = 16


EPS = 1e-05


def product(picked, weight, flipped):
    if flipped:
        return lax.dot_general(
            picked, weight, (((1,), (1,)), ((), ())), preferred_element_type=jnp.float32
        )
    return jnp.dot(picked, weight, preferred_element_type=jnp.float32)


def to_columns(moving, weight, flipped):
    gathered = lax.all_gather(moving, "col", axis=0, tiled=True)
    row_count = gathered.shape[0] // lax.axis_size("row")

    def term_rows(first_row, how_many):
        return product(gathered, weight, flipped)

    result = lax.psum_scatter(
        term_rows(jnp.int32(0), lax.axis_size("row") * row_count),
        "row",
        scatter_dimension=0,
        tiled=True,
    )
    return (result, gathered)


def to_rows(moving, weight, flipped):
    gathered = lax.all_gather(moving, "row", axis=0, tiled=True)
    row_count = gathered.shape[0] // lax.axis_size("col")

    def term_rows(first_row, how_many):
        return product(gathered, weight, flipped)

    return (
        lax.psum_scatter(
            term_rows(jnp.int32(0), lax.axis_size("col") * row_count),
            "col",
            scatter_dimension=0,
            tiled=True,
        ),
        gathered,
    )


def norm_sums(first_sum, second_sum):
    return lax.psum((first_sum, second_sum), "row")


def norm_forward(moving, gain_row, shift_row):
    totals, squares = norm_sums(jnp.sum(moving, axis=1), jnp.sum(moving * moving, axis=1))
    center = totals / D
    spread = squares / D - center * center
    inverse = lax.rsqrt(spread + EPS)
    normed = (moving - center[:, None]) * inverse[:, None]
    return (normed * gain_row + shift_row, normed, inverse)


def norm_backward(upstream, normed, inverse, gain_row):
    scaled = upstream * gain_row
    first_sum, second_sum = norm_sums(jnp.sum(scaled, axis=1), jnp.sum(scaled * normed, axis=1))
    return inverse[:, None] * (scaled - first_sum[:, None] / D - normed * (second_sum[:, None] / D))


def head_masks(random_blocks, global_blocks):
    block_ids = jnp.arange(NB, dtype=jnp.int32)
    nearby = jnp.abs(block_ids[:, None] - block_ids[None, :]) <= 1
    chosen = jnp.any(random_blocks[:, :, :, None] == block_ids[None, None, None, :], axis=2)
    marked = jnp.any(global_blocks[:, None] == block_ids[None, :], axis=0)
    block_table = nearby[None] | chosen | marked[None, None, :] | marked[None, :, None]
    return jnp.repeat(jnp.repeat(block_table, BLK, axis=1), BLK, axis=2)


def seq_logits(seq_queries, seq_keys, labels, pattern):
    same_doc = (labels[:, None] == labels[None, :]) & (labels[None, :] != 0)
    raw_scores = jnp.einsum(
        "qhd,khd->hqk", seq_queries, seq_keys, preferred_element_type=jnp.float32
    )
    return jnp.where(pattern & same_doc[None], raw_scores * (1.0 / math.sqrt(HD)), -1000000000.0)


def attend_plain(queries, key_block, value_block, segments, pattern):

    def one_seq(pieces):
        seq_queries, seq_keys, seq_values, labels = pieces
        logits = seq_logits(seq_queries, seq_keys, labels, pattern)
        row_peak = jnp.max(logits, axis=2, keepdims=True)
        exp_terms = jnp.exp(logits - row_peak)
        row_total = jnp.sum(exp_terms, axis=2, keepdims=True)
        softmax = (exp_terms / row_total).astype(jnp.bfloat16)
        attended = jnp.einsum(
            "hqk,khd->qhd", softmax, seq_values, preferred_element_type=jnp.float32
        )
        live_rows = (labels != 0).astype(jnp.float32)
        return (attended * live_rows[:, None, None], (row_peak + jnp.log(row_total))[:, :, 0])

    return lax.map(one_seq, (queries, key_block, value_block, segments))


def attend_plain_backward(queries, key_block, value_block, segments, pattern, grad_heads, log_total):

    def one_seq(pieces):
        seq_queries, seq_keys, seq_values, labels, seq_grads, seq_log = pieces
        logits = seq_logits(seq_queries, seq_keys, labels, pattern)
        softmax = jnp.exp(logits - seq_log[:, :, None])
        grad_probs = jnp.einsum(
            "qhd,khd->hqk", seq_grads, seq_values, preferred_element_type=jnp.float32
        )
        grad_values = jnp.einsum(
            "hqk,qhd->khd",
            softmax.astype(jnp.bfloat16),
            seq_grads,
            preferred_element_type=jnp.float32,
        )
        inner_sum = jnp.sum(softmax * grad_probs, axis=2, keepdims=True)
        grad_raw = (softmax * (grad_probs - inner_sum) * (1.0 / math.sqrt(HD))).astype(jnp.bfloat16)
        grad_queries = jnp.einsum(
            "hqk,khd->qhd", grad_raw, seq_keys, preferred_element_type=jnp.float32
        )
        grad_keys = jnp.einsum(
            "hqk,qhd->khd", grad_raw, seq_queries, preferred_element_type=jnp.float32
        )
        return (grad_queries, grad_keys, grad_values)

    return lax.map(one_seq, (queries, key_block, value_block, segments, grad_heads, log_total))


def gelu_tanh(values):
    return jax.nn.gelu(values, approximate=True)


def weight_grad(left, right):
    return lax.dot_general(
        left, right, (((0,), (0,)), ((), ())), preferred_element_type=jnp.float32
    )


def body(
    inputs,
    gain_first,
    shift_first,
    w_query,
    w_key,
    w_value,
    w_output,
    gain_second,
    shift_second,
    w_up,
    bias_up,
    w_down,
    bias_down,
    segments,
    random_blocks,
    global_blocks,
    cotangent,
):
    seq_count, seq_len = segments.shape
    head_width = w_query.shape[1]
    heads_here = random_blocks.shape[0]
    seq_shape = (seq_count, seq_len, heads_here, HD)
    pattern = head_masks(random_blocks, global_blocks)
    live_tokens = (segments != 0).reshape(-1)
    x_first = inputs.astype(jnp.float32)
    first_full, normed_one, inverse_one = norm_forward(x_first, gain_first, shift_first)
    first_low = first_full.astype(jnp.bfloat16)
    stacked = jnp.concatenate((w_query, w_key, w_value), axis=1)
    projected, first_all = to_columns(first_low, stacked, False)
    proj_low = projected.astype(jnp.bfloat16)
    queries = proj_low[:, :head_width].reshape(seq_shape)
    key_block = proj_low[:, head_width : 2 * head_width].reshape(seq_shape)
    value_block = proj_low[:, 2 * head_width :].reshape(seq_shape)
    heads_out, log_total = attend_plain(queries, key_block, value_block, segments, pattern)
    heads_low = heads_out.reshape(-1, head_width).astype(jnp.bfloat16)
    mixed_out, heads_all = to_rows(heads_low, w_output, False)
    residual = x_first + mixed_out
    second_full, normed_two, inverse_two = norm_forward(residual, gain_second, shift_second)
    second_low = second_full.astype(jnp.bfloat16)
    upward, second_all = to_columns(second_low, w_up, False)
    upward = upward + bias_up
    hidden_low = gelu_tanh(upward).astype(jnp.bfloat16)
    downward, hidden_all = to_rows(hidden_low, w_down, False)
    layer_out = (residual + (downward + bias_down)).astype(jnp.bfloat16)
    grad_hidden, cotangent_all = to_columns(cotangent, w_down, True)
    activated, pull_back = jax.vjp(gelu_tanh, upward)
    grad_upward = pull_back(grad_hidden)[0].astype(jnp.bfloat16)
    grad_second, grad_upward_all = to_rows(grad_upward, w_up, True)
    grad_residual = cotangent.astype(jnp.float32) + norm_backward(
        grad_second, normed_two, inverse_two, gain_second
    )
    grad_mixed = grad_residual.astype(jnp.bfloat16)
    grad_heads, grad_mixed_all = to_columns(grad_mixed, w_output, True)
    grad_heads = jnp.where(live_tokens[:, None], grad_heads, 0.0).astype(jnp.bfloat16)
    grad_queries, grad_keys, grad_values = attend_plain_backward(
        queries, key_block, value_block, segments, pattern, grad_heads.reshape(seq_shape), log_total
    )
    grad_proj = jnp.concatenate(
        (
            grad_queries.reshape(-1, head_width),
            grad_keys.reshape(-1, head_width),
            grad_values.reshape(-1, head_width),
        ),
        axis=1,
    ).astype(jnp.bfloat16)
    grad_first, grad_proj_all = to_rows(grad_proj, stacked, True)
    grad_inputs = grad_residual + norm_backward(grad_first, normed_one, inverse_one, gain_first)
    grad_stacked = weight_grad(first_all, grad_proj_all)
    grad_out_weight = weight_grad(heads_all, grad_mixed_all)
    grad_up_weight = weight_grad(second_all, grad_upward_all)
    grad_down_weight = weight_grad(hidden_all, cotangent_all)
    grad_up_bias = jnp.sum(grad_upward_all, axis=0, dtype=jnp.float32)
    grad_down_bias = jnp.sum(cotangent_all, axis=0, dtype=jnp.float32)
    gain_terms = lax.psum(
        (
            jnp.sum(grad_first * normed_one, axis=0),
            jnp.sum(grad_first, axis=0),
            jnp.sum(grad_second * normed_two, axis=0),
            jnp.sum(grad_second, axis=0),
        ),
        ("dp", "col"),
    )
    summed = (
        lax.psum(grad_stacked.astype(jnp.bfloat16), "dp").astype(jnp.float32),
        lax.psum(grad_out_weight.astype(jnp.bfloat16), "dp").astype(jnp.float32),
        lax.psum(grad_up_weight.astype(jnp.bfloat16), "dp").astype(jnp.float32),
        lax.psum(grad_down_weight.astype(jnp.bfloat16), "dp").astype(jnp.float32),
        lax.psum(grad_up_bias.astype(jnp.bfloat16), "dp").astype(jnp.float32),
        lax.psum(grad_down_bias.astype(jnp.bfloat16), "dp").astype(jnp.float32),
    )
    return (
        layer_out,
        grad_inputs,
        gain_terms[0],
        gain_terms[1],
        summed[0][:, :head_width],
        summed[0][:, head_width : 2 * head_width],
        summed[0][:, 2 * head_width :],
        summed[1],
        gain_terms[2],
        gain_terms[3],
        summed[2],
        summed[4],
        summed[3],
        summed[5],
    )


SWAP = [(0, 1), (1, 0)]
LOW = jnp.bfloat16
FULL = jnp.float32
TILE = 256
BIG = 1e30


def swap(array, axis):
    return lax.ppermute(array, axis, SWAP)


def dot_nn(left, right):
    return lax.dot_general(left, right, (((1,), (0,)), ((), ())), preferred_element_type=FULL)


def dot_nt(left, right):
    return lax.dot_general(left, right, (((1,), (1,)), ((), ())), preferred_element_type=FULL)


def dot_tn(left, right):
    return lax.dot_general(left, right, (((0,), (0,)), ((), ())), preferred_element_type=FULL)


def attention_extras(labels, random_blocks, global_blocks):
    length = labels.shape[0]
    blocks = length // BLK
    block_ids = jnp.arange(blocks, dtype=jnp.int32)
    nearby = jnp.abs(block_ids[:, None] - block_ids[None, :]) <= 1
    chosen = jnp.any(random_blocks[:, :, :, None] == block_ids[None, None, None, :], axis=2)
    marked = jnp.any(global_blocks[:, None] == block_ids[None, :], axis=0)
    table = nearby[None] | chosen | marked[None, None, :] | marked[None, :, None]
    heads = table.shape[0]
    lane = jnp.arange(HD, dtype=jnp.int32)
    place = jnp.arange(length, dtype=jnp.int32) // BLK
    doc_lane = blocks + jnp.where(labels == 0, 4, labels - 1)
    row_extra = ((lane[None, :] == place[:, None]) | (lane[None, :] == doc_lane[:, None])).astype(LOW)
    table_keys = jnp.pad(jnp.swapaxes(table, 1, 2), ((0, 0), (0, 0), (0, HD - blocks)), constant_values=True)
    table_keys = jnp.repeat(table_keys, BLK, axis=1)
    is_doc = (lane >= blocks) & (lane <= blocks + 4)
    doc_bad = is_doc[None, :] & (lane[None, :] != doc_lane[:, None])
    doc_bad = doc_bad | (lane[None, :] == blocks + 4)
    key_extra = jnp.where(table_keys & ~doc_bad[None], 0.0, -BIG)
    key_extra = jnp.where((lane >= blocks + 5) & (lane <= blocks + 7), 1.0, key_extra).astype(LOW)
    rows = jnp.stack((jnp.pad(row_extra, ((0, 0), (HD, 0))), jnp.pad(row_extra, ((0, 0), (0, HD)))))
    even = jnp.pad(key_extra[0::2], ((0, 0), (0, 0), (HD, 0)))
    odd = jnp.pad(key_extra[1::2], ((0, 0), (0, 0), (0, HD)))
    keys = jnp.stack((even, odd), axis=1).reshape(heads, length, 2 * HD)
    tiles = length // TILE
    known = labels[None, :] == jnp.arange(1, 5, dtype=jnp.int32)[:, None]
    present = jnp.any(known.reshape(4, tiles, TILE), axis=2)
    wanted = jnp.any(present[:, :, None] & known[:, None, :], axis=0)
    spots = jnp.arange(length, dtype=jnp.int32)
    first = jnp.min(jnp.where(wanted, spots[None, :], length - 1), axis=1)
    last = jnp.max(jnp.where(wanted, spots[None, :], 0), axis=1)
    start = first // 128
    count = jnp.maximum((last + 1 - start * 128 + 255) // 256, 1)
    start = jnp.minimum(start, length // 128 - 2 * count)
    return rows, keys, jnp.stack((start, count)).astype(jnp.int32)


def attend_forward_kernel(where_ref, q_ref, k_ref, v_ref, rows_ref, keys_ref, out_ref, kept_ref, kk, vv):
    length = q_ref.shape[0]
    lane = lax.broadcasted_iota(jnp.int32, (length, 2 * HD), 1)
    for e in range(2):
        data = (lane < HD) if e == 0 else (lane >= HD)
        kk[e] = jnp.where(data, k_ref[...], keys_ref[e])
        vv[e] = jnp.where(data, v_ref[...], jnp.ones_like(v_ref[...]))
    tile_lane = lax.broadcasted_iota(jnp.int32, (TILE, 2 * HD), 1)

    def one_tile(t, carry):
        rows = pl.ds(pl.multiple_of(t * TILE, TILE), TILE)
        start = pl.multiple_of(where_ref[0, t] * 128, 128)
        count = where_ref[1, t]
        q_pair = q_ref[rows, :] * jnp.bfloat16(1.0 / math.sqrt(HD))
        for n in range(1, length // TILE + 1):

            @pl.when(count == n)
            def _():
                span = pl.ds(start, n * TILE)
                outs = []
                for e in range(2):
                    data = (tile_lane < HD) if e == 0 else (tile_lane >= HD)
                    base = HD if e == 0 else 0
                    extra = rows_ref[e, rows, :]
                    q_one = jnp.where(data, q_pair, extra)
                    logits = dot_nt(q_one, kk[e, span, :])
                    peak = jnp.max(logits, axis=1, keepdims=True)
                    terms = jnp.exp(logits - peak)
                    mixed = dot_nn(terms.astype(LOW), vv[e, span, :])
                    total = pltpu.roll(mixed, HD, 1)
                    outs.append(mixed / total)
                    total_one = jnp.max(jnp.where(data, total, 0.0), axis=1, keepdims=True)
                    padded = jnp.max(
                        jnp.where(tile_lane == base + 20, extra.astype(FULL), 0.0), axis=1, keepdims=True
                    )
                    log_total = jnp.where(padded > 0.5, 0.0, -(peak + jnp.log(total_one)))
                    high = log_total.astype(LOW).astype(FULL)
                    middle = (log_total - high).astype(LOW).astype(FULL)
                    low = log_total - high - middle
                    packed = jnp.where(tile_lane == base + 21, high, q_one.astype(FULL))
                    packed = jnp.where(tile_lane == base + 22, middle, packed)
                    packed = jnp.where(tile_lane == base + 23, low, packed)
                    kept_ref[e, rows, :] = packed.astype(LOW)
                joined = jnp.where(tile_lane < HD, outs[0], outs[1])
                out_ref[rows, :] = jnp.where(padded > 0.5, 0.0, joined).astype(LOW)

        return carry

    lax.fori_loop(0, length // TILE, one_tile, 0)


def attend_forward(qkv, rows_extra, keys_extra, where_table):
    length, width = qkv.shape
    pairs = width // (3 * 2 * HD)
    wide = 2 * HD
    return pl.pallas_call(
        attend_forward_kernel,
        out_shape=(
            jax.ShapeDtypeStruct((length, width // 3), LOW),
            jax.ShapeDtypeStruct((2 * pairs, length, wide), LOW),
        ),
        grid_spec=pltpu.PrefetchScalarGridSpec(
            num_scalar_prefetch=1,
            grid=(pairs,),
            in_specs=[
                pl.BlockSpec((length, wide), lambda p, w: (0, p)),
                pl.BlockSpec((length, wide), lambda p, w: (0, pairs + p)),
                pl.BlockSpec((length, wide), lambda p, w: (0, 2 * pairs + p)),
                pl.BlockSpec((2, length, wide), lambda p, w: (0, 0, 0)),
                pl.BlockSpec((2, length, wide), lambda p, w: (p, 0, 0)),
            ],
            out_specs=(
                pl.BlockSpec((length, wide), lambda p, w: (0, p)),
                pl.BlockSpec((2, length, wide), lambda p, w: (p, 0, 0)),
            ),
            scratch_shapes=[pltpu.VMEM((2, length, wide), LOW), pltpu.VMEM((2, length, wide), LOW)],
        ),
        name="attend_forward",
        cost_estimate=pl.CostEstimate(
            flops=8 * pairs * length * length * HD, bytes_accessed=16 * length * width, transcendentals=0
        ),
    )(where_table, qkv, qkv, qkv, rows_extra, keys_extra)


def attend_backward_kernel(
    where_ref, kept_ref, k_ref, v_ref, keys_ref, heads_ref, grads_ref, out_ref, kk, va, dk_sum, dv_sum
):
    length = k_ref.shape[0]
    wide = 2 * HD
    third = out_ref.shape[1] // 3
    pair = pl.program_id(0) * wide
    lane = lax.broadcasted_iota(jnp.int32, (length, wide), 1)
    for e in range(2):
        data = (lane < HD) if e == 0 else (lane >= HD)
        base = HD if e == 0 else 0
        kk[e] = jnp.where(data, k_ref[...], keys_ref[e])
        ones = jnp.where((lane == base) | (lane == base + 1), 1.0, 0.0).astype(LOW)
        va[e] = jnp.where(data, v_ref[...], ones)
    dk_sum[...] = jnp.zeros_like(dk_sum)
    dv_sum[...] = jnp.zeros_like(dv_sum)
    tile_lane = lax.broadcasted_iota(jnp.int32, (TILE, wide), 1)

    def one_tile(t, carry):
        rows = pl.ds(pl.multiple_of(t * TILE, TILE), TILE)
        start = pl.multiple_of(where_ref[0, t] * 128, 128)
        count = where_ref[1, t]
        grads = grads_ref[rows, :]
        both = grads.astype(FULL) * heads_ref[rows, :].astype(FULL)
        for n in range(1, length // TILE + 1):

            @pl.when(count == n)
            def _():
                span = pl.ds(start, n * TILE)
                outs = []
                for e in range(2):
                    data = (tile_lane < HD) if e == 0 else (tile_lane >= HD)
                    base = HD if e == 0 else 0
                    inner = -jnp.sum(jnp.where(data, both, 0.0), axis=1, keepdims=True)
                    high = inner.astype(LOW).astype(FULL)
                    only = jnp.where(data, grads, jnp.zeros_like(grads))
                    packed = jnp.where(tile_lane == base, high, only.astype(FULL))
                    packed = jnp.where(tile_lane == base + 1, inner - high, packed).astype(LOW)
                    q_one = kept_ref[e, rows, :]
                    q_only = jnp.where(data, q_one, jnp.zeros_like(q_one))
                    probs = jnp.exp(dot_nt(kk[e, span, :], q_one))
                    grad_raw = (probs * dot_nt(va[e, span, :], packed)).astype(LOW)
                    dv_sum[span, :] += dot_nn(probs.astype(LOW), only)
                    dk_sum[span, :] += dot_nn(grad_raw, q_only)
                    outs.append(dot_tn(grad_raw, kk[e, span, :]))
                joined = jnp.where(tile_lane < HD, outs[0], outs[1])
                lanes = pl.ds(pl.multiple_of(pair, wide), wide)
                out_ref[rows, lanes] = (joined * (1.0 / math.sqrt(HD))).astype(LOW)

        return carry

    lax.fori_loop(0, length // TILE, one_tile, 0)
    out_ref[:, pl.ds(pl.multiple_of(third + pair, wide), wide)] = dk_sum[...].astype(LOW)
    out_ref[:, pl.ds(pl.multiple_of(2 * third + pair, wide), wide)] = dv_sum[...].astype(LOW)


def attend_backward(kept, qkv, keys_extra, heads, grads, group, where_table):
    length, width = qkv.shape
    pairs = width // (3 * 2 * HD)
    wide = 2 * HD
    stacked = pl.BlockSpec((2, length, wide), lambda p, w: (p, 0, 0))
    return pl.pallas_call(
        attend_backward_kernel,
        out_shape=jax.ShapeDtypeStruct((length, width), LOW),
        grid_spec=pltpu.PrefetchScalarGridSpec(
            num_scalar_prefetch=1,
            grid=(pairs,),
            in_specs=[
                stacked,
                pl.BlockSpec((length, wide), lambda p, w: (0, pairs + p)),
                pl.BlockSpec((length, wide), lambda p, w: (0, 2 * pairs + p)),
                stacked,
                pl.BlockSpec((length, wide), lambda p, w: (0, p)),
                pl.BlockSpec((length, wide), lambda p, w: (0, group * pairs + p)),
            ],
            out_specs=pl.BlockSpec((length, width), lambda p, w: (0, 0)),
            scratch_shapes=[
                pltpu.VMEM((2, length, wide), LOW),
                pltpu.VMEM((2, length, wide), LOW),
                pltpu.VMEM((length, wide), FULL),
                pltpu.VMEM((length, wide), FULL),
            ],
        ),
        name="attend_backward",
        cost_estimate=pl.CostEstimate(
            flops=20 * pairs * length * length * HD, bytes_accessed=20 * length * width, transcendentals=0
        ),
    )(where_table, kept, qkv, qkv, keys_extra, heads, grads)


def row_tiles(count):
    def spec(width):
        return pl.BlockSpec((TILE, width), lambda t: (t, 0))

    return spec


def whole(shape):
    return pl.BlockSpec(shape, lambda t: (0,) * len(shape))


def cost(flops, moved):
    return pl.CostEstimate(flops=int(flops), bytes_accessed=int(moved), transcendentals=0)


def norm_parts(blocks):
    width = sum(b.shape[1] for b in blocks)
    total = sum(jnp.sum(b, axis=1, keepdims=True) for b in blocks)
    squares = sum(jnp.sum(b * b, axis=1, keepdims=True) for b in blocks)
    center = total / width
    return center, lax.rsqrt(squares / width - center * center + EPS)


def columns(ref, index, width):
    return ref[:, index * width : (index + 1) * width]


def first_norm_kernel(x0, x1, x2, x3, gain_ref, shift_ref, low_ref, high_ref):
    blocks = [x[...].astype(FULL) for x in (x0, x1, x2, x3)]
    n = blocks[0].shape[1]
    center, inverse = norm_parts(blocks)
    for i, block in enumerate(blocks):
        value = (block - center) * inverse * columns(gain_ref, i, n) + columns(shift_ref, i, n)
        (low_ref, high_ref)[i // 2][:, (i % 2) * n : (i % 2 + 1) * n] = value.astype(LOW)


def first_norm(blocks, gain, shift):
    length, n = blocks[0].shape
    rows = row_tiles(length)
    half = jax.ShapeDtypeStruct((length, 2 * n), LOW)
    return pl.pallas_call(
        first_norm_kernel,
        out_shape=(half, half),
        grid=(length // TILE,),
        in_specs=[rows(n)] * 4 + [whole((1, 4 * n))] * 2,
        out_specs=(rows(2 * n), rows(2 * n)),
        name="first_norm",
        cost_estimate=cost(20 * length * n, 16 * length * n),
    )(*blocks, gain, shift)


def second_norm_kernel(x0, x1, x2, x3, part_ref, got_ref, gain_ref, shift_ref, residual_ref, second_ref):
    n = x0.shape[1]
    blocks = []
    for i, x in enumerate((x0, x1, x2, x3)):
        mixed = columns(part_ref, i, n).astype(FULL) + columns(got_ref, i ^ 1, n).astype(FULL)
        blocks.append(x[...].astype(FULL) + mixed)
    center, inverse = norm_parts(blocks)
    for i, block in enumerate(blocks):
        residual_ref[:, i * n : (i + 1) * n] = block
        value = (block - center) * inverse * columns(gain_ref, i, n) + columns(shift_ref, i, n)
        second_ref[i // 2, :, (i % 2) * n : (i % 2 + 1) * n] = value.astype(LOW)


def second_norm(blocks, part, got, gain, shift):
    length, n = blocks[0].shape
    rows = row_tiles(length)
    return pl.pallas_call(
        second_norm_kernel,
        out_shape=(jax.ShapeDtypeStruct((length, 4 * n), FULL), jax.ShapeDtypeStruct((2, length, 2 * n), LOW)),
        grid=(length // TILE,),
        in_specs=[rows(n)] * 4 + [rows(4 * n)] * 2 + [whole((1, 4 * n))] * 2,
        out_specs=(rows(4 * n), pl.BlockSpec((2, TILE, 2 * n), lambda t: (0, t, 0))),
        name="second_norm",
        cost_estimate=cost(30 * length * n, 48 * length * n),
    )(*blocks, part, got, gain, shift)


def norm_gradient(blocks, part_ref, got_ref, gain_ref, sums_ref):
    n = blocks[0].shape[1]
    center, inverse = norm_parts(blocks)
    normed = [(b - center) * inverse for b in blocks]
    grads = [columns(part_ref, i, n).astype(FULL) + columns(got_ref, i ^ 1, n).astype(FULL) for i in range(4)]
    scaled = [g * columns(gain_ref, i, n) for i, g in enumerate(grads)]
    mean_one = sum(jnp.sum(s, axis=1, keepdims=True) for s in scaled) / (4 * n)
    mean_two = sum(jnp.sum(s * z, axis=1, keepdims=True) for s, z in zip(scaled, normed)) / (4 * n)

    @pl.when(pl.program_id(0) == 0)
    def _():
        sums_ref[...] = jnp.zeros_like(sums_ref)

    for slot, i in enumerate((0, 2)):
        place = slice(slot * n, (slot + 1) * n)
        sums_ref[0:1, place] += jnp.sum(grads[i] * normed[i], axis=0, keepdims=True)
        sums_ref[1:2, place] += jnp.sum(grads[i], axis=0, keepdims=True)
    return [inverse * (s - mean_one - z * mean_two) for s, z in zip(scaled, normed)]


def second_norm_back_kernel(
    residual_ref, part_ref, got_ref, cots_ref, gain_ref, own_ref, other_ref, mixed_ref, sums_ref
):
    n = residual_ref.shape[1] // 4
    blocks = [columns(residual_ref, i, n) for i in range(4)]
    for i, grad in enumerate(norm_gradient(blocks, part_ref, got_ref, gain_ref, sums_ref)):
        total = cots_ref[i // 2, :, (i % 2) * n : (i % 2 + 1) * n].astype(FULL) + grad
        mixed_ref[:, i * n : (i + 1) * n] = total.astype(LOW)
        if i % 2 == 0:
            (own_ref, other_ref)[i // 2][...] = total


def second_norm_back(residual, part, got, cots, gain):
    length, width = residual.shape
    n = width // 4
    rows = row_tiles(length)
    one = jax.ShapeDtypeStruct((length, n), FULL)
    return pl.pallas_call(
        second_norm_back_kernel,
        out_shape=(one, one, jax.ShapeDtypeStruct((length, width), LOW), jax.ShapeDtypeStruct((8, 2 * n), FULL)),
        grid=(length // TILE,),
        in_specs=[rows(width)] * 3 + [pl.BlockSpec((2, TILE, 2 * n), lambda t: (0, t, 0)), whole((1, width))],
        out_specs=(rows(n), rows(n), rows(width), whole((8, 2 * n))),
        name="second_norm_back",
        cost_estimate=cost(60 * length * n, 64 * length * n),
    )(residual, part, got, cots, gain)


def first_norm_back_kernel(
    x0, x1, x2, x3, part_ref, got_ref, own_ref, other_ref, gain_ref, mine_ref, theirs_ref, sums_ref
):
    blocks = [x[...].astype(FULL) for x in (x0, x1, x2, x3)]
    grads = norm_gradient(blocks, part_ref, got_ref, gain_ref, sums_ref)
    mine_ref[...] = own_ref[...] + grads[0]
    theirs_ref[...] = (other_ref[...] + grads[2]).astype(LOW)


def first_norm_back(blocks, part, got, own, other, gain):
    length, n = blocks[0].shape
    rows = row_tiles(length)
    return pl.pallas_call(
        first_norm_back_kernel,
        out_shape=(
            jax.ShapeDtypeStruct((length, n), FULL),
            jax.ShapeDtypeStruct((length, n), LOW),
            jax.ShapeDtypeStruct((8, 2 * n), FULL),
        ),
        grid=(length // TILE,),
        in_specs=[rows(n)] * 4 + [rows(4 * n)] * 2 + [rows(n)] * 2 + [whole((1, 4 * n))],
        out_specs=(rows(n), rows(n), whole((8, 2 * n))),
        name="first_norm_back",
        cost_estimate=cost(60 * length * n, 40 * length * n),
    )(*blocks, part, got, own, other, gain)


def mix_kernel(h0, h1, w0, w1, out_ref):
    out_ref[...] = (dot_nn(h0[...], w0[...]) + dot_nn(h1[...], w1[...])).astype(LOW)


def mix_heads(heads, weights):
    length, depth = heads[0].shape
    width = weights[0].shape[1]
    rows = row_tiles(length)
    return pl.pallas_call(
        mix_kernel,
        out_shape=jax.ShapeDtypeStruct((length, width), LOW),
        grid=(length // TILE,),
        in_specs=[rows(depth)] * 2 + [whole((depth, width))] * 2,
        out_specs=rows(width),
        name="mix_heads",
        cost_estimate=cost(4 * length * depth * width, 4 * length * (depth + width)),
    )(*heads, *weights)


ROOT = math.sqrt(2.0 / math.pi)


def feed_forward_kernel(
    at_ref, s_ref, c_ref, u_low, u_high, d_low, d_high, bias_ref, part_ref, hidden_ref, grad_ref, bias_sum, low_sum, high_sum
):
    step = pl.program_id(0)

    @pl.when(step == 0)
    def _():
        low_sum[...] = jnp.zeros_like(low_sum)
        high_sum[...] = jnp.zeros_like(high_sum)

    totals = 0.0
    for t in range(s_ref.shape[1] // TILE):
        rows = slice(t * TILE, (t + 1) * TILE)
        upward = dot_nn(s_ref[0, rows, :], u_low[0]) + dot_nn(s_ref[1, rows, :], u_high[0]) + bias_ref[0]
        grad_hidden = dot_nt(c_ref[0, rows, :], d_low[0]) + dot_nt(c_ref[1, rows, :], d_high[0])
        square = upward * upward
        bent = jnp.tanh(upward * (ROOT + (ROOT * 0.044715) * square))
        lifted = 0.5 + 0.5 * bent
        slope = lifted + (0.5 * upward) * (1.0 - bent * bent) * (ROOT + (ROOT * 3 * 0.044715) * square)
        hidden_ref[0, rows, :] = (upward * lifted).astype(LOW)
        grad = grad_hidden * slope
        totals = totals + jnp.sum(grad, axis=0, keepdims=True)
        grad = grad.astype(LOW)
        grad_ref[0, rows, :] = grad
        low_sum[rows, :] += dot_nt(grad, u_low[0])
        high_sum[rows, :] += dot_nt(grad, u_high[0])
    bias_sum[0] = jnp.broadcast_to(totals, bias_sum.shape[1:])

    @pl.when(step == pl.num_programs(0) - 1)
    def _():
        n = low_sum.shape[1]
        part_ref[:, :n] = low_sum[...].astype(LOW)
        part_ref[:, n:] = high_sum[...].astype(LOW)


def feed_forward(at, seconds, cots, weights, biases):
    _, length, h = seconds.shape
    each = weights.shape[1] // 2
    tiles = each // TILE
    per = h // TILE
    keep = pl.BlockSpec((2, length, h), lambda i, at: (0, 0, 0))

    def up_spec(flip):
        return pl.BlockSpec(
            (1, h, TILE),
            lambda i, at: (
                (at[0] ^ flip) * 2 + (at[1] ^ (i // tiles)), lax.rem(i, tiles) // per, lax.rem(lax.rem(i, tiles), per)
            ),
        )

    def down_spec(flip):
        return pl.BlockSpec(
            (1, TILE, h), lambda i, at: ((at[0] ^ flip) * 2 + (at[1] ^ (i // tiles)), tiles + lax.rem(i, tiles), 0)
        )

    side = pl.BlockSpec((1, length, TILE), lambda i, at: (i // tiles, 0, lax.rem(i, tiles)))
    one = jax.ShapeDtypeStruct((2, length, each), LOW)
    return pl.pallas_call(
        feed_forward_kernel,
        out_shape=(
            jax.ShapeDtypeStruct((length, 2 * h), LOW), one, one, jax.ShapeDtypeStruct((2 * tiles, 8, TILE), FULL),
        ),
        grid_spec=pltpu.PrefetchScalarGridSpec(
            num_scalar_prefetch=1,
            grid=(2 * tiles,),
            in_specs=[keep] * 2
            + [up_spec(0), up_spec(1), down_spec(0), down_spec(1)]
            + [pl.BlockSpec((1, 1, TILE), lambda i, at: (i, 0, 0))],
            out_specs=(
                pl.BlockSpec((length, 2 * h), lambda i, at: (0, 0)), side, side,
                pl.BlockSpec((1, 8, TILE), lambda i, at: (i, 0, 0)),
            ),
            scratch_shapes=[pltpu.VMEM((length, h), FULL), pltpu.VMEM((length, h), FULL)],
        ),
        name="feed_forward",
        cost_estimate=cost(12 * length * 2 * h * each, 8 * length * h + 16 * h * each + 16 * length * each),
    )(at, seconds, cots, weights, weights, weights, weights, biases.reshape(2 * tiles, 1, TILE))


def up_grads_kernel(at_ref, s_ref, grad_ref, out_ref, turned):
    h = out_ref.shape[2]

    @pl.when(pl.program_id(1) == 0)
    def _():
        turned[...] = s_ref[0].T

    for i in range(out_ref.shape[1] // h):
        part = dot_nn(turned[...], grad_ref[0, :, i * h : (i + 1) * h])
        out_ref[0, i * h : (i + 1) * h, :] = part.astype(LOW)


def up_grads(at, seconds, grads):
    _, length, h = seconds.shape
    each = grads.shape[2]
    return pl.pallas_call(
        up_grads_kernel,
        out_shape=jax.ShapeDtypeStruct((4, each, h), LOW),
        grid_spec=pltpu.PrefetchScalarGridSpec(
            num_scalar_prefetch=1,
            grid=(2, 2),
            in_specs=[
                pl.BlockSpec((1, length, h), lambda y, c, at: (y, 0, 0)),
                pl.BlockSpec((1, length, each), lambda y, c, at: (c, 0, 0)),
            ],
            out_specs=pl.BlockSpec((1, each, h), lambda y, c, at: ((at[0] ^ y) * 2 + (at[1] ^ c), 0, 0)),
            scratch_shapes=[pltpu.VMEM((h, length), LOW)],
        ),
        name="up_grads",
        cost_estimate=cost(8 * length * h * each, 4 * length * each + 8 * h * each),
    )(at, seconds, grads)


def down_grads_kernel(at_ref, hidden_ref, c_ref, out_ref):
    turned = hidden_ref[0].T
    for y in range(2):
        out_ref[at_ref[0] ^ y, 0] = dot_nn(turned, c_ref[y]).astype(LOW)


def down_grads(at, hiddens, cots):
    _, length, h = cots.shape
    each = hiddens.shape[2]
    return pl.pallas_call(
        down_grads_kernel,
        out_shape=jax.ShapeDtypeStruct((2, 2, each, h), LOW),
        grid_spec=pltpu.PrefetchScalarGridSpec(
            num_scalar_prefetch=1,
            grid=(2, each // h),
            in_specs=[
                pl.BlockSpec((1, length, h), lambda c, b, at: (c, 0, b)),
                pl.BlockSpec((2, length, h), lambda c, b, at: (0, 0, 0)),
            ],
            out_specs=pl.BlockSpec((2, 1, h, h), lambda c, b, at: (0, at[1] ^ c, b, 0)),
        ),
        name="down_grads",
        cost_estimate=cost(8 * length * h * each, 4 * length * each + 8 * h * each),
    )(at, hiddens, cots)


def layer_end_kernel(at_ref, h0, h1, w00, w01, w10, w11, own_ref, theirs_ref):
    n = own_ref.shape[1] // 2
    for j, (a, b) in enumerate(((w00, w01), (w10, w11))):
        part = dot_nn(h0[0], a[0]) + dot_nn(h1[0], b[0])
        own_ref[:, j * n : (j + 1) * n] = part[:, :n]
        theirs_ref[:, j * n : (j + 1) * n] = part[:, n:].astype(LOW)


def layer_end(at, hiddens, weights):
    _, length, each = hiddens.shape
    h = weights.shape[2]
    out = pl.BlockSpec((TILE, h), lambda t, at: (t, 0))

    def rows(c):
        return pl.BlockSpec((1, TILE, each), lambda t, at: (c, t, 0))

    def weight(y, col):
        return pl.BlockSpec((1, each, h), lambda t, at: ((at[0] ^ y) * 2 + (at[1] ^ col), 1, 0))

    return pl.pallas_call(
        layer_end_kernel,
        out_shape=(jax.ShapeDtypeStruct((length, h), FULL), jax.ShapeDtypeStruct((length, h), LOW)),
        grid_spec=pltpu.PrefetchScalarGridSpec(
            num_scalar_prefetch=1,
            grid=(length // TILE,),
            in_specs=[rows(0), rows(1), weight(0, 0), weight(0, 1), weight(1, 0), weight(1, 1)],
            out_specs=(out, out),
        ),
        name="layer_end",
        cost_estimate=cost(8 * length * h * each, 8 * h * each + 12 * length * h),
    )(at, hiddens, hiddens, weights, weights, weights, weights)


def after(values, *late):
    return lax.optimization_barrier((values, late))[0]


def pick(pair, index):
    return lax.dynamic_index_in_dim(pair, index, 0, keepdims=False)


def ordered(own, other, index):
    flip = index == 0
    return jnp.stack((jnp.where(flip, own, other), jnp.where(flip, other, own)))


def swap_across(array):
    return lax.ppermute(array, ("y", "col"), [(0, 3), (3, 0), (1, 2), (2, 1)])


def plane_gather(block):
    return block, swap(block, "y"), swap(block, "col"), swap_across(block)


def plane_exchange(at_y, at_col, across):
    return swap(at_y, "y"), swap(at_col, "col"), swap_across(across)


def plane_sum(own, got):
    return (own.astype(FULL) + sum(g.astype(FULL) for g in got)).astype(LOW)


def add_low(left, right):
    return (left.astype(FULL) + right.astype(FULL)).astype(LOW)


PAIRS = [(0, 1), (1, 0), (2, 3), (3, 2)]
FAR = [(0, 2), (2, 0), (1, 3), (3, 1)]


def depth_pair(array, odd):
    halves = array.reshape(2, array.shape[0] // 2, array.shape[1])
    return add_low(pick(halves, odd), lax.ppermute(pick(halves, 1 - odd), "dp", PAIRS))


def depth_far(part):
    return add_low(part, lax.ppermute(part, "dp", FAR))


def depth_join(part, odd):
    return ordered(part, lax.ppermute(part, "dp", PAIRS), odd).reshape(-1, part.shape[1])


def half(weight, axis, index):
    size = weight.shape[axis] // 2
    return lax.dynamic_slice_in_dim(weight, index * size, size, axis)


def fast_body(
    inputs, gain_first, shift_first, w_query, w_key, w_value, w_output, gain_second, shift_second,
    w_up, bias_up, w_down, bias_down, segments, random_blocks, global_blocks, cotangent,
):
    depth_at, y_at, core_at, col_at = (lax.axis_index(name) for name in ("dp", "y", "core", "col"))
    length = segments.shape[1]
    n = inputs.shape[1]
    h = 2 * n
    at = jnp.stack((y_at, col_at)).astype(jnp.int32)

    def chip_block(weights, axis, join):
        mine = jnp.concatenate([half(w, axis, core_at) for w in weights], axis=axis)
        theirs = swap(jnp.concatenate([half(w, axis, 1 - core_at) for w in weights], axis=axis), "core")
        return jnp.concatenate((mine, theirs), axis=join)

    inputs_pair = inputs.reshape(2, length, n)
    x_own = pick(inputs_pair, y_at)
    x_y = swap(pick(inputs_pair, 1 - y_at), "y")
    qkv_block = chip_block((w_query, w_key, w_value), 1, 0)
    qkv_own, qkv_y, qkv_x, qkv_xy = plane_gather(qkv_block)
    xs = (x_own, swap(x_own, "core"), x_y, swap(x_y, "core"))
    w_up, w_down = after((w_up, w_down), qkv_block)
    up_block, down_block = chip_block((w_up,), 1, 0), chip_block((w_down,), 0, 1)
    ups = up_block.shape[1] // h
    ffn_block = jnp.concatenate([up_block[:, i * h : (i + 1) * h] for i in range(ups)] + [down_block])
    ffn_block, w_output, cotangent_late = after((ffn_block, w_output, cotangent), qkv_y, qkv_x)
    ffn = lax.all_gather(ffn_block, ("y", "col"), axis=0, tiled=False)
    out_own, out_y, out_x, out_xy = plane_gather(chip_block((w_output,), 0, 1))
    cot_pair = cotangent_late.reshape(2, length, n)

    vectors = jnp.stack((gain_first, shift_first, gain_second, shift_second, bias_down))
    vectors = jnp.concatenate((vectors, swap(vectors, "core")), axis=1)
    vectors = jnp.concatenate((vectors, swap(vectors, "y")), axis=1)
    gain_one, shift_one, gain_two, shift_two, bias_low = (vectors[i : i + 1] for i in range(5))
    heads_half = half(random_blocks, 0, core_at)
    hidden_bias = half(bias_up, 0, core_at)
    each = hidden_bias.shape[0]
    small = swap(jnp.concatenate((hidden_bias, heads_half.astype(FULL).reshape(-1))), "col")
    biases = jnp.concatenate((hidden_bias, small[:each]))
    heads_half_x = small[each:].reshape(heads_half.shape).astype(jnp.int32)
    moves = []
    for y in range(2):
        for core in range(2):
            for col in range(2):
                moves.append(((col * 2 + y) * 2 + core, (y * 2 + core) * 2 + col))
    labels = lax.ppermute(segments, ("y", "core", "col"), moves)[0]
    all_heads = jnp.concatenate((heads_half, heads_half_x), axis=0)
    rows_extra, keys_extra, where_table = attention_extras(labels, all_heads, global_blocks)
    near_heads = heads_half.shape[0]
    keys_of = (keys_extra[:near_heads], keys_extra[near_heads:])
    live = (labels != 0)[:, None]

    cot_own = pick(cot_pair, y_at)
    cot_y = swap(pick(cot_pair, 1 - y_at), "y")
    cot_swapped = swap(cot_y, "core")
    cots = jnp.stack([jnp.concatenate(c, axis=1) for c in ((cot_own, swap(cot_own, "core")), (cot_y, cot_swapped))])

    firsts = first_norm(after(xs, qkv_xy), gain_one, shift_one)
    qkv_x = after(qkv_x, out_y, out_x, out_xy, cot_y)
    w_qkv = (jnp.concatenate((qkv_own, qkv_y), axis=0), jnp.concatenate((qkv_x, qkv_xy), axis=0))
    first = jnp.concatenate(firsts, axis=1)
    out_own = after(out_own, cots)
    w_out = (jnp.concatenate((out_own, out_y), axis=1), jnp.concatenate((out_x, out_xy), axis=1))
    qkv, heads, kept = [], [], []
    for i in range(2):
        qkv.append(dot_nn(first, w_qkv[i]).astype(LOW))
        done, saved = attend_forward(qkv[i], rows_extra, keys_of[i], where_table)
        heads.append(done)
        kept.append(saved)
    mixed_part = mix_heads(heads, w_out)
    residual, seconds = second_norm(xs, mixed_part, swap(mixed_part, "core"), gain_two, shift_two)

    second_part, hiddens, up_sides, bias_sum = feed_forward(at, seconds, cots, ffn, biases)
    down_parts = down_grads(at, hiddens, cots).reshape(4, -1, h)
    down_scattered = lax.psum_scatter(down_parts, ("y", "col"), scatter_dimension=0, tiled=True)[0]
    up_parts = up_grads(at, seconds, after(up_sides, down_parts))
    up_scattered = lax.psum_scatter(up_parts, ("y", "col"), scatter_dimension=0, tiled=True)[0]
    second_got = after(swap(second_part, "core"), up_parts)

    grad_own, grad_other, grad_mixed, sums_two = second_norm_back(residual, second_part, second_got, cots, gain_two)
    grads = jnp.where(live, dot_nt(grad_mixed, jnp.concatenate(w_out, axis=0)), 0.0).astype(LOW)
    out_grads = [[dot_tn(grad_mixed[:, j * h : (j + 1) * h], head).astype(LOW) for j in range(2)] for head in heads]
    qkv_sides, qkv_grads = [None, None], [None, None]
    for i in (1, 0):
        qkv_sides[i] = attend_backward(kept[i], qkv[i], keys_of[i], heads[i], grads, i, where_table)
        qkv_grads[i] = [dot_tn(f, qkv_sides[i]).astype(LOW) for f in firsts]
    odd = lax.rem(depth_at, 2)
    out_got = plane_exchange(out_grads[0][1], out_grads[1][0], out_grads[1][1])
    qkv_sides = after(qkv_sides, qkv_grads)
    first_part = dot_nt(jnp.concatenate(qkv_sides, axis=1), jnp.concatenate(w_qkv, axis=1)).astype(LOW)
    down_part = depth_pair(after(down_scattered, qkv_sides[0]), odd)
    down_part = depth_far(down_part)
    first_part = after(first_part, out_got, down_part)
    mine, theirs, sums_one = first_norm_back(xs, first_part, swap(first_part, "core"), grad_own, grad_other, gain_one)
    theirs = swap(theirs, "y")
    grad_inputs = ordered(mine, theirs.astype(FULL), y_at).reshape(2 * length, n)

    gains = jnp.concatenate((sums_one[:2, :n], sums_two[:2, :n])).reshape(-1)
    gains_y = jnp.concatenate((sums_one[:2, n:], sums_two[:2, n:])).reshape(-1)
    up_bias = bias_sum[:, 0, :].reshape(-1)
    got = swap(jnp.concatenate((gains_y, up_bias)), "y")
    gains = gains + got[: 4 * n]
    up_bias = up_bias + got[4 * n :]
    near = jnp.concatenate((gains, jnp.sum(cotangent, axis=0, dtype=FULL), up_bias[:each]))
    near = near + swap(jnp.concatenate((near[: 5 * n], up_bias[each:])), "col")
    up_scattered = after(up_scattered, near)
    up_part = depth_pair(up_scattered, odd)
    qkv_got = plane_exchange(*after((qkv_grads[0][1], qkv_grads[1][0], qkv_grads[1][1]), up_scattered))
    up_far = depth_far(up_part)
    ends_own, ends_other = layer_end(at, after(hiddens, up_part), ffn)
    down_total = depth_join(after(down_part, up_far), odd)
    kept_two = jnp.concatenate((residual[:, :n], residual[:, 2 * n : 3 * n]), axis=1)
    bias_two = jnp.concatenate((bias_low[:, :n], bias_low[:, 2 * n : 3 * n]), axis=1)
    ends = (kept_two + ends_own + swap(ends_other, "core").astype(FULL) + bias_two).astype(LOW)
    ends_got = swap(ends[:, n:], "y")
    layer_out = ordered(ends[:, :n], ends_got, y_at).reshape(2 * length, n)

    near = after(near, up_part)
    near = near + lax.ppermute(near, "dp", [(0, 1), (1, 0), (2, 3), (3, 2)])
    near = near + lax.ppermute(near, "dp", [(0, 2), (2, 0), (1, 3), (3, 1)])
    gains = near[: 5 * n].reshape(5, n)
    up_bias = ordered(near[5 * n :], swap(near[5 * n :], "core"), core_at).reshape(-1)

    def finish(total, axis, parts):
        keep = lax.slice_in_dim(total, 0, n, axis=axis)
        got = swap(lax.slice_in_dim(total, n, 2 * n, axis=axis), "core")
        size = keep.shape[1 - axis] // parts
        flip = core_at == 0
        out = []
        for i in range(parts):
            a, b = (lax.slice_in_dim(z, i * size, (i + 1) * size, axis=1 - axis) for z in (keep, got))
            out.append(jnp.concatenate((jnp.where(flip, a, b), jnp.where(flip, b, a)), axis=1 - axis).astype(FULL))
        return out

    four = jnp.concatenate(
        (plane_sum(after(qkv_grads[0][0], up_part), qkv_got), plane_sum(out_grads[0][0], out_got)), axis=1
    )
    four = depth_pair(after(four, up_far, near, ends_own), odd)
    up_total = depth_join(up_far, odd)
    four = depth_far(after(four, theirs, ends))
    four = depth_join(after(four, ends_got), odd)
    grad_query, grad_key, grad_value, grad_out = finish(four, 0, 4)
    (grad_down,) = finish(down_total, 1, 1)
    (grad_up,) = finish(jnp.concatenate([up_total[i * h : (i + 1) * h] for i in range(ups)], axis=1), 0, 1)
    return (
        layer_out, grad_inputs, gains[0], gains[1], grad_query, grad_key, grad_value, grad_out.T, gains[2], gains[3],
        grad_up, up_bias, grad_down, gains[4],
    )


def whole_sequences(mesh):
    return mesh.shape["row"] == 4 and mesh.shape["col"] == 2 and mesh.shape["dp"] == 4


def placements(row):
    tokens = P(("dp", "col"), row)
    rows = P(row)
    weight = P(row, "col")
    turned = P("col", row)
    placed = (
        tokens, rows, rows, weight, weight, weight, turned, rows, rows, weight, P("col"), turned, rows,
        P(("dp", *row), None), P("col", None, None), P(), tokens,
    )
    given = (
        tokens, tokens, rows, rows, weight, weight, weight, turned, rows, rows, weight, P("col"), turned, rows,
    )
    return placed, given


def solution(mesh):
    sizes = mesh.shape
    split = jax.sharding.Mesh(
        mesh.devices.reshape(sizes["dp"], sizes["row"] // 2, 2, sizes["col"]), ("dp", "y", "core", "col")
    )

    def run(*arrays):
        tokens, length = arrays[0].shape[0], arrays[13].shape[1]
        if whole_sequences(mesh) and tokens == sizes["dp"] * sizes["col"] * 2 * length:
            placed, given = placements(("y", "core"))
            step = jax.shard_map(fast_body, mesh=split, in_specs=placed, out_specs=given, check_vma=False)
        else:
            placed, given = placements(("row",))
            step = jax.shard_map(body, mesh=mesh, in_specs=placed, out_specs=given, check_vma=False)
        return step(*arrays)

    return run
```

```python
import math

import jax
import jax.numpy as jnp
from jax import lax
from jax.experimental import pallas as pl
from jax.experimental.pallas import tpu as pltpu
from jax.sharding import PartitionSpec as P

D = 1024
HD = 64
BLK = 64
NB = 16


EPS = 1e-05


def product(picked, weight, flipped):
    if flipped:
        return lax.dot_general(
            picked, weight, (((1,), (1,)), ((), ())), preferred_element_type=jnp.float32
        )
    return jnp.dot(picked, weight, preferred_element_type=jnp.float32)


def to_columns(moving, weight, flipped):
    gathered = lax.all_gather(moving, "col", axis=0, tiled=True)
    row_count = gathered.shape[0] // lax.axis_size("row")

    def term_rows(first_row, how_many):
        return product(gathered, weight, flipped)

    result = lax.psum_scatter(
        term_rows(jnp.int32(0), lax.axis_size("row") * row_count),
        "row",
        scatter_dimension=0,
        tiled=True,
    )
    return (result, gathered)


def to_rows(moving, weight, flipped):
    gathered = lax.all_gather(moving, "row", axis=0, tiled=True)
    row_count = gathered.shape[0] // lax.axis_size("col")

    def term_rows(first_row, how_many):
        return product(gathered, weight, flipped)

    return (
        lax.psum_scatter(
            term_rows(jnp.int32(0), lax.axis_size("col") * row_count),
            "col",
            scatter_dimension=0,
            tiled=True,
        ),
        gathered,
    )


def norm_sums(first_sum, second_sum):
    return lax.psum((first_sum, second_sum), "row")


def norm_forward(moving, gain_row, shift_row):
    totals, squares = norm_sums(jnp.sum(moving, axis=1), jnp.sum(moving * moving, axis=1))
    center = totals / D
    spread = squares / D - center * center
    inverse = lax.rsqrt(spread + EPS)
    normed = (moving - center[:, None]) * inverse[:, None]
    return (normed * gain_row + shift_row, normed, inverse)


def norm_backward(upstream, normed, inverse, gain_row):
    scaled = upstream * gain_row
    first_sum, second_sum = norm_sums(jnp.sum(scaled, axis=1), jnp.sum(scaled * normed, axis=1))
    return inverse[:, None] * (scaled - first_sum[:, None] / D - normed * (second_sum[:, None] / D))


def head_masks(random_blocks, global_blocks):
    block_ids = jnp.arange(NB, dtype=jnp.int32)
    nearby = jnp.abs(block_ids[:, None] - block_ids[None, :]) <= 1
    chosen = jnp.any(random_blocks[:, :, :, None] == block_ids[None, None, None, :], axis=2)
    marked = jnp.any(global_blocks[:, None] == block_ids[None, :], axis=0)
    block_table = nearby[None] | chosen | marked[None, None, :] | marked[None, :, None]
    return jnp.repeat(jnp.repeat(block_table, BLK, axis=1), BLK, axis=2)


def seq_logits(seq_queries, seq_keys, labels, pattern):
    same_doc = (labels[:, None] == labels[None, :]) & (labels[None, :] != 0)
    raw_scores = jnp.einsum(
        "qhd,khd->hqk", seq_queries, seq_keys, preferred_element_type=jnp.float32
    )
    return jnp.where(pattern & same_doc[None], raw_scores * (1.0 / math.sqrt(HD)), -1000000000.0)


def attend_plain(queries, key_block, value_block, segments, pattern):

    def one_seq(pieces):
        seq_queries, seq_keys, seq_values, labels = pieces
        logits = seq_logits(seq_queries, seq_keys, labels, pattern)
        row_peak = jnp.max(logits, axis=2, keepdims=True)
        exp_terms = jnp.exp(logits - row_peak)
        row_total = jnp.sum(exp_terms, axis=2, keepdims=True)
        softmax = (exp_terms / row_total).astype(jnp.bfloat16)
        attended = jnp.einsum(
            "hqk,khd->qhd", softmax, seq_values, preferred_element_type=jnp.float32
        )
        live_rows = (labels != 0).astype(jnp.float32)
        return (attended * live_rows[:, None, None], (row_peak + jnp.log(row_total))[:, :, 0])

    return lax.map(one_seq, (queries, key_block, value_block, segments))


def attend_plain_backward(queries, key_block, value_block, segments, pattern, grad_heads, log_total):

    def one_seq(pieces):
        seq_queries, seq_keys, seq_values, labels, seq_grads, seq_log = pieces
        logits = seq_logits(seq_queries, seq_keys, labels, pattern)
        softmax = jnp.exp(logits - seq_log[:, :, None])
        grad_probs = jnp.einsum(
            "qhd,khd->hqk", seq_grads, seq_values, preferred_element_type=jnp.float32
        )
        grad_values = jnp.einsum(
            "hqk,qhd->khd",
            softmax.astype(jnp.bfloat16),
            seq_grads,
            preferred_element_type=jnp.float32,
        )
        inner_sum = jnp.sum(softmax * grad_probs, axis=2, keepdims=True)
        grad_raw = (softmax * (grad_probs - inner_sum) * (1.0 / math.sqrt(HD))).astype(jnp.bfloat16)
        grad_queries = jnp.einsum(
            "hqk,khd->qhd", grad_raw, seq_keys, preferred_element_type=jnp.float32
        )
        grad_keys = jnp.einsum(
            "hqk,qhd->khd", grad_raw, seq_queries, preferred_element_type=jnp.float32
        )
        return (grad_queries, grad_keys, grad_values)

    return lax.map(one_seq, (queries, key_block, value_block, segments, grad_heads, log_total))


def gelu_tanh(values):
    return jax.nn.gelu(values, approximate=True)


def weight_grad(left, right):
    return lax.dot_general(
        left, right, (((0,), (0,)), ((), ())), preferred_element_type=jnp.float32
    )


def body(
    inputs,
    gain_first,
    shift_first,
    w_query,
    w_key,
    w_value,
    w_output,
    gain_second,
    shift_second,
    w_up,
    bias_up,
    w_down,
    bias_down,
    segments,
    random_blocks,
    global_blocks,
    cotangent,
):
    seq_count, seq_len = segments.shape
    head_width = w_query.shape[1]
    heads_here = random_blocks.shape[0]
    seq_shape = (seq_count, seq_len, heads_here, HD)
    pattern = head_masks(random_blocks, global_blocks)
    live_tokens = (segments != 0).reshape(-1)
    x_first = inputs.astype(jnp.float32)
    first_full, normed_one, inverse_one = norm_forward(x_first, gain_first, shift_first)
    first_low = first_full.astype(jnp.bfloat16)
    stacked = jnp.concatenate((w_query, w_key, w_value), axis=1)
    projected, first_all = to_columns(first_low, stacked, False)
    proj_low = projected.astype(jnp.bfloat16)
    queries = proj_low[:, :head_width].reshape(seq_shape)
    key_block = proj_low[:, head_width : 2 * head_width].reshape(seq_shape)
    value_block = proj_low[:, 2 * head_width :].reshape(seq_shape)
    heads_out, log_total = attend_plain(queries, key_block, value_block, segments, pattern)
    heads_low = heads_out.reshape(-1, head_width).astype(jnp.bfloat16)
    mixed_out, heads_all = to_rows(heads_low, w_output, False)
    residual = x_first + mixed_out
    second_full, normed_two, inverse_two = norm_forward(residual, gain_second, shift_second)
    second_low = second_full.astype(jnp.bfloat16)
    upward, second_all = to_columns(second_low, w_up, False)
    upward = upward + bias_up
    hidden_low = gelu_tanh(upward).astype(jnp.bfloat16)
    downward, hidden_all = to_rows(hidden_low, w_down, False)
    layer_out = (residual + (downward + bias_down)).astype(jnp.bfloat16)
    grad_hidden, cotangent_all = to_columns(cotangent, w_down, True)
    activated, pull_back = jax.vjp(gelu_tanh, upward)
    grad_upward = pull_back(grad_hidden)[0].astype(jnp.bfloat16)
    grad_second, grad_upward_all = to_rows(grad_upward, w_up, True)
    grad_residual = cotangent.astype(jnp.float32) + norm_backward(
        grad_second, normed_two, inverse_two, gain_second
    )
    grad_mixed = grad_residual.astype(jnp.bfloat16)
    grad_heads, grad_mixed_all = to_columns(grad_mixed, w_output, True)
    grad_heads = jnp.where(live_tokens[:, None], grad_heads, 0.0).astype(jnp.bfloat16)
    grad_queries, grad_keys, grad_values = attend_plain_backward(
        queries, key_block, value_block, segments, pattern, grad_heads.reshape(seq_shape), log_total
    )
    grad_proj = jnp.concatenate(
        (
            grad_queries.reshape(-1, head_width),
            grad_keys.reshape(-1, head_width),
            grad_values.reshape(-1, head_width),
        ),
        axis=1,
    ).astype(jnp.bfloat16)
    grad_first, grad_proj_all = to_rows(grad_proj, stacked, True)
    grad_inputs = grad_residual + norm_backward(grad_first, normed_one, inverse_one, gain_first)
    grad_stacked = weight_grad(first_all, grad_proj_all)
    grad_out_weight = weight_grad(heads_all, grad_mixed_all)
    grad_up_weight = weight_grad(second_all, grad_upward_all)
    grad_down_weight = weight_grad(hidden_all, cotangent_all)
    grad_up_bias = jnp.sum(grad_upward_all, axis=0, dtype=jnp.float32)
    grad_down_bias = jnp.sum(cotangent_all, axis=0, dtype=jnp.float32)
    gain_terms = lax.psum(
        (
            jnp.sum(grad_first * normed_one, axis=0),
            jnp.sum(grad_first, axis=0),
            jnp.sum(grad_second * normed_two, axis=0),
            jnp.sum(grad_second, axis=0),
        ),
        ("dp", "col"),
    )
    summed = (
        lax.psum(grad_stacked.astype(jnp.bfloat16), "dp").astype(jnp.float32),
        lax.psum(grad_out_weight.astype(jnp.bfloat16), "dp").astype(jnp.float32),
        lax.psum(grad_up_weight.astype(jnp.bfloat16), "dp").astype(jnp.float32),
        lax.psum(grad_down_weight.astype(jnp.bfloat16), "dp").astype(jnp.float32),
        lax.psum(grad_up_bias.astype(jnp.bfloat16), "dp").astype(jnp.float32),
        lax.psum(grad_down_bias.astype(jnp.bfloat16), "dp").astype(jnp.float32),
    )
    return (
        layer_out,
        grad_inputs,
        gain_terms[0],
        gain_terms[1],
        summed[0][:, :head_width],
        summed[0][:, head_width : 2 * head_width],
        summed[0][:, 2 * head_width :],
        summed[1],
        gain_terms[2],
        gain_terms[3],
        summed[2],
        summed[4],
        summed[3],
        summed[5],
    )


SWAP = [(0, 1), (1, 0)]
LOW = jnp.bfloat16
FULL = jnp.float32
TILE = 256
BIG = 1e30


def swap(array, axis):
    return lax.ppermute(array, axis, SWAP)


def dot_nn(left, right):
    return lax.dot_general(left, right, (((1,), (0,)), ((), ())), preferred_element_type=FULL)


def dot_nt(left, right):
    return lax.dot_general(left, right, (((1,), (1,)), ((), ())), preferred_element_type=FULL)


def dot_tn(left, right):
    return lax.dot_general(left, right, (((0,), (0,)), ((), ())), preferred_element_type=FULL)


def attention_extras(labels, random_blocks, global_blocks):
    length = labels.shape[0]
    blocks = length // BLK
    block_ids = jnp.arange(blocks, dtype=jnp.int32)
    nearby = jnp.abs(block_ids[:, None] - block_ids[None, :]) <= 1
    chosen = jnp.any(random_blocks[:, :, :, None] == block_ids[None, None, None, :], axis=2)
    marked = jnp.any(global_blocks[:, None] == block_ids[None, :], axis=0)
    table = nearby[None] | chosen | marked[None, None, :] | marked[None, :, None]
    heads = table.shape[0]
    lane = jnp.arange(HD, dtype=jnp.int32)
    place = jnp.arange(length, dtype=jnp.int32) // BLK
    doc_lane = blocks + jnp.where(labels == 0, 4, labels - 1)
    row_extra = ((lane[None, :] == place[:, None]) | (lane[None, :] == doc_lane[:, None])).astype(LOW)
    table_keys = jnp.pad(jnp.swapaxes(table, 1, 2), ((0, 0), (0, 0), (0, HD - blocks)), constant_values=True)
    table_keys = jnp.repeat(table_keys, BLK, axis=1)
    is_doc = (lane >= blocks) & (lane <= blocks + 4)
    doc_bad = is_doc[None, :] & (lane[None, :] != doc_lane[:, None])
    doc_bad = doc_bad | (lane[None, :] == blocks + 4)
    key_extra = jnp.where(table_keys & ~doc_bad[None], 0.0, -BIG)
    key_extra = jnp.where((lane >= blocks + 5) & (lane <= blocks + 7), 1.0, key_extra).astype(LOW)
    rows = jnp.stack((jnp.pad(row_extra, ((0, 0), (HD, 0))), jnp.pad(row_extra, ((0, 0), (0, HD)))))
    even = jnp.pad(key_extra[0::2], ((0, 0), (0, 0), (HD, 0)))
    odd = jnp.pad(key_extra[1::2], ((0, 0), (0, 0), (0, HD)))
    keys = jnp.stack((even, odd), axis=1).reshape(heads, length, 2 * HD)
    tiles = length // TILE
    known = labels[None, :] == jnp.arange(1, 5, dtype=jnp.int32)[:, None]
    present = jnp.any(known.reshape(4, tiles, TILE), axis=2)
    wanted = jnp.any(present[:, :, None] & known[:, None, :], axis=0)
    spots = jnp.arange(length, dtype=jnp.int32)
    first = jnp.min(jnp.where(wanted, spots[None, :], length - 1), axis=1)
    last = jnp.max(jnp.where(wanted, spots[None, :], 0), axis=1)
    start = first // 128
    count = jnp.maximum((last + 1 - start * 128 + 255) // 256, 1)
    start = jnp.minimum(start, length // 128 - 2 * count)
    return rows, keys, jnp.stack((start, count)).astype(jnp.int32)


def attend_forward_kernel(where_ref, q_ref, k_ref, v_ref, rows_ref, keys_ref, out_ref, kept_ref, kk, vv):
    length = q_ref.shape[0]
    lane = lax.broadcasted_iota(jnp.int32, (length, 2 * HD), 1)
    for e in range(2):
        data = (lane < HD) if e == 0 else (lane >= HD)
        kk[e] = jnp.where(data, k_ref[...], keys_ref[e])
        vv[e] = jnp.where(data, v_ref[...], jnp.ones_like(v_ref[...]))
    tile_lane = lax.broadcasted_iota(jnp.int32, (TILE, 2 * HD), 1)

    def one_tile(t, carry):
        rows = pl.ds(pl.multiple_of(t * TILE, TILE), TILE)
        start = pl.multiple_of(where_ref[0, t] * 128, 128)
        count = where_ref[1, t]
        q_pair = q_ref[rows, :] * jnp.bfloat16(1.0 / math.sqrt(HD))
        for n in range(1, length // TILE + 1):

            @pl.when(count == n)
            def _():
                span = pl.ds(start, n * TILE)
                outs = []
                for e in range(2):
                    data = (tile_lane < HD) if e == 0 else (tile_lane >= HD)
                    base = HD if e == 0 else 0
                    extra = rows_ref[e, rows, :]
                    q_one = jnp.where(data, q_pair, extra)
                    logits = dot_nt(q_one, kk[e, span, :])
                    peak = jnp.max(logits, axis=1, keepdims=True)
                    terms = jnp.exp(logits - peak)
                    mixed = dot_nn(terms.astype(LOW), vv[e, span, :])
                    total = pltpu.roll(mixed, HD, 1)
                    outs.append(mixed / total)
                    total_one = jnp.max(jnp.where(data, total, 0.0), axis=1, keepdims=True)
                    padded = jnp.max(
                        jnp.where(tile_lane == base + 20, extra.astype(FULL), 0.0), axis=1, keepdims=True
                    )
                    log_total = jnp.where(padded > 0.5, 0.0, -(peak + jnp.log(total_one)))
                    high = log_total.astype(LOW).astype(FULL)
                    middle = (log_total - high).astype(LOW).astype(FULL)
                    low = log_total - high - middle
                    packed = jnp.where(tile_lane == base + 21, high, q_one.astype(FULL))
                    packed = jnp.where(tile_lane == base + 22, middle, packed)
                    packed = jnp.where(tile_lane == base + 23, low, packed)
                    kept_ref[e, rows, :] = packed.astype(LOW)
                joined = jnp.where(tile_lane < HD, outs[0], outs[1])
                out_ref[rows, :] = jnp.where(padded > 0.5, 0.0, joined).astype(LOW)

        return carry

    lax.fori_loop(0, length // TILE, one_tile, 0)


def attend_forward(qkv, rows_extra, keys_extra, where_table):
    length, width = qkv.shape
    pairs = width // (3 * 2 * HD)
    wide = 2 * HD
    return pl.pallas_call(
        attend_forward_kernel,
        out_shape=(
            jax.ShapeDtypeStruct((length, width // 3), LOW),
            jax.ShapeDtypeStruct((2 * pairs, length, wide), LOW),
        ),
        grid_spec=pltpu.PrefetchScalarGridSpec(
            num_scalar_prefetch=1,
            grid=(pairs,),
            in_specs=[
                pl.BlockSpec((length, wide), lambda p, w: (0, p)),
                pl.BlockSpec((length, wide), lambda p, w: (0, pairs + p)),
                pl.BlockSpec((length, wide), lambda p, w: (0, 2 * pairs + p)),
                pl.BlockSpec((2, length, wide), lambda p, w: (0, 0, 0)),
                pl.BlockSpec((2, length, wide), lambda p, w: (p, 0, 0)),
            ],
            out_specs=(
                pl.BlockSpec((length, wide), lambda p, w: (0, p)),
                pl.BlockSpec((2, length, wide), lambda p, w: (p, 0, 0)),
            ),
            scratch_shapes=[pltpu.VMEM((2, length, wide), LOW), pltpu.VMEM((2, length, wide), LOW)],
        ),
        name="attend_forward",
        cost_estimate=pl.CostEstimate(
            flops=8 * pairs * length * length * HD, bytes_accessed=16 * length * width, transcendentals=0
        ),
    )(where_table, qkv, qkv, qkv, rows_extra, keys_extra)


def attend_backward_kernel(
    where_ref, kept_ref, k_ref, v_ref, keys_ref, heads_ref, grads_ref, out_ref, kk, va, dk_sum, dv_sum
):
    length = k_ref.shape[0]
    wide = 2 * HD
    third = out_ref.shape[1] // 3
    pair = pl.program_id(0) * wide
    lane = lax.broadcasted_iota(jnp.int32, (length, wide), 1)
    for e in range(2):
        data = (lane < HD) if e == 0 else (lane >= HD)
        base = HD if e == 0 else 0
        kk[e] = jnp.where(data, k_ref[...], keys_ref[e])
        ones = jnp.where((lane == base) | (lane == base + 1), 1.0, 0.0).astype(LOW)
        va[e] = jnp.where(data, v_ref[...], ones)
    dk_sum[...] = jnp.zeros_like(dk_sum)
    dv_sum[...] = jnp.zeros_like(dv_sum)
    tile_lane = lax.broadcasted_iota(jnp.int32, (TILE, wide), 1)

    def one_tile(t, carry):
        rows = pl.ds(pl.multiple_of(t * TILE, TILE), TILE)
        start = pl.multiple_of(where_ref[0, t] * 128, 128)
        count = where_ref[1, t]
        grads = grads_ref[rows, :]
        both = grads.astype(FULL) * heads_ref[rows, :].astype(FULL)
        for n in range(1, length // TILE + 1):

            @pl.when(count == n)
            def _():
                span = pl.ds(start, n * TILE)
                outs = []
                for e in range(2):
                    data = (tile_lane < HD) if e == 0 else (tile_lane >= HD)
                    base = HD if e == 0 else 0
                    inner = -jnp.sum(jnp.where(data, both, 0.0), axis=1, keepdims=True)
                    high = inner.astype(LOW).astype(FULL)
                    only = jnp.where(data, grads, jnp.zeros_like(grads))
                    packed = jnp.where(tile_lane == base, high, only.astype(FULL))
                    packed = jnp.where(tile_lane == base + 1, inner - high, packed).astype(LOW)
                    q_one = kept_ref[e, rows, :]
                    q_only = jnp.where(data, q_one, jnp.zeros_like(q_one))
                    probs = jnp.exp(dot_nt(kk[e, span, :], q_one))
                    grad_raw = (probs * dot_nt(va[e, span, :], packed)).astype(LOW)
                    dv_sum[span, :] += dot_nn(probs.astype(LOW), only)
                    dk_sum[span, :] += dot_nn(grad_raw, q_only)
                    outs.append(dot_tn(grad_raw, kk[e, span, :]))
                joined = jnp.where(tile_lane < HD, outs[0], outs[1])
                lanes = pl.ds(pl.multiple_of(pair, wide), wide)
                out_ref[rows, lanes] = (joined * (1.0 / math.sqrt(HD))).astype(LOW)

        return carry

    lax.fori_loop(0, length // TILE, one_tile, 0)
    out_ref[:, pl.ds(pl.multiple_of(third + pair, wide), wide)] = dk_sum[...].astype(LOW)
    out_ref[:, pl.ds(pl.multiple_of(2 * third + pair, wide), wide)] = dv_sum[...].astype(LOW)


def attend_backward(kept, qkv, keys_extra, heads, grads, group, where_table):
    length, width = qkv.shape
    pairs = width // (3 * 2 * HD)
    wide = 2 * HD
    stacked = pl.BlockSpec((2, length, wide), lambda p, w: (p, 0, 0))
    return pl.pallas_call(
        attend_backward_kernel,
        out_shape=jax.ShapeDtypeStruct((length, width), LOW),
        grid_spec=pltpu.PrefetchScalarGridSpec(
            num_scalar_prefetch=1,
            grid=(pairs,),
            in_specs=[
                stacked,
                pl.BlockSpec((length, wide), lambda p, w: (0, pairs + p)),
                pl.BlockSpec((length, wide), lambda p, w: (0, 2 * pairs + p)),
                stacked,
                pl.BlockSpec((length, wide), lambda p, w: (0, p)),
                pl.BlockSpec((length, wide), lambda p, w: (0, group * pairs + p)),
            ],
            out_specs=pl.BlockSpec((length, width), lambda p, w: (0, 0)),
            scratch_shapes=[
                pltpu.VMEM((2, length, wide), LOW),
                pltpu.VMEM((2, length, wide), LOW),
                pltpu.VMEM((length, wide), FULL),
                pltpu.VMEM((length, wide), FULL),
            ],
        ),
        name="attend_backward",
        cost_estimate=pl.CostEstimate(
            flops=20 * pairs * length * length * HD, bytes_accessed=20 * length * width, transcendentals=0
        ),
    )(where_table, kept, qkv, qkv, keys_extra, heads, grads)


def row_tiles(count):
    def spec(width):
        return pl.BlockSpec((TILE, width), lambda t: (t, 0))

    return spec


def whole(shape):
    return pl.BlockSpec(shape, lambda t: (0,) * len(shape))


def cost(flops, moved):
    return pl.CostEstimate(flops=int(flops), bytes_accessed=int(moved), transcendentals=0)


def norm_parts(blocks):
    width = sum(b.shape[1] for b in blocks)
    total = sum(jnp.sum(b, axis=1, keepdims=True) for b in blocks)
    squares = sum(jnp.sum(b * b, axis=1, keepdims=True) for b in blocks)
    center = total / width
    return center, lax.rsqrt(squares / width - center * center + EPS)


def columns(ref, index, width):
    return ref[:, index * width : (index + 1) * width]


def first_norm_kernel(x0, x1, x2, x3, gain_ref, shift_ref, low_ref, high_ref):
    blocks = [x[...].astype(FULL) for x in (x0, x1, x2, x3)]
    n = blocks[0].shape[1]
    center, inverse = norm_parts(blocks)
    for i, block in enumerate(blocks):
        value = (block - center) * inverse * columns(gain_ref, i, n) + columns(shift_ref, i, n)
        (low_ref, high_ref)[i // 2][:, (i % 2) * n : (i % 2 + 1) * n] = value.astype(LOW)


def first_norm(blocks, gain, shift):
    length, n = blocks[0].shape
    rows = row_tiles(length)
    half = jax.ShapeDtypeStruct((length, 2 * n), LOW)
    return pl.pallas_call(
        first_norm_kernel,
        out_shape=(half, half),
        grid=(length // TILE,),
        in_specs=[rows(n)] * 4 + [whole((1, 4 * n))] * 2,
        out_specs=(rows(2 * n), rows(2 * n)),
        name="first_norm",
        cost_estimate=cost(20 * length * n, 16 * length * n),
    )(*blocks, gain, shift)


def second_norm_kernel(x0, x1, x2, x3, part_ref, got_ref, gain_ref, shift_ref, residual_ref, second_ref):
    n = x0.shape[1]
    blocks = []
    for i, x in enumerate((x0, x1, x2, x3)):
        mixed = columns(part_ref, i, n).astype(FULL) + columns(got_ref, i ^ 1, n).astype(FULL)
        blocks.append(x[...].astype(FULL) + mixed)
    center, inverse = norm_parts(blocks)
    for i, block in enumerate(blocks):
        residual_ref[:, i * n : (i + 1) * n] = block
        value = (block - center) * inverse * columns(gain_ref, i, n) + columns(shift_ref, i, n)
        second_ref[i // 2, :, (i % 2) * n : (i % 2 + 1) * n] = value.astype(LOW)


def second_norm(blocks, part, got, gain, shift):
    length, n = blocks[0].shape
    rows = row_tiles(length)
    return pl.pallas_call(
        second_norm_kernel,
        out_shape=(jax.ShapeDtypeStruct((length, 4 * n), FULL), jax.ShapeDtypeStruct((2, length, 2 * n), LOW)),
        grid=(length // TILE,),
        in_specs=[rows(n)] * 4 + [rows(4 * n)] * 2 + [whole((1, 4 * n))] * 2,
        out_specs=(rows(4 * n), pl.BlockSpec((2, TILE, 2 * n), lambda t: (0, t, 0))),
        name="second_norm",
        cost_estimate=cost(30 * length * n, 48 * length * n),
    )(*blocks, part, got, gain, shift)


def norm_gradient(blocks, part_ref, got_ref, gain_ref, sums_ref):
    n = blocks[0].shape[1]
    center, inverse = norm_parts(blocks)
    normed = [(b - center) * inverse for b in blocks]
    grads = [columns(part_ref, i, n).astype(FULL) + columns(got_ref, i ^ 1, n).astype(FULL) for i in range(4)]
    scaled = [g * columns(gain_ref, i, n) for i, g in enumerate(grads)]
    mean_one = sum(jnp.sum(s, axis=1, keepdims=True) for s in scaled) / (4 * n)
    mean_two = sum(jnp.sum(s * z, axis=1, keepdims=True) for s, z in zip(scaled, normed)) / (4 * n)

    @pl.when(pl.program_id(0) == 0)
    def _():
        sums_ref[...] = jnp.zeros_like(sums_ref)

    for slot, i in enumerate((0, 2)):
        place = slice(slot * n, (slot + 1) * n)
        sums_ref[0:1, place] += jnp.sum(grads[i] * normed[i], axis=0, keepdims=True)
        sums_ref[1:2, place] += jnp.sum(grads[i], axis=0, keepdims=True)
    return [inverse * (s - mean_one - z * mean_two) for s, z in zip(scaled, normed)]


def second_norm_back_kernel(
    residual_ref, part_ref, got_ref, cots_ref, gain_ref, own_ref, other_ref, mixed_ref, sums_ref
):
    n = residual_ref.shape[1] // 4
    blocks = [columns(residual_ref, i, n) for i in range(4)]
    for i, grad in enumerate(norm_gradient(blocks, part_ref, got_ref, gain_ref, sums_ref)):
        total = cots_ref[i // 2, :, (i % 2) * n : (i % 2 + 1) * n].astype(FULL) + grad
        mixed_ref[:, i * n : (i + 1) * n] = total.astype(LOW)
        if i % 2 == 0:
            (own_ref, other_ref)[i // 2][...] = total


def second_norm_back(residual, part, got, cots, gain):
    length, width = residual.shape
    n = width // 4
    rows = row_tiles(length)
    one = jax.ShapeDtypeStruct((length, n), FULL)
    return pl.pallas_call(
        second_norm_back_kernel,
        out_shape=(one, one, jax.ShapeDtypeStruct((length, width), LOW), jax.ShapeDtypeStruct((8, 2 * n), FULL)),
        grid=(length // TILE,),
        in_specs=[rows(width)] * 3 + [pl.BlockSpec((2, TILE, 2 * n), lambda t: (0, t, 0)), whole((1, width))],
        out_specs=(rows(n), rows(n), rows(width), whole((8, 2 * n))),
        name="second_norm_back",
        cost_estimate=cost(60 * length * n, 64 * length * n),
    )(residual, part, got, cots, gain)


def first_norm_back_kernel(
    x0, x1, x2, x3, part_ref, got_ref, own_ref, other_ref, gain_ref, mine_ref, theirs_ref, sums_ref
):
    blocks = [x[...].astype(FULL) for x in (x0, x1, x2, x3)]
    grads = norm_gradient(blocks, part_ref, got_ref, gain_ref, sums_ref)
    mine_ref[...] = own_ref[...] + grads[0]
    theirs_ref[...] = (other_ref[...] + grads[2]).astype(LOW)


def first_norm_back(blocks, part, got, own, other, gain):
    length, n = blocks[0].shape
    rows = row_tiles(length)
    return pl.pallas_call(
        first_norm_back_kernel,
        out_shape=(
            jax.ShapeDtypeStruct((length, n), FULL),
            jax.ShapeDtypeStruct((length, n), LOW),
            jax.ShapeDtypeStruct((8, 2 * n), FULL),
        ),
        grid=(length // TILE,),
        in_specs=[rows(n)] * 4 + [rows(4 * n)] * 2 + [rows(n)] * 2 + [whole((1, 4 * n))],
        out_specs=(rows(n), rows(n), whole((8, 2 * n))),
        name="first_norm_back",
        cost_estimate=cost(60 * length * n, 40 * length * n),
    )(*blocks, part, got, own, other, gain)


def mix_kernel(h0, h1, w0, w1, out_ref):
    out_ref[...] = (dot_nn(h0[...], w0[...]) + dot_nn(h1[...], w1[...])).astype(LOW)


def mix_heads(heads, weights):
    length, depth = heads[0].shape
    width = weights[0].shape[1]
    rows = row_tiles(length)
    return pl.pallas_call(
        mix_kernel,
        out_shape=jax.ShapeDtypeStruct((length, width), LOW),
        grid=(length // TILE,),
        in_specs=[rows(depth)] * 2 + [whole((depth, width))] * 2,
        out_specs=rows(width),
        name="mix_heads",
        cost_estimate=cost(4 * length * depth * width, 4 * length * (depth + width)),
    )(*heads, *weights)


ROOT = math.sqrt(2.0 / math.pi)


def feed_forward_kernel(
    at_ref, s_ref, c_ref, u_low, u_high, d_low, d_high, bias_ref, part_ref, hidden_ref, grad_ref, bias_sum, low_sum, high_sum
):
    step = pl.program_id(0)

    @pl.when(step == 0)
    def _():
        low_sum[...] = jnp.zeros_like(low_sum)
        high_sum[...] = jnp.zeros_like(high_sum)

    totals = 0.0
    for t in range(s_ref.shape[1] // TILE):
        rows = slice(t * TILE, (t + 1) * TILE)
        upward = dot_nn(s_ref[0, rows, :], u_low[0]) + dot_nn(s_ref[1, rows, :], u_high[0]) + bias_ref[0]
        grad_hidden = dot_nt(c_ref[0, rows, :], d_low[0]) + dot_nt(c_ref[1, rows, :], d_high[0])
        square = upward * upward
        bent = jnp.tanh(upward * (ROOT + (ROOT * 0.044715) * square))
        lifted = 0.5 + 0.5 * bent
        slope = lifted + (0.5 * upward) * (1.0 - bent * bent) * (ROOT + (ROOT * 3 * 0.044715) * square)
        hidden_ref[0, rows, :] = (upward * lifted).astype(LOW)
        grad = grad_hidden * slope
        totals = totals + jnp.sum(grad, axis=0, keepdims=True)
        grad = grad.astype(LOW)
        grad_ref[0, rows, :] = grad
        low_sum[rows, :] += dot_nt(grad, u_low[0])
        high_sum[rows, :] += dot_nt(grad, u_high[0])
    bias_sum[0] = jnp.broadcast_to(totals, bias_sum.shape[1:])

    @pl.when(step == pl.num_programs(0) - 1)
    def _():
        n = low_sum.shape[1]
        part_ref[:, :n] = low_sum[...].astype(LOW)
        part_ref[:, n:] = high_sum[...].astype(LOW)


def feed_forward(at, seconds, cots, weights, biases):
    _, length, h = seconds.shape
    each = weights.shape[1] // 2
    tiles = each // TILE
    per = h // TILE
    keep = pl.BlockSpec((2, length, h), lambda i, at: (0, 0, 0))

    def up_spec(flip):
        return pl.BlockSpec(
            (1, h, TILE),
            lambda i, at: (
                (at[0] ^ flip) * 2 + (at[1] ^ (i // tiles)), lax.rem(i, tiles) // per, lax.rem(lax.rem(i, tiles), per)
            ),
        )

    def down_spec(flip):
        return pl.BlockSpec(
            (1, TILE, h), lambda i, at: ((at[0] ^ flip) * 2 + (at[1] ^ (i // tiles)), tiles + lax.rem(i, tiles), 0)
        )

    side = pl.BlockSpec((1, length, TILE), lambda i, at: (i // tiles, 0, lax.rem(i, tiles)))
    one = jax.ShapeDtypeStruct((2, length, each), LOW)
    return pl.pallas_call(
        feed_forward_kernel,
        out_shape=(
            jax.ShapeDtypeStruct((length, 2 * h), LOW), one, one, jax.ShapeDtypeStruct((2 * tiles, 8, TILE), FULL),
        ),
        grid_spec=pltpu.PrefetchScalarGridSpec(
            num_scalar_prefetch=1,
            grid=(2 * tiles,),
            in_specs=[keep] * 2
            + [up_spec(0), up_spec(1), down_spec(0), down_spec(1)]
            + [pl.BlockSpec((1, 1, TILE), lambda i, at: (i, 0, 0))],
            out_specs=(
                pl.BlockSpec((length, 2 * h), lambda i, at: (0, 0)), side, side,
                pl.BlockSpec((1, 8, TILE), lambda i, at: (i, 0, 0)),
            ),
            scratch_shapes=[pltpu.VMEM((length, h), FULL), pltpu.VMEM((length, h), FULL)],
        ),
        name="feed_forward",
        cost_estimate=cost(12 * length * 2 * h * each, 8 * length * h + 16 * h * each + 16 * length * each),
    )(at, seconds, cots, weights, weights, weights, weights, biases.reshape(2 * tiles, 1, TILE))


def up_grads_kernel(at_ref, s_ref, grad_ref, out_ref, turned):
    h = out_ref.shape[2]

    @pl.when(pl.program_id(1) == 0)
    def _():
        turned[...] = s_ref[0].T

    for i in range(out_ref.shape[1] // h):
        part = dot_nn(turned[...], grad_ref[0, :, i * h : (i + 1) * h])
        out_ref[0, i * h : (i + 1) * h, :] = part.astype(LOW)


def up_grads(at, seconds, grads):
    _, length, h = seconds.shape
    each = grads.shape[2]
    return pl.pallas_call(
        up_grads_kernel,
        out_shape=jax.ShapeDtypeStruct((4, each, h), LOW),
        grid_spec=pltpu.PrefetchScalarGridSpec(
            num_scalar_prefetch=1,
            grid=(2, 2),
            in_specs=[
                pl.BlockSpec((1, length, h), lambda y, c, at: (y, 0, 0)),
                pl.BlockSpec((1, length, each), lambda y, c, at: (c, 0, 0)),
            ],
            out_specs=pl.BlockSpec((1, each, h), lambda y, c, at: ((at[0] ^ y) * 2 + (at[1] ^ c), 0, 0)),
            scratch_shapes=[pltpu.VMEM((h, length), LOW)],
        ),
        name="up_grads",
        cost_estimate=cost(8 * length * h * each, 4 * length * each + 8 * h * each),
    )(at, seconds, grads)


def down_grads_kernel(at_ref, hidden_ref, c_ref, out_ref):
    turned = hidden_ref[0].T
    for y in range(2):
        out_ref[at_ref[0] ^ y, 0] = dot_nn(turned, c_ref[y]).astype(LOW)


def down_grads(at, hiddens, cots):
    _, length, h = cots.shape
    each = hiddens.shape[2]
    return pl.pallas_call(
        down_grads_kernel,
        out_shape=jax.ShapeDtypeStruct((2, 2, each, h), LOW),
        grid_spec=pltpu.PrefetchScalarGridSpec(
            num_scalar_prefetch=1,
            grid=(2, each // h),
            in_specs=[
                pl.BlockSpec((1, length, h), lambda c, b, at: (c, 0, b)),
                pl.BlockSpec((2, length, h), lambda c, b, at: (0, 0, 0)),
            ],
            out_specs=pl.BlockSpec((2, 1, h, h), lambda c, b, at: (0, at[1] ^ c, b, 0)),
        ),
        name="down_grads",
        cost_estimate=cost(8 * length * h * each, 4 * length * each + 8 * h * each),
    )(at, hiddens, cots)


def layer_end_kernel(at_ref, h0, h1, w00, w01, w10, w11, own_ref, theirs_ref):
    n = own_ref.shape[1] // 2
    for j, (a, b) in enumerate(((w00, w01), (w10, w11))):
        part = dot_nn(h0[0], a[0]) + dot_nn(h1[0], b[0])
        own_ref[:, j * n : (j + 1) * n] = part[:, :n]
        theirs_ref[:, j * n : (j + 1) * n] = part[:, n:].astype(LOW)


def layer_end(at, hiddens, weights):
    _, length, each = hiddens.shape
    h = weights.shape[2]
    out = pl.BlockSpec((TILE, h), lambda t, at: (t, 0))

    def rows(c):
        return pl.BlockSpec((1, TILE, each), lambda t, at: (c, t, 0))

    def weight(y, col):
        return pl.BlockSpec((1, each, h), lambda t, at: ((at[0] ^ y) * 2 + (at[1] ^ col), 1, 0))

    return pl.pallas_call(
        layer_end_kernel,
        out_shape=(jax.ShapeDtypeStruct((length, h), FULL), jax.ShapeDtypeStruct((length, h), LOW)),
        grid_spec=pltpu.PrefetchScalarGridSpec(
            num_scalar_prefetch=1,
            grid=(length // TILE,),
            in_specs=[rows(0), rows(1), weight(0, 0), weight(0, 1), weight(1, 0), weight(1, 1)],
            out_specs=(out, out),
        ),
        name="layer_end",
        cost_estimate=cost(8 * length * h * each, 8 * h * each + 12 * length * h),
    )(at, hiddens, hiddens, weights, weights, weights, weights)


def after(values, *late):
    return lax.optimization_barrier((values, late))[0]


def pick(pair, index):
    return lax.dynamic_index_in_dim(pair, index, 0, keepdims=False)


def ordered(own, other, index):
    flip = index == 0
    return jnp.stack((jnp.where(flip, own, other), jnp.where(flip, other, own)))


def swap_across(array):
    return lax.ppermute(array, ("y", "col"), [(0, 3), (3, 0), (1, 2), (2, 1)])


def plane_gather(block):
    return block, swap(block, "y"), swap(block, "col"), swap_across(block)


def plane_exchange(at_y, at_col, across):
    return swap(at_y, "y"), swap(at_col, "col"), swap_across(across)


def plane_sum(own, got):
    return (own.astype(FULL) + sum(g.astype(FULL) for g in got)).astype(LOW)


def add_low(left, right):
    return (left.astype(FULL) + right.astype(FULL)).astype(LOW)


PAIRS = [(0, 1), (1, 0), (2, 3), (3, 2)]
FAR = [(0, 2), (2, 0), (1, 3), (3, 1)]


def depth_pair(array, odd):
    halves = array.reshape(2, array.shape[0] // 2, array.shape[1])
    return add_low(pick(halves, odd), lax.ppermute(pick(halves, 1 - odd), "dp", PAIRS))


def depth_far(part):
    return add_low(part, lax.ppermute(part, "dp", FAR))


def depth_join(part, odd):
    return ordered(part, lax.ppermute(part, "dp", PAIRS), odd).reshape(-1, part.shape[1])


def half(weight, axis, index):
    size = weight.shape[axis] // 2
    return lax.dynamic_slice_in_dim(weight, index * size, size, axis)


def fast_body(
    inputs, gain_first, shift_first, w_query, w_key, w_value, w_output, gain_second, shift_second,
    w_up, bias_up, w_down, bias_down, segments, random_blocks, global_blocks, cotangent,
):
    depth_at, y_at, core_at, col_at = (lax.axis_index(name) for name in ("dp", "y", "core", "col"))
    length = segments.shape[1]
    n = inputs.shape[1]
    h = 2 * n
    at = jnp.stack((y_at, col_at)).astype(jnp.int32)

    def chip_block(weights, axis, join):
        mine = jnp.concatenate([half(w, axis, core_at) for w in weights], axis=axis)
        theirs = swap(jnp.concatenate([half(w, axis, 1 - core_at) for w in weights], axis=axis), "core")
        return jnp.concatenate((mine, theirs), axis=join)

    inputs_pair = inputs.reshape(2, length, n)
    x_own = pick(inputs_pair, y_at)
    x_y = swap(pick(inputs_pair, 1 - y_at), "y")
    qkv_block = chip_block((w_query, w_key, w_value), 1, 0)
    qkv_own, qkv_y, qkv_x, qkv_xy = plane_gather(qkv_block)
    xs = (x_own, swap(x_own, "core"), x_y, swap(x_y, "core"))
    w_up, w_down = after((w_up, w_down), qkv_block)
    up_block, down_block = chip_block((w_up,), 1, 0), chip_block((w_down,), 0, 1)
    ups = up_block.shape[1] // h
    ffn_block = jnp.concatenate([up_block[:, i * h : (i + 1) * h] for i in range(ups)] + [down_block])
    ffn_block, w_output, cotangent_late = after((ffn_block, w_output, cotangent), qkv_y, qkv_x)
    ffn = lax.all_gather(ffn_block, ("y", "col"), axis=0, tiled=False)
    out_own, out_y, out_x, out_xy = plane_gather(chip_block((w_output,), 0, 1))
    cot_pair = cotangent_late.reshape(2, length, n)

    vectors = jnp.stack((gain_first, shift_first, gain_second, shift_second, bias_down))
    vectors = jnp.concatenate((vectors, swap(vectors, "core")), axis=1)
    vectors = jnp.concatenate((vectors, swap(vectors, "y")), axis=1)
    gain_one, shift_one, gain_two, shift_two, bias_low = (vectors[i : i + 1] for i in range(5))
    heads_half = half(random_blocks, 0, core_at)
    hidden_bias = half(bias_up, 0, core_at)
    each = hidden_bias.shape[0]
    small = swap(jnp.concatenate((hidden_bias, heads_half.astype(FULL).reshape(-1))), "col")
    biases = jnp.concatenate((hidden_bias, small[:each]))
    heads_half_x = small[each:].reshape(heads_half.shape).astype(jnp.int32)
    moves = []
    for y in range(2):
        for core in range(2):
            for col in range(2):
                moves.append(((col * 2 + y) * 2 + core, (y * 2 + core) * 2 + col))
    labels = lax.ppermute(segments, ("y", "core", "col"), moves)[0]
    all_heads = jnp.concatenate((heads_half, heads_half_x), axis=0)
    rows_extra, keys_extra, where_table = attention_extras(labels, all_heads, global_blocks)
    near_heads = heads_half.shape[0]
    keys_of = (keys_extra[:near_heads], keys_extra[near_heads:])
    live = (labels != 0)[:, None]

    cot_own = pick(cot_pair, y_at)
    cot_y = swap(pick(cot_pair, 1 - y_at), "y")
    cot_swapped = swap(cot_y, "core")
    cots = jnp.stack([jnp.concatenate(c, axis=1) for c in ((cot_own, swap(cot_own, "core")), (cot_y, cot_swapped))])

    firsts = first_norm(after(xs, qkv_xy), gain_one, shift_one)
    qkv_x = after(qkv_x, out_y, out_x, out_xy, cot_y)
    w_qkv = (jnp.concatenate((qkv_own, qkv_y), axis=0), jnp.concatenate((qkv_x, qkv_xy), axis=0))
    first = jnp.concatenate(firsts, axis=1)
    out_own = after(out_own, cots)
    w_out = (jnp.concatenate((out_own, out_y), axis=1), jnp.concatenate((out_x, out_xy), axis=1))
    qkv, heads, kept = [], [], []
    for i in range(2):
        qkv.append(dot_nn(first, w_qkv[i]).astype(LOW))
        done, saved = attend_forward(qkv[i], rows_extra, keys_of[i], where_table)
        heads.append(done)
        kept.append(saved)
    mixed_part = mix_heads(heads, w_out)
    residual, seconds = second_norm(xs, mixed_part, swap(mixed_part, "core"), gain_two, shift_two)

    second_part, hiddens, up_sides, bias_sum = feed_forward(at, seconds, cots, ffn, biases)
    down_parts = down_grads(at, hiddens, cots).reshape(4, -1, h)
    down_scattered = lax.psum_scatter(down_parts, ("y", "col"), scatter_dimension=0, tiled=True)[0]
    up_parts = up_grads(at, seconds, after(up_sides, down_parts))
    up_scattered = lax.psum_scatter(up_parts, ("y", "col"), scatter_dimension=0, tiled=True)[0]
    second_got = after(swap(second_part, "core"), up_parts)

    grad_own, grad_other, grad_mixed, sums_two = second_norm_back(residual, second_part, second_got, cots, gain_two)
    grads = jnp.where(live, dot_nt(grad_mixed, jnp.concatenate(w_out, axis=0)), 0.0).astype(LOW)
    out_grads = [[dot_tn(grad_mixed[:, j * h : (j + 1) * h], head).astype(LOW) for j in range(2)] for head in heads]
    qkv_sides, qkv_grads = [None, None], [None, None]
    for i in (1, 0):
        qkv_sides[i] = attend_backward(kept[i], qkv[i], keys_of[i], heads[i], grads, i, where_table)
        qkv_grads[i] = [dot_tn(f, qkv_sides[i]).astype(LOW) for f in firsts]
    odd = lax.rem(depth_at, 2)
    out_got = plane_exchange(out_grads[0][1], out_grads[1][0], out_grads[1][1])
    qkv_sides = after(qkv_sides, qkv_grads)
    first_part = dot_nt(jnp.concatenate(qkv_sides, axis=1), jnp.concatenate(w_qkv, axis=1)).astype(LOW)
    down_part = depth_pair(after(down_scattered, qkv_sides[0]), odd)
    down_part = depth_far(down_part)
    first_part = after(first_part, out_got, down_part)
    mine, theirs, sums_one = first_norm_back(xs, first_part, swap(first_part, "core"), grad_own, grad_other, gain_one)

    gains = jnp.concatenate((sums_one[:2, :n], sums_two[:2, :n])).reshape(-1)
    gains_y = jnp.concatenate((sums_one[:2, n:], sums_two[:2, n:])).reshape(-1)
    up_bias = bias_sum[:, 0, :].reshape(-1)
    got = swap(jnp.concatenate((gains_y, up_bias)), "y")
    gains = gains + got[: 4 * n]
    up_bias = up_bias + got[4 * n :]
    near = jnp.concatenate((gains, jnp.sum(cotangent, axis=0, dtype=FULL), up_bias[:each]))
    near = near + swap(jnp.concatenate((near[: 5 * n], up_bias[each:])), "col")
    up_scattered = after(up_scattered, near)
    up_part = depth_pair(up_scattered, odd)
    qkv_got = plane_exchange(*after((qkv_grads[0][1], qkv_grads[1][0], qkv_grads[1][1]), up_scattered))
    up_far = depth_far(up_part)
    theirs = swap(after(theirs, up_far), "y")
    grad_inputs = ordered(mine, theirs.astype(FULL), y_at).reshape(2 * length, n)
    ends_own, ends_other = layer_end(at, after(hiddens, up_part), ffn)
    down_total = depth_join(after(down_part, up_far), odd)
    kept_two = jnp.concatenate((residual[:, :n], residual[:, 2 * n : 3 * n]), axis=1)
    bias_two = jnp.concatenate((bias_low[:, :n], bias_low[:, 2 * n : 3 * n]), axis=1)
    ends = (kept_two + ends_own + swap(ends_other, "core").astype(FULL) + bias_two).astype(LOW)
    ends_got = swap(ends[:, n:], "y")
    layer_out = ordered(ends[:, :n], ends_got, y_at).reshape(2 * length, n)

    near = after(near, up_part)
    near = near + lax.ppermute(near, "dp", [(0, 1), (1, 0), (2, 3), (3, 2)])
    near = near + lax.ppermute(near, "dp", [(0, 2), (2, 0), (1, 3), (3, 1)])
    gains = near[: 5 * n].reshape(5, n)
    up_bias = ordered(near[5 * n :], swap(near[5 * n :], "core"), core_at).reshape(-1)

    def finish(total, axis, parts):
        keep = lax.slice_in_dim(total, 0, n, axis=axis)
        got = swap(lax.slice_in_dim(total, n, 2 * n, axis=axis), "core")
        size = keep.shape[1 - axis] // parts
        flip = core_at == 0
        out = []
        for i in range(parts):
            a, b = (lax.slice_in_dim(z, i * size, (i + 1) * size, axis=1 - axis) for z in (keep, got))
            out.append(jnp.concatenate((jnp.where(flip, a, b), jnp.where(flip, b, a)), axis=1 - axis).astype(FULL))
        return out

    four = jnp.concatenate(
        (plane_sum(after(qkv_grads[0][0], up_part), qkv_got), plane_sum(out_grads[0][0], out_got)), axis=1
    )
    four = depth_pair(after(four, up_far, near, ends_own), odd)
    up_total = depth_join(up_far, odd)
    four = depth_far(after(four, theirs, ends))
    four = depth_join(after(four, ends_got), odd)
    grad_query, grad_key, grad_value, grad_out = finish(four, 0, 4)
    (grad_down,) = finish(down_total, 1, 1)
    (grad_up,) = finish(jnp.concatenate([up_total[i * h : (i + 1) * h] for i in range(ups)], axis=1), 0, 1)
    return (
        layer_out, grad_inputs, gains[0], gains[1], grad_query, grad_key, grad_value, grad_out.T, gains[2], gains[3],
        grad_up, up_bias, grad_down, gains[4],
    )


def whole_sequences(mesh):
    return mesh.shape["row"] == 4 and mesh.shape["col"] == 2 and mesh.shape["dp"] == 4


def placements(row):
    tokens = P(("dp", "col"), row)
    rows = P(row)
    weight = P(row, "col")
    turned = P("col", row)
    placed = (
        tokens, rows, rows, weight, weight, weight, turned, rows, rows, weight, P("col"), turned, rows,
        P(("dp", *row), None), P("col", None, None), P(), tokens,
    )
    given = (
        tokens, tokens, rows, rows, weight, weight, weight, turned, rows, rows, weight, P("col"), turned, rows,
    )
    return placed, given


def solution(mesh):
    sizes = mesh.shape
    split = jax.sharding.Mesh(
        mesh.devices.reshape(sizes["dp"], sizes["row"] // 2, 2, sizes["col"]), ("dp", "y", "core", "col")
    )

    def run(*arrays):
        tokens, length = arrays[0].shape[0], arrays[13].shape[1]
        if whole_sequences(mesh) and tokens == sizes["dp"] * sizes["col"] * 2 * length:
            placed, given = placements(("y", "core"))
            step = jax.shard_map(fast_body, mesh=split, in_specs=placed, out_specs=given, check_vma=False)
        else:
            placed, given = placements(("row",))
            step = jax.shard_map(body, mesh=mesh, in_specs=placed, out_specs=given, check_vma=False)
        return step(*arrays)

    return run
```

```python
import math

import jax
import jax.numpy as jnp
from jax import lax
from jax.experimental import pallas as pl
from jax.experimental.pallas import tpu as pltpu
from jax.sharding import PartitionSpec as P

D = 1024
HD = 64
BLK = 64
NB = 16


EPS = 1e-05


def product(picked, weight, flipped):
    if flipped:
        return lax.dot_general(
            picked, weight, (((1,), (1,)), ((), ())), preferred_element_type=jnp.float32
        )
    return jnp.dot(picked, weight, preferred_element_type=jnp.float32)


def to_columns(moving, weight, flipped):
    gathered = lax.all_gather(moving, "col", axis=0, tiled=True)
    row_count = gathered.shape[0] // lax.axis_size("row")

    def term_rows(first_row, how_many):
        return product(gathered, weight, flipped)

    result = lax.psum_scatter(
        term_rows(jnp.int32(0), lax.axis_size("row") * row_count),
        "row",
        scatter_dimension=0,
        tiled=True,
    )
    return (result, gathered)


def to_rows(moving, weight, flipped):
    gathered = lax.all_gather(moving, "row", axis=0, tiled=True)
    row_count = gathered.shape[0] // lax.axis_size("col")

    def term_rows(first_row, how_many):
        return product(gathered, weight, flipped)

    return (
        lax.psum_scatter(
            term_rows(jnp.int32(0), lax.axis_size("col") * row_count),
            "col",
            scatter_dimension=0,
            tiled=True,
        ),
        gathered,
    )


def norm_sums(first_sum, second_sum):
    return lax.psum((first_sum, second_sum), "row")


def norm_forward(moving, gain_row, shift_row):
    totals, squares = norm_sums(jnp.sum(moving, axis=1), jnp.sum(moving * moving, axis=1))
    center = totals / D
    spread = squares / D - center * center
    inverse = lax.rsqrt(spread + EPS)
    normed = (moving - center[:, None]) * inverse[:, None]
    return (normed * gain_row + shift_row, normed, inverse)


def norm_backward(upstream, normed, inverse, gain_row):
    scaled = upstream * gain_row
    first_sum, second_sum = norm_sums(jnp.sum(scaled, axis=1), jnp.sum(scaled * normed, axis=1))
    return inverse[:, None] * (scaled - first_sum[:, None] / D - normed * (second_sum[:, None] / D))


def head_masks(random_blocks, global_blocks):
    block_ids = jnp.arange(NB, dtype=jnp.int32)
    nearby = jnp.abs(block_ids[:, None] - block_ids[None, :]) <= 1
    chosen = jnp.any(random_blocks[:, :, :, None] == block_ids[None, None, None, :], axis=2)
    marked = jnp.any(global_blocks[:, None] == block_ids[None, :], axis=0)
    block_table = nearby[None] | chosen | marked[None, None, :] | marked[None, :, None]
    return jnp.repeat(jnp.repeat(block_table, BLK, axis=1), BLK, axis=2)


def seq_logits(seq_queries, seq_keys, labels, pattern):
    same_doc = (labels[:, None] == labels[None, :]) & (labels[None, :] != 0)
    raw_scores = jnp.einsum(
        "qhd,khd->hqk", seq_queries, seq_keys, preferred_element_type=jnp.float32
    )
    return jnp.where(pattern & same_doc[None], raw_scores * (1.0 / math.sqrt(HD)), -1000000000.0)


def attend_plain(queries, key_block, value_block, segments, pattern):

    def one_seq(pieces):
        seq_queries, seq_keys, seq_values, labels = pieces
        logits = seq_logits(seq_queries, seq_keys, labels, pattern)
        row_peak = jnp.max(logits, axis=2, keepdims=True)
        exp_terms = jnp.exp(logits - row_peak)
        row_total = jnp.sum(exp_terms, axis=2, keepdims=True)
        softmax = (exp_terms / row_total).astype(jnp.bfloat16)
        attended = jnp.einsum(
            "hqk,khd->qhd", softmax, seq_values, preferred_element_type=jnp.float32
        )
        live_rows = (labels != 0).astype(jnp.float32)
        return (attended * live_rows[:, None, None], (row_peak + jnp.log(row_total))[:, :, 0])

    return lax.map(one_seq, (queries, key_block, value_block, segments))


def attend_plain_backward(queries, key_block, value_block, segments, pattern, grad_heads, log_total):

    def one_seq(pieces):
        seq_queries, seq_keys, seq_values, labels, seq_grads, seq_log = pieces
        logits = seq_logits(seq_queries, seq_keys, labels, pattern)
        softmax = jnp.exp(logits - seq_log[:, :, None])
        grad_probs = jnp.einsum(
            "qhd,khd->hqk", seq_grads, seq_values, preferred_element_type=jnp.float32
        )
        grad_values = jnp.einsum(
            "hqk,qhd->khd",
            softmax.astype(jnp.bfloat16),
            seq_grads,
            preferred_element_type=jnp.float32,
        )
        inner_sum = jnp.sum(softmax * grad_probs, axis=2, keepdims=True)
        grad_raw = (softmax * (grad_probs - inner_sum) * (1.0 / math.sqrt(HD))).astype(jnp.bfloat16)
        grad_queries = jnp.einsum(
            "hqk,khd->qhd", grad_raw, seq_keys, preferred_element_type=jnp.float32
        )
        grad_keys = jnp.einsum(
            "hqk,qhd->khd", grad_raw, seq_queries, preferred_element_type=jnp.float32
        )
        return (grad_queries, grad_keys, grad_values)

    return lax.map(one_seq, (queries, key_block, value_block, segments, grad_heads, log_total))


def gelu_tanh(values):
    return jax.nn.gelu(values, approximate=True)


def weight_grad(left, right):
    return lax.dot_general(
        left, right, (((0,), (0,)), ((), ())), preferred_element_type=jnp.float32
    )


def body(
    inputs,
    gain_first,
    shift_first,
    w_query,
    w_key,
    w_value,
    w_output,
    gain_second,
    shift_second,
    w_up,
    bias_up,
    w_down,
    bias_down,
    segments,
    random_blocks,
    global_blocks,
    cotangent,
):
    seq_count, seq_len = segments.shape
    head_width = w_query.shape[1]
    heads_here = random_blocks.shape[0]
    seq_shape = (seq_count, seq_len, heads_here, HD)
    pattern = head_masks(random_blocks, global_blocks)
    live_tokens = (segments != 0).reshape(-1)
    x_first = inputs.astype(jnp.float32)
    first_full, normed_one, inverse_one = norm_forward(x_first, gain_first, shift_first)
    first_low = first_full.astype(jnp.bfloat16)
    stacked = jnp.concatenate((w_query, w_key, w_value), axis=1)
    projected, first_all = to_columns(first_low, stacked, False)
    proj_low = projected.astype(jnp.bfloat16)
    queries = proj_low[:, :head_width].reshape(seq_shape)
    key_block = proj_low[:, head_width : 2 * head_width].reshape(seq_shape)
    value_block = proj_low[:, 2 * head_width :].reshape(seq_shape)
    heads_out, log_total = attend_plain(queries, key_block, value_block, segments, pattern)
    heads_low = heads_out.reshape(-1, head_width).astype(jnp.bfloat16)
    mixed_out, heads_all = to_rows(heads_low, w_output, False)
    residual = x_first + mixed_out
    second_full, normed_two, inverse_two = norm_forward(residual, gain_second, shift_second)
    second_low = second_full.astype(jnp.bfloat16)
    upward, second_all = to_columns(second_low, w_up, False)
    upward = upward + bias_up
    hidden_low = gelu_tanh(upward).astype(jnp.bfloat16)
    downward, hidden_all = to_rows(hidden_low, w_down, False)
    layer_out = (residual + (downward + bias_down)).astype(jnp.bfloat16)
    grad_hidden, cotangent_all = to_columns(cotangent, w_down, True)
    activated, pull_back = jax.vjp(gelu_tanh, upward)
    grad_upward = pull_back(grad_hidden)[0].astype(jnp.bfloat16)
    grad_second, grad_upward_all = to_rows(grad_upward, w_up, True)
    grad_residual = cotangent.astype(jnp.float32) + norm_backward(
        grad_second, normed_two, inverse_two, gain_second
    )
    grad_mixed = grad_residual.astype(jnp.bfloat16)
    grad_heads, grad_mixed_all = to_columns(grad_mixed, w_output, True)
    grad_heads = jnp.where(live_tokens[:, None], grad_heads, 0.0).astype(jnp.bfloat16)
    grad_queries, grad_keys, grad_values = attend_plain_backward(
        queries, key_block, value_block, segments, pattern, grad_heads.reshape(seq_shape), log_total
    )
    grad_proj = jnp.concatenate(
        (
            grad_queries.reshape(-1, head_width),
            grad_keys.reshape(-1, head_width),
            grad_values.reshape(-1, head_width),
        ),
        axis=1,
    ).astype(jnp.bfloat16)
    grad_first, grad_proj_all = to_rows(grad_proj, stacked, True)
    grad_inputs = grad_residual + norm_backward(grad_first, normed_one, inverse_one, gain_first)
    grad_stacked = weight_grad(first_all, grad_proj_all)
    grad_out_weight = weight_grad(heads_all, grad_mixed_all)
    grad_up_weight = weight_grad(second_all, grad_upward_all)
    grad_down_weight = weight_grad(hidden_all, cotangent_all)
    grad_up_bias = jnp.sum(grad_upward_all, axis=0, dtype=jnp.float32)
    grad_down_bias = jnp.sum(cotangent_all, axis=0, dtype=jnp.float32)
    gain_terms = lax.psum(
        (
            jnp.sum(grad_first * normed_one, axis=0),
            jnp.sum(grad_first, axis=0),
            jnp.sum(grad_second * normed_two, axis=0),
            jnp.sum(grad_second, axis=0),
        ),
        ("dp", "col"),
    )
    summed = (
        lax.psum(grad_stacked.astype(jnp.bfloat16), "dp").astype(jnp.float32),
        lax.psum(grad_out_weight.astype(jnp.bfloat16), "dp").astype(jnp.float32),
        lax.psum(grad_up_weight.astype(jnp.bfloat16), "dp").astype(jnp.float32),
        lax.psum(grad_down_weight.astype(jnp.bfloat16), "dp").astype(jnp.float32),
        lax.psum(grad_up_bias.astype(jnp.bfloat16), "dp").astype(jnp.float32),
        lax.psum(grad_down_bias.astype(jnp.bfloat16), "dp").astype(jnp.float32),
    )
    return (
        layer_out,
        grad_inputs,
        gain_terms[0],
        gain_terms[1],
        summed[0][:, :head_width],
        summed[0][:, head_width : 2 * head_width],
        summed[0][:, 2 * head_width :],
        summed[1],
        gain_terms[2],
        gain_terms[3],
        summed[2],
        summed[4],
        summed[3],
        summed[5],
    )


SWAP = [(0, 1), (1, 0)]
LOW = jnp.bfloat16
FULL = jnp.float32
TILE = 256
BIG = 1e30


def swap(array, axis):
    return lax.ppermute(array, axis, SWAP)


def dot_nn(left, right):
    return lax.dot_general(left, right, (((1,), (0,)), ((), ())), preferred_element_type=FULL)


def dot_nt(left, right):
    return lax.dot_general(left, right, (((1,), (1,)), ((), ())), preferred_element_type=FULL)


def dot_tn(left, right):
    return lax.dot_general(left, right, (((0,), (0,)), ((), ())), preferred_element_type=FULL)


def attention_extras(labels, random_blocks, global_blocks):
    length = labels.shape[0]
    blocks = length // BLK
    block_ids = jnp.arange(blocks, dtype=jnp.int32)
    nearby = jnp.abs(block_ids[:, None] - block_ids[None, :]) <= 1
    chosen = jnp.any(random_blocks[:, :, :, None] == block_ids[None, None, None, :], axis=2)
    marked = jnp.any(global_blocks[:, None] == block_ids[None, :], axis=0)
    table = nearby[None] | chosen | marked[None, None, :] | marked[None, :, None]
    heads = table.shape[0]
    lane = jnp.arange(HD, dtype=jnp.int32)
    place = jnp.arange(length, dtype=jnp.int32) // BLK
    doc_lane = blocks + jnp.where(labels == 0, 4, labels - 1)
    row_extra = ((lane[None, :] == place[:, None]) | (lane[None, :] == doc_lane[:, None])).astype(LOW)
    table_keys = jnp.pad(jnp.swapaxes(table, 1, 2), ((0, 0), (0, 0), (0, HD - blocks)), constant_values=True)
    table_keys = jnp.repeat(table_keys, BLK, axis=1)
    is_doc = (lane >= blocks) & (lane <= blocks + 4)
    doc_bad = is_doc[None, :] & (lane[None, :] != doc_lane[:, None])
    doc_bad = doc_bad | (lane[None, :] == blocks + 4)
    key_extra = jnp.where(table_keys & ~doc_bad[None], 0.0, -BIG)
    key_extra = jnp.where((lane >= blocks + 5) & (lane <= blocks + 7), 1.0, key_extra).astype(LOW)
    rows = jnp.stack((jnp.pad(row_extra, ((0, 0), (HD, 0))), jnp.pad(row_extra, ((0, 0), (0, HD)))))
    even = jnp.pad(key_extra[0::2], ((0, 0), (0, 0), (HD, 0)))
    odd = jnp.pad(key_extra[1::2], ((0, 0), (0, 0), (0, HD)))
    keys = jnp.stack((even, odd), axis=1).reshape(heads, length, 2 * HD)
    tiles = length // TILE
    known = labels[None, :] == jnp.arange(1, 5, dtype=jnp.int32)[:, None]
    present = jnp.any(known.reshape(4, tiles, TILE), axis=2)
    wanted = jnp.any(present[:, :, None] & known[:, None, :], axis=0)
    spots = jnp.arange(length, dtype=jnp.int32)
    first = jnp.min(jnp.where(wanted, spots[None, :], length - 1), axis=1)
    last = jnp.max(jnp.where(wanted, spots[None, :], 0), axis=1)
    start = first // 128
    count = jnp.maximum((last + 1 - start * 128 + 255) // 256, 1)
    start = jnp.minimum(start, length // 128 - 2 * count)
    return rows, keys, jnp.stack((start, count)).astype(jnp.int32)


def attend_forward_kernel(where_ref, q_ref, k_ref, v_ref, rows_ref, keys_ref, out_ref, kept_ref, kk, vv):
    length = q_ref.shape[0]
    lane = lax.broadcasted_iota(jnp.int32, (length, 2 * HD), 1)
    for e in range(2):
        data = (lane < HD) if e == 0 else (lane >= HD)
        kk[e] = jnp.where(data, k_ref[...], keys_ref[e])
        vv[e] = jnp.where(data, v_ref[...], jnp.ones_like(v_ref[...]))
    tile_lane = lax.broadcasted_iota(jnp.int32, (TILE, 2 * HD), 1)

    def one_tile(t, carry):
        rows = pl.ds(pl.multiple_of(t * TILE, TILE), TILE)
        start = pl.multiple_of(where_ref[0, t] * 128, 128)
        count = where_ref[1, t]
        q_pair = q_ref[rows, :] * jnp.bfloat16(1.0 / math.sqrt(HD))
        for n in range(1, length // TILE + 1):

            @pl.when(count == n)
            def _():
                span = pl.ds(start, n * TILE)
                outs = []
                for e in range(2):
                    data = (tile_lane < HD) if e == 0 else (tile_lane >= HD)
                    base = HD if e == 0 else 0
                    extra = rows_ref[e, rows, :]
                    q_one = jnp.where(data, q_pair, extra)
                    logits = dot_nt(q_one, kk[e, span, :])
                    peak = jnp.max(logits, axis=1, keepdims=True)
                    terms = jnp.exp(logits - peak)
                    mixed = dot_nn(terms.astype(LOW), vv[e, span, :])
                    total = pltpu.roll(mixed, HD, 1)
                    outs.append(mixed / total)
                    total_one = jnp.max(jnp.where(data, total, 0.0), axis=1, keepdims=True)
                    padded = jnp.max(
                        jnp.where(tile_lane == base + 20, extra.astype(FULL), 0.0), axis=1, keepdims=True
                    )
                    log_total = jnp.where(padded > 0.5, 0.0, -(peak + jnp.log(total_one)))
                    high = log_total.astype(LOW).astype(FULL)
                    middle = (log_total - high).astype(LOW).astype(FULL)
                    low = log_total - high - middle
                    packed = jnp.where(tile_lane == base + 21, high, q_one.astype(FULL))
                    packed = jnp.where(tile_lane == base + 22, middle, packed)
                    packed = jnp.where(tile_lane == base + 23, low, packed)
                    kept_ref[e, rows, :] = packed.astype(LOW)
                joined = jnp.where(tile_lane < HD, outs[0], outs[1])
                out_ref[rows, :] = jnp.where(padded > 0.5, 0.0, joined).astype(LOW)

        return carry

    lax.fori_loop(0, length // TILE, one_tile, 0)


def attend_forward(qkv, rows_extra, keys_extra, where_table):
    length, width = qkv.shape
    pairs = width // (3 * 2 * HD)
    wide = 2 * HD
    return pl.pallas_call(
        attend_forward_kernel,
        out_shape=(
            jax.ShapeDtypeStruct((length, width // 3), LOW),
            jax.ShapeDtypeStruct((2 * pairs, length, wide), LOW),
        ),
        grid_spec=pltpu.PrefetchScalarGridSpec(
            num_scalar_prefetch=1,
            grid=(pairs,),
            in_specs=[
                pl.BlockSpec((length, wide), lambda p, w: (0, p)),
                pl.BlockSpec((length, wide), lambda p, w: (0, pairs + p)),
                pl.BlockSpec((length, wide), lambda p, w: (0, 2 * pairs + p)),
                pl.BlockSpec((2, length, wide), lambda p, w: (0, 0, 0)),
                pl.BlockSpec((2, length, wide), lambda p, w: (p, 0, 0)),
            ],
            out_specs=(
                pl.BlockSpec((length, wide), lambda p, w: (0, p)),
                pl.BlockSpec((2, length, wide), lambda p, w: (p, 0, 0)),
            ),
            scratch_shapes=[pltpu.VMEM((2, length, wide), LOW), pltpu.VMEM((2, length, wide), LOW)],
        ),
        name="attend_forward",
        cost_estimate=pl.CostEstimate(
            flops=8 * pairs * length * length * HD, bytes_accessed=16 * length * width, transcendentals=0
        ),
    )(where_table, qkv, qkv, qkv, rows_extra, keys_extra)


def attend_backward_kernel(
    where_ref, kept_ref, k_ref, v_ref, keys_ref, heads_ref, grads_ref, out_ref, kk, va, dk_sum, dv_sum
):
    length = k_ref.shape[0]
    wide = 2 * HD
    third = out_ref.shape[1] // 3
    pair = pl.program_id(0) * wide
    lane = lax.broadcasted_iota(jnp.int32, (length, wide), 1)
    for e in range(2):
        data = (lane < HD) if e == 0 else (lane >= HD)
        base = HD if e == 0 else 0
        kk[e] = jnp.where(data, k_ref[...], keys_ref[e])
        ones = jnp.where((lane == base) | (lane == base + 1), 1.0, 0.0).astype(LOW)
        va[e] = jnp.where(data, v_ref[...], ones)
    dk_sum[...] = jnp.zeros_like(dk_sum)
    dv_sum[...] = jnp.zeros_like(dv_sum)
    tile_lane = lax.broadcasted_iota(jnp.int32, (TILE, wide), 1)

    def one_tile(t, carry):
        rows = pl.ds(pl.multiple_of(t * TILE, TILE), TILE)
        start = pl.multiple_of(where_ref[0, t] * 128, 128)
        count = where_ref[1, t]
        grads = grads_ref[rows, :]
        both = grads.astype(FULL) * heads_ref[rows, :].astype(FULL)
        for n in range(1, length // TILE + 1):

            @pl.when(count == n)
            def _():
                span = pl.ds(start, n * TILE)
                outs = []
                for e in range(2):
                    data = (tile_lane < HD) if e == 0 else (tile_lane >= HD)
                    base = HD if e == 0 else 0
                    inner = -jnp.sum(jnp.where(data, both, 0.0), axis=1, keepdims=True)
                    high = inner.astype(LOW).astype(FULL)
                    only = jnp.where(data, grads, jnp.zeros_like(grads))
                    packed = jnp.where(tile_lane == base, high, only.astype(FULL))
                    packed = jnp.where(tile_lane == base + 1, inner - high, packed).astype(LOW)
                    q_one = kept_ref[e, rows, :]
                    q_only = jnp.where(data, q_one, jnp.zeros_like(q_one))
                    probs = jnp.exp(dot_nt(kk[e, span, :], q_one))
                    grad_raw = (probs * dot_nt(va[e, span, :], packed)).astype(LOW)
                    dv_sum[span, :] += dot_nn(probs.astype(LOW), only)
                    dk_sum[span, :] += dot_nn(grad_raw, q_only)
                    outs.append(dot_tn(grad_raw, kk[e, span, :]))
                joined = jnp.where(tile_lane < HD, outs[0], outs[1])
                lanes = pl.ds(pl.multiple_of(pair, wide), wide)
                out_ref[rows, lanes] = (joined * (1.0 / math.sqrt(HD))).astype(LOW)

        return carry

    lax.fori_loop(0, length // TILE, one_tile, 0)
    out_ref[:, pl.ds(pl.multiple_of(third + pair, wide), wide)] = dk_sum[...].astype(LOW)
    out_ref[:, pl.ds(pl.multiple_of(2 * third + pair, wide), wide)] = dv_sum[...].astype(LOW)


def attend_backward(kept, qkv, keys_extra, heads, grads, group, where_table):
    length, width = qkv.shape
    pairs = width // (3 * 2 * HD)
    wide = 2 * HD
    stacked = pl.BlockSpec((2, length, wide), lambda p, w: (p, 0, 0))
    return pl.pallas_call(
        attend_backward_kernel,
        out_shape=jax.ShapeDtypeStruct((length, width), LOW),
        grid_spec=pltpu.PrefetchScalarGridSpec(
            num_scalar_prefetch=1,
            grid=(pairs,),
            in_specs=[
                stacked,
                pl.BlockSpec((length, wide), lambda p, w: (0, pairs + p)),
                pl.BlockSpec((length, wide), lambda p, w: (0, 2 * pairs + p)),
                stacked,
                pl.BlockSpec((length, wide), lambda p, w: (0, p)),
                pl.BlockSpec((length, wide), lambda p, w: (0, group * pairs + p)),
            ],
            out_specs=pl.BlockSpec((length, width), lambda p, w: (0, 0)),
            scratch_shapes=[
                pltpu.VMEM((2, length, wide), LOW),
                pltpu.VMEM((2, length, wide), LOW),
                pltpu.VMEM((length, wide), FULL),
                pltpu.VMEM((length, wide), FULL),
            ],
        ),
        name="attend_backward",
        cost_estimate=pl.CostEstimate(
            flops=20 * pairs * length * length * HD, bytes_accessed=20 * length * width, transcendentals=0
        ),
    )(where_table, kept, qkv, qkv, keys_extra, heads, grads)


def row_tiles(count):
    def spec(width):
        return pl.BlockSpec((TILE, width), lambda t: (t, 0))

    return spec


def whole(shape):
    return pl.BlockSpec(shape, lambda t: (0,) * len(shape))


def cost(flops, moved):
    return pl.CostEstimate(flops=int(flops), bytes_accessed=int(moved), transcendentals=0)


def norm_parts(blocks):
    width = sum(b.shape[1] for b in blocks)
    total = sum(jnp.sum(b, axis=1, keepdims=True) for b in blocks)
    squares = sum(jnp.sum(b * b, axis=1, keepdims=True) for b in blocks)
    center = total / width
    return center, lax.rsqrt(squares / width - center * center + EPS)


def columns(ref, index, width):
    return ref[:, index * width : (index + 1) * width]


def first_norm_kernel(x0, x1, x2, x3, gain_ref, shift_ref, low_ref, high_ref):
    blocks = [x[...].astype(FULL) for x in (x0, x1, x2, x3)]
    n = blocks[0].shape[1]
    center, inverse = norm_parts(blocks)
    for i, block in enumerate(blocks):
        value = (block - center) * inverse * columns(gain_ref, i, n) + columns(shift_ref, i, n)
        (low_ref, high_ref)[i // 2][:, (i % 2) * n : (i % 2 + 1) * n] = value.astype(LOW)


def first_norm(blocks, gain, shift):
    length, n = blocks[0].shape
    rows = row_tiles(length)
    half = jax.ShapeDtypeStruct((length, 2 * n), LOW)
    return pl.pallas_call(
        first_norm_kernel,
        out_shape=(half, half),
        grid=(length // TILE,),
        in_specs=[rows(n)] * 4 + [whole((1, 4 * n))] * 2,
        out_specs=(rows(2 * n), rows(2 * n)),
        name="first_norm",
        cost_estimate=cost(20 * length * n, 16 * length * n),
    )(*blocks, gain, shift)


def second_norm_kernel(x0, x1, x2, x3, part_ref, got_ref, gain_ref, shift_ref, residual_ref, second_ref):
    n = x0.shape[1]
    blocks = []
    for i, x in enumerate((x0, x1, x2, x3)):
        mixed = columns(part_ref, i, n).astype(FULL) + columns(got_ref, i ^ 1, n).astype(FULL)
        blocks.append(x[...].astype(FULL) + mixed)
    center, inverse = norm_parts(blocks)
    for i, block in enumerate(blocks):
        residual_ref[:, i * n : (i + 1) * n] = block
        value = (block - center) * inverse * columns(gain_ref, i, n) + columns(shift_ref, i, n)
        second_ref[i // 2, :, (i % 2) * n : (i % 2 + 1) * n] = value.astype(LOW)


def second_norm(blocks, part, got, gain, shift):
    length, n = blocks[0].shape
    rows = row_tiles(length)
    return pl.pallas_call(
        second_norm_kernel,
        out_shape=(jax.ShapeDtypeStruct((length, 4 * n), FULL), jax.ShapeDtypeStruct((2, length, 2 * n), LOW)),
        grid=(length // TILE,),
        in_specs=[rows(n)] * 4 + [rows(4 * n)] * 2 + [whole((1, 4 * n))] * 2,
        out_specs=(rows(4 * n), pl.BlockSpec((2, TILE, 2 * n), lambda t: (0, t, 0))),
        name="second_norm",
        cost_estimate=cost(30 * length * n, 48 * length * n),
    )(*blocks, part, got, gain, shift)


def norm_gradient(blocks, part_ref, got_ref, gain_ref, sums_ref):
    n = blocks[0].shape[1]
    center, inverse = norm_parts(blocks)
    normed = [(b - center) * inverse for b in blocks]
    grads = [columns(part_ref, i, n).astype(FULL) + columns(got_ref, i ^ 1, n).astype(FULL) for i in range(4)]
    scaled = [g * columns(gain_ref, i, n) for i, g in enumerate(grads)]
    mean_one = sum(jnp.sum(s, axis=1, keepdims=True) for s in scaled) / (4 * n)
    mean_two = sum(jnp.sum(s * z, axis=1, keepdims=True) for s, z in zip(scaled, normed)) / (4 * n)

    @pl.when(pl.program_id(0) == 0)
    def _():
        sums_ref[...] = jnp.zeros_like(sums_ref)

    for slot, i in enumerate((0, 2)):
        place = slice(slot * n, (slot + 1) * n)
        sums_ref[0:1, place] += jnp.sum(grads[i] * normed[i], axis=0, keepdims=True)
        sums_ref[1:2, place] += jnp.sum(grads[i], axis=0, keepdims=True)
    return [inverse * (s - mean_one - z * mean_two) for s, z in zip(scaled, normed)]


def second_norm_back_kernel(
    residual_ref, part_ref, got_ref, cots_ref, gain_ref, own_ref, other_ref, mixed_ref, sums_ref
):
    n = residual_ref.shape[1] // 4
    blocks = [columns(residual_ref, i, n) for i in range(4)]
    for i, grad in enumerate(norm_gradient(blocks, part_ref, got_ref, gain_ref, sums_ref)):
        total = cots_ref[i // 2, :, (i % 2) * n : (i % 2 + 1) * n].astype(FULL) + grad
        mixed_ref[:, i * n : (i + 1) * n] = total.astype(LOW)
        if i % 2 == 0:
            (own_ref, other_ref)[i // 2][...] = total


def second_norm_back(residual, part, got, cots, gain):
    length, width = residual.shape
    n = width // 4
    rows = row_tiles(length)
    one = jax.ShapeDtypeStruct((length, n), FULL)
    return pl.pallas_call(
        second_norm_back_kernel,
        out_shape=(one, one, jax.ShapeDtypeStruct((length, width), LOW), jax.ShapeDtypeStruct((8, 2 * n), FULL)),
        grid=(length // TILE,),
        in_specs=[rows(width)] * 3 + [pl.BlockSpec((2, TILE, 2 * n), lambda t: (0, t, 0)), whole((1, width))],
        out_specs=(rows(n), rows(n), rows(width), whole((8, 2 * n))),
        name="second_norm_back",
        cost_estimate=cost(60 * length * n, 64 * length * n),
    )(residual, part, got, cots, gain)


def first_norm_back_kernel(
    x0, x1, x2, x3, part_ref, got_ref, own_ref, other_ref, gain_ref, mine_ref, theirs_ref, sums_ref
):
    blocks = [x[...].astype(FULL) for x in (x0, x1, x2, x3)]
    grads = norm_gradient(blocks, part_ref, got_ref, gain_ref, sums_ref)
    mine_ref[...] = own_ref[...] + grads[0]
    theirs_ref[...] = (other_ref[...] + grads[2]).astype(LOW)


def first_norm_back(blocks, part, got, own, other, gain):
    length, n = blocks[0].shape
    rows = row_tiles(length)
    return pl.pallas_call(
        first_norm_back_kernel,
        out_shape=(
            jax.ShapeDtypeStruct((length, n), FULL),
            jax.ShapeDtypeStruct((length, n), LOW),
            jax.ShapeDtypeStruct((8, 2 * n), FULL),
        ),
        grid=(length // TILE,),
        in_specs=[rows(n)] * 4 + [rows(4 * n)] * 2 + [rows(n)] * 2 + [whole((1, 4 * n))],
        out_specs=(rows(n), rows(n), whole((8, 2 * n))),
        name="first_norm_back",
        cost_estimate=cost(60 * length * n, 40 * length * n),
    )(*blocks, part, got, own, other, gain)


def mix_kernel(h0, h1, w0, w1, out_ref):
    out_ref[...] = (dot_nn(h0[...], w0[...]) + dot_nn(h1[...], w1[...])).astype(LOW)


def mix_heads(heads, weights):
    length, depth = heads[0].shape
    width = weights[0].shape[1]
    rows = row_tiles(length)
    return pl.pallas_call(
        mix_kernel,
        out_shape=jax.ShapeDtypeStruct((length, width), LOW),
        grid=(length // TILE,),
        in_specs=[rows(depth)] * 2 + [whole((depth, width))] * 2,
        out_specs=rows(width),
        name="mix_heads",
        cost_estimate=cost(4 * length * depth * width, 4 * length * (depth + width)),
    )(*heads, *weights)


ROOT = math.sqrt(2.0 / math.pi)


def feed_forward_kernel(
    at_ref, s_ref, c_ref, u_low, u_high, d_low, d_high, bias_ref, part_ref, hidden_ref, grad_ref, bias_sum, low_sum, high_sum
):
    step = pl.program_id(0)

    @pl.when(step == 0)
    def _():
        low_sum[...] = jnp.zeros_like(low_sum)
        high_sum[...] = jnp.zeros_like(high_sum)

    totals = 0.0
    for t in range(s_ref.shape[1] // TILE):
        rows = slice(t * TILE, (t + 1) * TILE)
        upward = dot_nn(s_ref[0, rows, :], u_low[0]) + dot_nn(s_ref[1, rows, :], u_high[0]) + bias_ref[0]
        grad_hidden = dot_nt(c_ref[0, rows, :], d_low[0]) + dot_nt(c_ref[1, rows, :], d_high[0])
        square = upward * upward
        bent = jnp.tanh(upward * (ROOT + (ROOT * 0.044715) * square))
        lifted = 0.5 + 0.5 * bent
        slope = lifted + (0.5 * upward) * (1.0 - bent * bent) * (ROOT + (ROOT * 3 * 0.044715) * square)
        hidden_ref[0, rows, :] = (upward * lifted).astype(LOW)
        grad = grad_hidden * slope
        totals = totals + jnp.sum(grad, axis=0, keepdims=True)
        grad = grad.astype(LOW)
        grad_ref[0, rows, :] = grad
        low_sum[rows, :] += dot_nt(grad, u_low[0])
        high_sum[rows, :] += dot_nt(grad, u_high[0])
    bias_sum[0] = jnp.broadcast_to(totals, bias_sum.shape[1:])

    @pl.when(step == pl.num_programs(0) - 1)
    def _():
        n = low_sum.shape[1]
        part_ref[:, :n] = low_sum[...].astype(LOW)
        part_ref[:, n:] = high_sum[...].astype(LOW)


def feed_forward(at, seconds, cots, weights, biases):
    _, length, h = seconds.shape
    each = weights.shape[1] // 2
    tiles = each // TILE
    per = h // TILE
    keep = pl.BlockSpec((2, length, h), lambda i, at: (0, 0, 0))

    def up_spec(flip):
        return pl.BlockSpec(
            (1, h, TILE),
            lambda i, at: (
                (at[0] ^ flip) * 2 + (at[1] ^ (i // tiles)), lax.rem(i, tiles) // per, lax.rem(lax.rem(i, tiles), per)
            ),
        )

    def down_spec(flip):
        return pl.BlockSpec(
            (1, TILE, h), lambda i, at: ((at[0] ^ flip) * 2 + (at[1] ^ (i // tiles)), tiles + lax.rem(i, tiles), 0)
        )

    side = pl.BlockSpec((1, length, TILE), lambda i, at: (i // tiles, 0, lax.rem(i, tiles)))
    one = jax.ShapeDtypeStruct((2, length, each), LOW)
    return pl.pallas_call(
        feed_forward_kernel,
        out_shape=(
            jax.ShapeDtypeStruct((length, 2 * h), LOW), one, one, jax.ShapeDtypeStruct((2 * tiles, 8, TILE), FULL),
        ),
        grid_spec=pltpu.PrefetchScalarGridSpec(
            num_scalar_prefetch=1,
            grid=(2 * tiles,),
            in_specs=[keep] * 2
            + [up_spec(0), up_spec(1), down_spec(0), down_spec(1)]
            + [pl.BlockSpec((1, 1, TILE), lambda i, at: (i, 0, 0))],
            out_specs=(
                pl.BlockSpec((length, 2 * h), lambda i, at: (0, 0)), side, side,
                pl.BlockSpec((1, 8, TILE), lambda i, at: (i, 0, 0)),
            ),
            scratch_shapes=[pltpu.VMEM((length, h), FULL), pltpu.VMEM((length, h), FULL)],
        ),
        name="feed_forward",
        cost_estimate=cost(12 * length * 2 * h * each, 8 * length * h + 16 * h * each + 16 * length * each),
    )(at, seconds, cots, weights, weights, weights, weights, biases.reshape(2 * tiles, 1, TILE))


def up_grads_kernel(at_ref, s_ref, grad_ref, out_ref, turned):
    h = out_ref.shape[2]

    @pl.when(pl.program_id(1) == 0)
    def _():
        turned[...] = s_ref[0].T

    for i in range(out_ref.shape[1] // h):
        part = dot_nn(turned[...], grad_ref[0, :, i * h : (i + 1) * h])
        out_ref[0, i * h : (i + 1) * h, :] = part.astype(LOW)


def up_grads(at, seconds, grads):
    _, length, h = seconds.shape
    each = grads.shape[2]
    return pl.pallas_call(
        up_grads_kernel,
        out_shape=jax.ShapeDtypeStruct((4, each, h), LOW),
        grid_spec=pltpu.PrefetchScalarGridSpec(
            num_scalar_prefetch=1,
            grid=(2, 2),
            in_specs=[
                pl.BlockSpec((1, length, h), lambda y, c, at: (y, 0, 0)),
                pl.BlockSpec((1, length, each), lambda y, c, at: (c, 0, 0)),
            ],
            out_specs=pl.BlockSpec((1, each, h), lambda y, c, at: ((at[0] ^ y) * 2 + (at[1] ^ c), 0, 0)),
            scratch_shapes=[pltpu.VMEM((h, length), LOW)],
        ),
        name="up_grads",
        cost_estimate=cost(8 * length * h * each, 4 * length * each + 8 * h * each),
    )(at, seconds, grads)


def down_grads_kernel(at_ref, hidden_ref, c_ref, out_ref):
    turned = hidden_ref[0].T
    for y in range(2):
        out_ref[at_ref[0] ^ y, 0] = dot_nn(turned, c_ref[y]).astype(LOW)


def down_grads(at, hiddens, cots):
    _, length, h = cots.shape
    each = hiddens.shape[2]
    return pl.pallas_call(
        down_grads_kernel,
        out_shape=jax.ShapeDtypeStruct((2, 2, each, h), LOW),
        grid_spec=pltpu.PrefetchScalarGridSpec(
            num_scalar_prefetch=1,
            grid=(2, each // h),
            in_specs=[
                pl.BlockSpec((1, length, h), lambda c, b, at: (c, 0, b)),
                pl.BlockSpec((2, length, h), lambda c, b, at: (0, 0, 0)),
            ],
            out_specs=pl.BlockSpec((2, 1, h, h), lambda c, b, at: (0, at[1] ^ c, b, 0)),
        ),
        name="down_grads",
        cost_estimate=cost(8 * length * h * each, 4 * length * each + 8 * h * each),
    )(at, hiddens, cots)


def layer_end_kernel(at_ref, h0, h1, w00, w01, w10, w11, own_ref, theirs_ref):
    n = own_ref.shape[1] // 2
    for j, (a, b) in enumerate(((w00, w01), (w10, w11))):
        part = dot_nn(h0[0], a[0]) + dot_nn(h1[0], b[0])
        own_ref[:, j * n : (j + 1) * n] = part[:, :n]
        theirs_ref[:, j * n : (j + 1) * n] = part[:, n:].astype(LOW)


def layer_end(at, hiddens, weights):
    _, length, each = hiddens.shape
    h = weights.shape[2]
    out = pl.BlockSpec((TILE, h), lambda t, at: (t, 0))

    def rows(c):
        return pl.BlockSpec((1, TILE, each), lambda t, at: (c, t, 0))

    def weight(y, col):
        return pl.BlockSpec((1, each, h), lambda t, at: ((at[0] ^ y) * 2 + (at[1] ^ col), 1, 0))

    return pl.pallas_call(
        layer_end_kernel,
        out_shape=(jax.ShapeDtypeStruct((length, h), FULL), jax.ShapeDtypeStruct((length, h), LOW)),
        grid_spec=pltpu.PrefetchScalarGridSpec(
            num_scalar_prefetch=1,
            grid=(length // TILE,),
            in_specs=[rows(0), rows(1), weight(0, 0), weight(0, 1), weight(1, 0), weight(1, 1)],
            out_specs=(out, out),
        ),
        name="layer_end",
        cost_estimate=cost(8 * length * h * each, 8 * h * each + 12 * length * h),
    )(at, hiddens, hiddens, weights, weights, weights, weights)


def after(values, *late):
    return lax.optimization_barrier((values, late))[0]


def pick(pair, index):
    return lax.dynamic_index_in_dim(pair, index, 0, keepdims=False)


def ordered(own, other, index):
    flip = index == 0
    return jnp.stack((jnp.where(flip, own, other), jnp.where(flip, other, own)))


def swap_across(array):
    return lax.ppermute(array, ("y", "col"), [(0, 3), (3, 0), (1, 2), (2, 1)])


def plane_gather(block):
    return block, swap(block, "y"), swap(block, "col"), swap_across(block)


def plane_exchange(at_y, at_col, across):
    return swap(at_y, "y"), swap(at_col, "col"), swap_across(across)


def plane_sum(own, got):
    return (own.astype(FULL) + sum(g.astype(FULL) for g in got)).astype(LOW)


def add_low(left, right):
    return (left.astype(FULL) + right.astype(FULL)).astype(LOW)


PAIRS = [(0, 1), (1, 0), (2, 3), (3, 2)]
FAR = [(0, 2), (2, 0), (1, 3), (3, 1)]


def depth_pair(array, odd):
    halves = array.reshape(2, array.shape[0] // 2, array.shape[1])
    return add_low(pick(halves, odd), lax.ppermute(pick(halves, 1 - odd), "dp", PAIRS))


def depth_far(part):
    return add_low(part, lax.ppermute(part, "dp", FAR))


def depth_join(part, odd):
    return ordered(part, lax.ppermute(part, "dp", PAIRS), odd).reshape(-1, part.shape[1])


def half(weight, axis, index):
    size = weight.shape[axis] // 2
    return lax.dynamic_slice_in_dim(weight, index * size, size, axis)


def fast_body(
    inputs, gain_first, shift_first, w_query, w_key, w_value, w_output, gain_second, shift_second,
    w_up, bias_up, w_down, bias_down, segments, random_blocks, global_blocks, cotangent,
):
    depth_at, y_at, core_at, col_at = (lax.axis_index(name) for name in ("dp", "y", "core", "col"))
    length = segments.shape[1]
    n = inputs.shape[1]
    h = 2 * n
    at = jnp.stack((y_at, col_at)).astype(jnp.int32)

    def chip_block(weights, axis, join):
        mine = jnp.concatenate([half(w, axis, core_at) for w in weights], axis=axis)
        theirs = swap(jnp.concatenate([half(w, axis, 1 - core_at) for w in weights], axis=axis), "core")
        return jnp.concatenate((mine, theirs), axis=join)

    inputs_pair = inputs.reshape(2, length, n)
    x_own = pick(inputs_pair, y_at)
    x_y = swap(pick(inputs_pair, 1 - y_at), "y")
    qkv_block = chip_block((w_query, w_key, w_value), 1, 0)
    qkv_own, qkv_y, qkv_x, qkv_xy = plane_gather(qkv_block)
    xs = (x_own, swap(x_own, "core"), x_y, swap(x_y, "core"))
    w_up, w_down = after((w_up, w_down), qkv_block)
    up_block, down_block = chip_block((w_up,), 1, 0), chip_block((w_down,), 0, 1)
    ups = up_block.shape[1] // h
    ffn_block = jnp.concatenate([up_block[:, i * h : (i + 1) * h] for i in range(ups)] + [down_block])
    ffn_block, w_output, cotangent_late = after((ffn_block, w_output, cotangent), qkv_y, qkv_x)
    ffn = lax.all_gather(ffn_block, ("y", "col"), axis=0, tiled=False)
    out_own, out_y, out_x, out_xy = plane_gather(chip_block((w_output,), 0, 1))
    cot_pair = cotangent_late.reshape(2, length, n)

    vectors = jnp.stack((gain_first, shift_first, gain_second, shift_second, bias_down))
    vectors = jnp.concatenate((vectors, swap(vectors, "core")), axis=1)
    vectors = jnp.concatenate((vectors, swap(vectors, "y")), axis=1)
    gain_one, shift_one, gain_two, shift_two, bias_low = (vectors[i : i + 1] for i in range(5))
    heads_half = half(random_blocks, 0, core_at)
    hidden_bias = half(bias_up, 0, core_at)
    each = hidden_bias.shape[0]
    small = swap(jnp.concatenate((hidden_bias, heads_half.astype(FULL).reshape(-1))), "col")
    biases = jnp.concatenate((hidden_bias, small[:each]))
    heads_half_x = small[each:].reshape(heads_half.shape).astype(jnp.int32)
    moves = []
    for y in range(2):
        for core in range(2):
            for col in range(2):
                moves.append(((col * 2 + y) * 2 + core, (y * 2 + core) * 2 + col))
    labels = lax.ppermute(segments, ("y", "core", "col"), moves)[0]
    all_heads = jnp.concatenate((heads_half, heads_half_x), axis=0)
    rows_extra, keys_extra, where_table = attention_extras(labels, all_heads, global_blocks)
    near_heads = heads_half.shape[0]
    keys_of = (keys_extra[:near_heads], keys_extra[near_heads:])
    live = (labels != 0)[:, None]

    cot_own = pick(cot_pair, y_at)
    cot_y = swap(pick(cot_pair, 1 - y_at), "y")
    cot_swapped = swap(cot_y, "core")
    cots = jnp.stack([jnp.concatenate(c, axis=1) for c in ((cot_own, swap(cot_own, "core")), (cot_y, cot_swapped))])

    firsts = first_norm(after(xs, qkv_xy), gain_one, shift_one)
    qkv_x = after(qkv_x, out_y, out_x, out_xy, cot_y)
    w_qkv = (jnp.concatenate((qkv_own, qkv_y), axis=0), jnp.concatenate((qkv_x, qkv_xy), axis=0))
    first = jnp.concatenate(firsts, axis=1)
    out_own = after(out_own, cots)
    w_out = (jnp.concatenate((out_own, out_y), axis=1), jnp.concatenate((out_x, out_xy), axis=1))
    qkv, heads, kept = [], [], []
    for i in range(2):
        qkv.append(dot_nn(first, w_qkv[i]).astype(LOW))
        done, saved = attend_forward(qkv[i], rows_extra, keys_of[i], where_table)
        heads.append(done)
        kept.append(saved)
    mixed_part = mix_heads(heads, w_out)
    residual, seconds = second_norm(xs, mixed_part, swap(mixed_part, "core"), gain_two, shift_two)

    second_part, hiddens, up_sides, bias_sum = feed_forward(at, seconds, cots, ffn, biases)
    down_parts = down_grads(at, hiddens, cots).reshape(4, -1, h)
    down_scattered = lax.psum_scatter(down_parts, ("y", "col"), scatter_dimension=0, tiled=True)[0]
    up_parts = up_grads(at, seconds, after(up_sides, down_parts))
    up_scattered = lax.psum_scatter(up_parts, ("y", "col"), scatter_dimension=0, tiled=True)[0]
    second_got = after(swap(second_part, "core"), up_parts)

    grad_own, grad_other, grad_mixed, sums_two = second_norm_back(residual, second_part, second_got, cots, gain_two)
    grads = jnp.where(live, dot_nt(grad_mixed, jnp.concatenate(w_out, axis=0)), 0.0).astype(LOW)
    out_grads = [[dot_tn(grad_mixed[:, j * h : (j + 1) * h], head).astype(LOW) for j in range(2)] for head in heads]
    qkv_sides, qkv_grads = [None, None], [None, None]
    for i in (1, 0):
        qkv_sides[i] = attend_backward(kept[i], qkv[i], keys_of[i], heads[i], grads, i, where_table)
        qkv_grads[i] = [dot_tn(f, qkv_sides[i]).astype(LOW) for f in firsts]
    odd = lax.rem(depth_at, 2)
    out_got = plane_exchange(out_grads[0][1], out_grads[1][0], out_grads[1][1])
    qkv_sides = after(qkv_sides, qkv_grads)
    first_part = dot_nt(jnp.concatenate(qkv_sides, axis=1), jnp.concatenate(w_qkv, axis=1)).astype(LOW)
    down_part = depth_pair(after(down_scattered, qkv_sides[0]), odd)
    down_part = depth_far(down_part)
    first_part = after(first_part, out_got, down_part)
    mine, theirs, sums_one = first_norm_back(xs, first_part, swap(first_part, "core"), grad_own, grad_other, gain_one)

    gains = jnp.concatenate((sums_one[:2, :n], sums_two[:2, :n])).reshape(-1)
    gains_y = jnp.concatenate((sums_one[:2, n:], sums_two[:2, n:])).reshape(-1)
    up_bias = bias_sum[:, 0, :].reshape(-1)
    got = swap(jnp.concatenate((gains_y, up_bias)), "y")
    gains = gains + got[: 4 * n]
    up_bias = up_bias + got[4 * n :]
    near = jnp.concatenate((gains, jnp.sum(cotangent, axis=0, dtype=FULL), up_bias[:each]))
    near = near + swap(jnp.concatenate((near[: 5 * n], up_bias[each:])), "col")
    up_scattered = after(up_scattered, near)
    up_part = depth_pair(up_scattered, odd)
    qkv_got = plane_exchange(*after((qkv_grads[0][1], qkv_grads[1][0], qkv_grads[1][1]), up_scattered))
    up_far = depth_far(up_part)
    theirs = swap(after(theirs, up_far), "y")
    grad_inputs = ordered(mine, theirs.astype(FULL), y_at).reshape(2 * length, n)
    ends_own, ends_other = layer_end(at, after(hiddens, up_part), ffn)
    down_total = depth_join(after(down_part, ends_own), odd)
    kept_two = jnp.concatenate((residual[:, :n], residual[:, 2 * n : 3 * n]), axis=1)
    bias_two = jnp.concatenate((bias_low[:, :n], bias_low[:, 2 * n : 3 * n]), axis=1)
    ends = (kept_two + ends_own + swap(ends_other, "core").astype(FULL) + bias_two).astype(LOW)
    ends_got = swap(ends[:, n:], "y")
    layer_out = ordered(ends[:, :n], ends_got, y_at).reshape(2 * length, n)

    near = after(near, up_part)
    near = near + lax.ppermute(near, "dp", [(0, 1), (1, 0), (2, 3), (3, 2)])
    near = near + lax.ppermute(near, "dp", [(0, 2), (2, 0), (1, 3), (3, 1)])
    gains = near[: 5 * n].reshape(5, n)
    up_bias = ordered(near[5 * n :], swap(near[5 * n :], "core"), core_at).reshape(-1)

    def finish(total, axis, parts):
        keep = lax.slice_in_dim(total, 0, n, axis=axis)
        got = swap(lax.slice_in_dim(total, n, 2 * n, axis=axis), "core")
        size = keep.shape[1 - axis] // parts
        flip = core_at == 0
        out = []
        for i in range(parts):
            a, b = (lax.slice_in_dim(z, i * size, (i + 1) * size, axis=1 - axis) for z in (keep, got))
            out.append(jnp.concatenate((jnp.where(flip, a, b), jnp.where(flip, b, a)), axis=1 - axis).astype(FULL))
        return out

    four = jnp.concatenate(
        (plane_sum(after(qkv_grads[0][0], up_part), qkv_got), plane_sum(out_grads[0][0], out_got)), axis=1
    )
    four = depth_pair(after(four, up_far, near, ends_own), odd)
    up_total = depth_join(up_far, odd)
    four = depth_far(after(four, theirs, ends))
    four = depth_join(after(four, ends_got), odd)
    grad_query, grad_key, grad_value, grad_out = finish(four, 0, 4)
    (grad_down,) = finish(down_total, 1, 1)
    (grad_up,) = finish(jnp.concatenate([up_total[i * h : (i + 1) * h] for i in range(ups)], axis=1), 0, 1)
    return (
        layer_out, grad_inputs, gains[0], gains[1], grad_query, grad_key, grad_value, grad_out.T, gains[2], gains[3],
        grad_up, up_bias, grad_down, gains[4],
    )


def whole_sequences(mesh):
    return mesh.shape["row"] == 4 and mesh.shape["col"] == 2 and mesh.shape["dp"] == 4


def placements(row):
    tokens = P(("dp", "col"), row)
    rows = P(row)
    weight = P(row, "col")
    turned = P("col", row)
    placed = (
        tokens, rows, rows, weight, weight, weight, turned, rows, rows, weight, P("col"), turned, rows,
        P(("dp", *row), None), P("col", None, None), P(), tokens,
    )
    given = (
        tokens, tokens, rows, rows, weight, weight, weight, turned, rows, rows, weight, P("col"), turned, rows,
    )
    return placed, given


def solution(mesh):
    sizes = mesh.shape
    split = jax.sharding.Mesh(
        mesh.devices.reshape(sizes["dp"], sizes["row"] // 2, 2, sizes["col"]), ("dp", "y", "core", "col")
    )

    def run(*arrays):
        tokens, length = arrays[0].shape[0], arrays[13].shape[1]
        if whole_sequences(mesh) and tokens == sizes["dp"] * sizes["col"] * 2 * length:
            placed, given = placements(("y", "core"))
            step = jax.shard_map(fast_body, mesh=split, in_specs=placed, out_specs=given, check_vma=False)
        else:
            placed, given = placements(("row",))
            step = jax.shard_map(body, mesh=mesh, in_specs=placed, out_specs=given, check_vma=False)
        return step(*arrays)

    return run
```
